32 devices in a mesh: seq: 4 (over z), tp: 8 (over y, x, core).
Axes of the slice: x: 2, y: 2, z: 4, core: 2. Of those that a mesh axis runs over, the one named last changes fastest.
Arguments:
- stream: float32 [512, 4, 2048], P(('seq', 'tp')), may hold values from -60 to 60
- norm_gain: float32 [2048], replicated, may hold values from 0.5 to 1.5
- norm_offset: float32 [2048], replicated, may hold values from -3 to 3
- attend_weight: bfloat16 [2048, 3, 2048], P(None, None, 'tp'), as said below
- attend_bias: float32 [3, 2048], P(None, 'tp'), may hold values from -3 to 3
- output_weight: bfloat16 [2048, 2048], P('tp'), may hold values from -2 to 2
- up_weight: bfloat16 [2048, 8192], P(None, 'tp'), may hold values from -0.125 to 0.125
- up_bias: float32 [8192], P('tp'), may hold values from -3 to 3
- down_weight: bfloat16 [8192, 2048], P('tp'), may hold values from -0.0625 to 0.0625
- final_bias: float32 [2048], replicated, may hold values from -3 to 3
- cotangent: float32 [512, 4, 2048], P(('seq', 'tp')), may hold values from -18 to 18
Outputs:
- result: float32 [512, 4, 2048], P(('seq', 'tp'))
- stream_grad: float32 [512, 4, 2048], P(('seq', 'tp'))
- norm_gain_grad: float32 [2048], replicated
- norm_offset_grad: float32 [2048], replicated
- attend_weight_grad: float32 [2048, 3, 2048], P(None, None, 'tp')
- attend_bias_grad: float32 [3, 2048], P(None, 'tp')
- output_weight_grad: float32 [2048, 2048], P('tp')
- up_weight_grad: float32 [2048, 8192], P(None, 'tp')
- up_bias_grad: float32 [8192], P('tp')
- down_weight_grad: float32 [8192, 2048], P('tp')
- final_bias_grad: float32 [2048], replicated
The draws below stay inside these ranges and needn't reach their ends.
Inputs may be any that keep to these rules, and one draw needn't show every extreme that they name: `attend_weight`: entries of order one over the root of 2048.
All inputs are finite; a program needn't handle non-finite values.
Results may differ from the reference program's by a relative error of at most 0.012.
The reference program's roundings to bfloat16 on the way count: a program that leaves them out, or rounds other values in their place, can miss the bound.
Values may be sent and summed in bfloat16 or wider, within the bound.
A program may use at most 192 MiB of HBM per device.

```python
import math
import jax
import jax.numpy as jnp
from jax import lax

D = 2048
HEADS = 32
HEAD_DIM = 64
ROT = 32
FF = 8192
SEQS = 4
LEN = 512


def draw_stream(key, part):
    sample_key, row_key, column_key = jax.random.split(jax.random.fold_in(key, 11), 3)
    row_scale = jnp.exp(jax.random.uniform(row_key, (LEN, SEQS, 1), jnp.float32) * math.log(10.0))
    column_scale = jnp.exp(jax.random.uniform(column_key, (1, 1, D), jnp.float32) * math.log(10.0))
    sample = jnp.clip(jax.random.normal(sample_key, (LEN, SEQS, D), jnp.float32), -6.0, 6.0)
    return (sample * row_scale * column_scale * 0.1).astype(jnp.float32)


def draw_cotangent(key, part):
    sample_key = jax.random.fold_in(key, 13)
    ramp_place = jnp.arange(LEN, dtype=jnp.float32)[:, None, None] / (LEN - 1)
    sample = jnp.clip(jax.random.normal(sample_key, (LEN, SEQS, D), jnp.float32), -6.0, 6.0)
    ramp_scale = 1.0 + 2.0 * ramp_place
    return (sample * ramp_scale).astype(jnp.float32)


def draw_attend_weight(key, part):
    shared_key = jax.random.fold_in(jax.random.fold_in(key, 17), 0)
    spread_unit = D ** (-0.5)
    sample = jnp.clip(jax.random.normal(shared_key, (D, 3, D), jnp.float32), -6.0, 6.0)
    return (sample * spread_unit).astype(jnp.bfloat16)


def level_of(stream_key, shape, pieces, least, largest):
    level = 1.0
    for dim, blocks in pieces:
        draws = jax.random.uniform(jax.random.fold_in(jax.random.fold_in(stream_key, 6), dim), (blocks,), jnp.float32, least / len(pieces), largest / len(pieces))
        level = level * jnp.repeat(jnp.exp(draws), shape[dim] // blocks).reshape((-1,) + (1,) * (len(shape) - 1 - dim))
    return level


def noise(own_key, shape, deviation, limit, cuts=(), held_as=jnp.bfloat16):
    entries = jax.random.normal(own_key, shape, jnp.float32) * deviation
    if len(cuts) > 0:
        entries = level_of(own_key, shape, cuts, -0.22, 0.18) * entries
    return jnp.clip(entries, min=-limit, max=limit).astype(held_as)


def setup_inputs(seed: int = 0) -> dict:
    key_list = jax.random.split(jax.random.key(seed), 12)
    return {
        "stream": draw_stream(jax.random.fold_in(key_list[11], 71), 0),
        "norm_gain": jnp.clip(1.0 + 0.1 * jax.random.normal(key_list[1], (D,), jnp.float32), 0.5, 1.5),
        "norm_offset": noise(key_list[2], (D,), 0.5, 3.0, (), jnp.float32),
        "attend_weight": draw_attend_weight(jax.random.fold_in(key_list[11], 71), 0),
        "attend_bias": noise(key_list[4], (3, D), 0.5, 3.0, ((1, 8),), jnp.float32),
        "output_weight": noise(key_list[5], (D, D), (max(D // 256, 1)) ** -0.5, 2.0, ((0, 8),)),
        "up_weight": noise(key_list[6], (D, FF), D ** -0.5, 0.125, ((1, 8),)),
        "up_bias": noise(key_list[7], (FF,), 0.5, 3.0, ((0, 8),), jnp.float32),
        "down_weight": noise(key_list[8], (FF, D), FF ** -0.5, 0.0625, ((0, 8),)),
        "final_bias": noise(key_list[9], (D,), 0.5, 3.0, (), jnp.float32),
        "cotangent": draw_cotangent(jax.random.fold_in(key_list[11], 71), 0),
    }


EPS = 1e-05
GELU_C = 0.7978845608028654
CUBIC = 0.044715
LOG_BASE = math.log(10000.0)

def gelu_parts(pre_act):
    inner_arg = GELU_C * (pre_act + CUBIC * pre_act * pre_act * pre_act)
    tanh_value = jnp.tanh(inner_arg)
    gelu_value = 0.5 * pre_act * (1.0 + tanh_value)
    gelu_slope = 0.5 * (1.0 + tanh_value) + 0.5 * pre_act * (1.0 - tanh_value * tanh_value) * GELU_C * (1.0 + 3.0 * CUBIC * pre_act * pre_act)
    return (gelu_value, gelu_slope)

def rotary_angles(positions):
    half_rot = ROT // 2
    frequency = jnp.exp(jnp.arange(half_rot, dtype=jnp.float32) * (-2.0 * LOG_BASE / ROT))
    angles = positions.astype(jnp.float32)[:, None] * frequency[None, :]
    return (jnp.cos(angles), jnp.sin(angles))

def rotate(vectors, cosine, sine_table):
    half_rot = ROT // 2
    first_half = vectors[..., :half_rot]
    second_half = vectors[..., half_rot:ROT]
    return jnp.concatenate([first_half * cosine - second_half * sine_table, second_half * cosine + first_half * sine_table, vectors[..., ROT:]], axis=-1)

def unrotate(vectors, cosine, sine_table):
    half_rot = ROT // 2
    first_half = vectors[..., :half_rot]
    second_half = vectors[..., half_rot:ROT]
    return jnp.concatenate([first_half * cosine + second_half * sine_table, second_half * cosine - first_half * sine_table, vectors[..., ROT:]], axis=-1)

def masked_scores(query_head, key_head):
    score_scale = HEAD_DIM ** (-0.5)
    scores = jnp.dot(query_head, key_head.T, preferred_element_type=jnp.float32) * score_scale
    places = jnp.arange(LEN)
    allowed = places[:, None] >= places[None, :]
    return jnp.where(allowed, scores, -jnp.inf)

def head_forward(operands):
    query_head, key_head, value_head = operands
    scores = masked_scores(query_head, key_head)
    row_max = lax.optimization_barrier(jnp.max(scores, axis=-1, keepdims=True))
    row_total = lax.optimization_barrier(jnp.sum(jnp.exp(scores - row_max), axis=-1, keepdims=True))
    log_total = row_max + jnp.log(row_total)
    weights = jnp.exp(scores - log_total).astype(jnp.bfloat16)
    context = jnp.dot(weights, value_head, preferred_element_type=jnp.float32).astype(jnp.bfloat16)
    return (context, log_total[:, 0])

def head_backward(operands):
    query_head, key_head, value_head, context_head, grad_head, log_total = operands
    score_scale = HEAD_DIM ** (-0.5)
    scores = masked_scores(query_head, key_head)
    probs = jnp.exp(scores - log_total[:, None])
    value_grad = jnp.dot(probs.astype(jnp.bfloat16).T, grad_head, preferred_element_type=jnp.float32)
    prob_grad = jnp.dot(grad_head, value_head.T, preferred_element_type=jnp.float32)
    row_delta = lax.optimization_barrier(jnp.sum(grad_head.astype(jnp.float32) * context_head.astype(jnp.float32), axis=-1, keepdims=True))
    score_grad = (probs * (prob_grad - row_delta) * score_scale).astype(jnp.bfloat16)
    query_grad = jnp.dot(score_grad, key_head, preferred_element_type=jnp.float32)
    key_grad = jnp.dot(score_grad.T, query_head, preferred_element_type=jnp.float32)
    return (query_grad, key_grad, value_grad)

def one_sequence(seq_stream, seq_cotangent, norm_gain, norm_offset, attend_weight, attend_bias, output_weight, up_weight, up_bias, down_weight):
    row_mean = lax.optimization_barrier(jnp.mean(seq_stream, axis=-1, keepdims=True))
    centred = seq_stream - row_mean
    inverse_std = lax.rsqrt(lax.optimization_barrier(jnp.mean(centred * centred, axis=-1, keepdims=True)) + EPS)
    unit_rows = centred * inverse_std
    normed = (unit_rows * norm_gain + norm_offset).astype(jnp.bfloat16)
    flat_attend = attend_weight.reshape(D, 3 * D)
    projected = jnp.dot(normed, flat_attend, preferred_element_type=jnp.float32).reshape(LEN, 3, HEADS, HEAD_DIM) + attend_bias.reshape(3, HEADS, HEAD_DIM)
    cosine, sine_table = rotary_angles(jnp.arange(LEN))
    cosine = cosine[:, None, :]
    sine_table = sine_table[:, None, :]
    queries = rotate(projected[:, 0], cosine, sine_table).astype(jnp.bfloat16)
    keys_all = rotate(projected[:, 1], cosine, sine_table).astype(jnp.bfloat16)
    values_all = projected[:, 2].astype(jnp.bfloat16)
    query_heads = jnp.swapaxes(queries, 0, 1)
    key_heads = jnp.swapaxes(keys_all, 0, 1)
    value_heads = jnp.swapaxes(values_all, 0, 1)
    context_heads, total_heads = lax.map(head_forward, (query_heads, key_heads, value_heads))
    context = jnp.swapaxes(context_heads, 0, 1).reshape(LEN, D)
    up_pre = jnp.dot(normed, up_weight, preferred_element_type=jnp.float32) + up_bias
    up_value, up_slope = gelu_parts(up_pre)
    up_hidden = up_value.astype(jnp.bfloat16)
    branch_total = jnp.dot(context, output_weight, preferred_element_type=jnp.float32) + jnp.dot(up_hidden, down_weight, preferred_element_type=jnp.float32)
    result_rows = seq_stream + branch_total
    grad_rows = seq_cotangent.astype(jnp.bfloat16)
    final_grad = lax.optimization_barrier(jnp.sum(seq_cotangent, axis=0))
    output_grad = jnp.dot(context.T, grad_rows, preferred_element_type=jnp.float32)
    down_grad = jnp.dot(up_hidden.T, grad_rows, preferred_element_type=jnp.float32)
    context_grad = jnp.dot(grad_rows, output_weight.T, preferred_element_type=jnp.float32).astype(jnp.bfloat16)
    pre_grad = jnp.dot(grad_rows, down_weight.T, preferred_element_type=jnp.float32) * up_slope
    up_bias_grad = lax.optimization_barrier(jnp.sum(pre_grad, axis=0))
    pre_rounded = pre_grad.astype(jnp.bfloat16)
    grad_heads = jnp.swapaxes(context_grad.reshape(LEN, HEADS, HEAD_DIM), 0, 1)
    query_grad, key_grad, value_grad = lax.map(head_backward, (query_heads, key_heads, value_heads, context_heads, grad_heads, total_heads))
    query_pre = unrotate(jnp.swapaxes(query_grad, 0, 1), cosine, sine_table)
    key_pre = unrotate(jnp.swapaxes(key_grad, 0, 1), cosine, sine_table)
    proj_grad = jnp.stack([query_pre, key_pre, jnp.swapaxes(value_grad, 0, 1)], axis=1)
    attend_bias_grad = lax.optimization_barrier(jnp.sum(proj_grad, axis=0)).reshape(3, D)
    proj_rounded = proj_grad.reshape(LEN, 3 * D).astype(jnp.bfloat16)
    attend_grad = jnp.dot(normed.T, proj_rounded, preferred_element_type=jnp.float32).reshape(D, 3, D)
    up_grad = jnp.dot(normed.T, pre_rounded, preferred_element_type=jnp.float32)
    normed_grad = jnp.dot(proj_rounded, flat_attend.T, preferred_element_type=jnp.float32) + jnp.dot(pre_rounded, up_weight.T, preferred_element_type=jnp.float32)
    gain_grad = lax.optimization_barrier(jnp.sum(normed_grad * unit_rows, axis=0))
    offset_grad = lax.optimization_barrier(jnp.sum(normed_grad, axis=0))
    scaled = normed_grad * norm_gain
    stream_rows = seq_cotangent + inverse_std * (scaled - lax.optimization_barrier(jnp.mean(scaled, axis=-1, keepdims=True)) - unit_rows * lax.optimization_barrier(jnp.mean(scaled * unit_rows, axis=-1, keepdims=True)))
    gradients = (gain_grad, offset_grad, attend_grad, attend_bias_grad, output_grad, up_grad, up_bias_grad, down_grad, final_grad)
    return (result_rows, stream_rows, gradients)

def reference(stream, norm_gain, norm_offset, attend_weight, attend_bias, output_weight, up_weight, up_bias, down_weight, final_bias, cotangent):
    stream_seqs = jnp.swapaxes(stream, 0, 1)
    cotangent_seqs = jnp.swapaxes(cotangent, 0, 1)
    zero_grads = (jnp.zeros((D,), jnp.float32), jnp.zeros((D,), jnp.float32), jnp.zeros((D, 3, D), jnp.float32), jnp.zeros((3, D), jnp.float32), jnp.zeros((D, D), jnp.float32), jnp.zeros((D, FF), jnp.float32), jnp.zeros((FF,), jnp.float32), jnp.zeros((FF, D), jnp.float32), jnp.zeros((D,), jnp.float32))

    def seq_step(totals, seq_pair):
        result_rows, stream_rows, gradients = one_sequence(seq_pair[0], seq_pair[1], norm_gain, norm_offset, attend_weight, attend_bias, output_weight, up_weight, up_bias, down_weight)
        result_rows = result_rows + final_bias
        return (jax.tree.map(jnp.add, totals, gradients), (result_rows, stream_rows))
    totals, (result_seqs, grad_seqs) = lax.scan(seq_step, zero_grads, (stream_seqs, cotangent_seqs))
    return (jnp.swapaxes(result_seqs, 0, 1), jnp.swapaxes(grad_seqs, 0, 1), totals[0], totals[1], totals[2], totals[3], totals[4], totals[5], totals[6], totals[7], totals[8])
```

```python
import functools
import math

import jax
import jax.numpy as jnp
from jax import lax
from jax.experimental import pallas as pl
from jax.experimental.pallas import tpu as pltpu
from jax.sharding import PartitionSpec as P

HEAD_DIM = 64
ROT = 32

EPS = 1e-05
GELU_C = 0.7978845608028654
CUBIC = 0.044715
LOG_BASE = math.log(10000.0)
BF = jnp.bfloat16
F32 = jnp.float32


def gelu_parts(pre_act):
    inner_arg = GELU_C * (pre_act + CUBIC * pre_act * pre_act * pre_act)
    tanh_value = jnp.tanh(inner_arg)
    gelu_value = 0.5 * pre_act * (1.0 + tanh_value)
    gelu_slope = 0.5 * (1.0 + tanh_value) + 0.5 * pre_act * (
        1.0 - tanh_value * tanh_value
    ) * GELU_C * (1.0 + 3.0 * CUBIC * pre_act * pre_act)
    return (gelu_value, gelu_slope)


def rotary_tables(length, width):
    half_rot = ROT // 2
    frequency = jnp.exp(jnp.arange(half_rot, dtype=F32) * (-2.0 * LOG_BASE / ROT))
    angles = jnp.arange(length, dtype=jnp.int32).astype(F32)[:, None] * frequency[None, :]
    cosine, sine = jnp.cos(angles), jnp.sin(angles)
    zero = jnp.zeros_like(sine)
    rest = jnp.zeros((length, HEAD_DIM - ROT), F32)
    own = jnp.concatenate([cosine, cosine, rest + 1.0], axis=1)
    right = jnp.concatenate([-sine, zero, rest], axis=1)
    left = jnp.concatenate([zero, sine, rest], axis=1)
    reps = (1, width // HEAD_DIM)
    return jnp.tile(own, reps), jnp.tile(right, reps), jnp.tile(left, reps)


def dot(a, b, dims, out=F32):
    return lax.dot_general(a, b, ((dims[:1], dims[1:]), ((), ())), preferred_element_type=out)


def attention_body(
    width, q_ref, k_ref, v_ref, g_ref, bq_ref, bk_ref, bv_ref, own_ref, right_ref, left_ref,
    ctx_ref, dq_ref, dk_ref, dv_ref, bias_ref,
):
    length = own_ref.shape[0]
    half = ROT // 2
    own, right, left = own_ref[...], right_ref[...], left_ref[...]

    def flat(ref):
        return ref[...].reshape(length, width)

    def rotated(x):
        return (
            x * own
            + pltpu.roll(x, width - half, 1) * right
            + pltpu.roll(x, half, 1) * left
        )

    def unrotated(x):
        return (
            x * own
            - pltpu.roll(x, width - half, 1) * right
            - pltpu.roll(x, half, 1) * left
        )

    q_all = rotated(flat(q_ref) + bq_ref[...]).astype(BF)
    k_all = rotated(flat(k_ref) + bk_ref[...]).astype(BF)
    v_all = (flat(v_ref) + bv_ref[...]).astype(BF)
    g_all = flat(g_ref)
    scale = HEAD_DIM ** (-0.5)
    block = min(256, length)
    ctx_heads, dq_heads, dk_heads, dv_heads = [], [], [], []
    for head in range(width // HEAD_DIM):
        lanes = slice(head * HEAD_DIM, (head + 1) * HEAD_DIM)
        q, k, v, g = q_all[:, lanes], k_all[:, lanes], v_all[:, lanes], g_all[:, lanes]
        ctx_rows, dq_rows = [], []
        dk = dv = None
        for start in range(0, length, block):
            stop = start + block
            qb, gb = q[start:stop], g[start:stop]
            s = dot(qb, k[:stop], (1, 1)) * scale
            row = lax.broadcasted_iota(jnp.int32, s.shape, 0) + start
            col = lax.broadcasted_iota(jnp.int32, s.shape, 1)
            s = jnp.where(row >= col, s, -jnp.inf)
            m = jnp.max(s, axis=1, keepdims=True)
            p = jnp.exp(s - m)
            p = p * (1.0 / jnp.sum(p, axis=1, keepdims=True))
            pb = p.astype(BF)
            ctx = dot(pb, v[:stop], (1, 0)).astype(BF)
            delta = jnp.sum(gb.astype(F32) * ctx.astype(F32), axis=1, keepdims=True)
            dp = dot(gb, v[:stop], (1, 1))
            ds = (p * (dp - delta) * scale).astype(BF)
            ctx_rows.append(ctx)
            dq_rows.append(dot(ds, k[:stop], (1, 0)))
            dvb = dot(pb, gb, (0, 0))
            dkb = dot(ds, qb, (0, 0))
            if start == 0:
                dk, dv = dkb, dvb
            else:
                dk = jnp.concatenate([dk + dkb[:start], dkb[start:]], axis=0)
                dv = jnp.concatenate([dv + dvb[:start], dvb[start:]], axis=0)
        ctx_heads.append(jnp.concatenate(ctx_rows, axis=0))
        dq_heads.append(jnp.concatenate(dq_rows, axis=0))
        dk_heads.append(dk)
        dv_heads.append(dv)

    def joined(parts):
        return jnp.concatenate(parts, axis=1)

    dq = unrotated(joined(dq_heads))
    dk = unrotated(joined(dk_heads))
    dv = joined(dv_heads)
    ctx_ref[...] = joined(ctx_heads).reshape(ctx_ref.shape)
    for place, (ref, value) in enumerate(((dq_ref, dq), (dk_ref, dk), (dv_ref, dv))):
        ref[...] = value.astype(BF).reshape(ref.shape)
        bias_ref[0, place : place + 1, :] = jnp.sum(value, axis=0, keepdims=True)


def attention(projected, ctx_grad, bias, devices, seqs, rows):
    local = ctx_grad.shape[1]
    width = min(128, local)
    groups = local // width
    length = devices * rows
    own, right, left = rotary_tables(length, width)
    proj4 = projected.reshape(devices, seqs, rows, 3 * local)
    grad4 = ctx_grad.reshape(devices, seqs, rows, local)

    def spec(part):
        return pl.BlockSpec((devices, None, rows, width), lambda s, h: (0, s, 0, part * groups + h))

    def bias_spec(part):
        return pl.BlockSpec((1, width), lambda s, h: (0, part * groups + h))

    table = pl.BlockSpec((length, width), lambda s, h: (0, 0))
    out4 = jax.ShapeDtypeStruct((devices, seqs, rows, local), BF)
    flat_bias = bias.reshape(1, 3 * local)
    ctx, dq, dk, dv, bias_grad = pl.pallas_call(
        functools.partial(attention_body, width),
        grid=(seqs, groups),
        in_specs=[spec(0), spec(1), spec(2), spec(0), bias_spec(0), bias_spec(1), bias_spec(2), table, table, table],
        out_specs=[spec(0)] * 4 + [pl.BlockSpec((1, 3, width), lambda s, h: (s, 0, h))],
        out_shape=[out4] * 4 + [jax.ShapeDtypeStruct((seqs, 3, local), F32)],
        name="attention",
    )(proj4, proj4, proj4, grad4, flat_bias, flat_bias, flat_bias, own, right, left)
    tokens = devices * seqs * rows
    return (
        ctx.reshape(tokens, local),
        [dq.reshape(tokens, local), dk.reshape(tokens, local), dv.reshape(tokens, local)],
        jnp.sum(bias_grad, axis=0),
    )


def per_device(
    stream,
    norm_gain,
    norm_offset,
    attend_weight,
    attend_bias,
    output_weight,
    up_weight,
    up_bias,
    down_weight,
    final_bias,
    cotangent,
):
    rows, seqs, width = stream.shape
    local = attend_weight.shape[2]
    tp = lax.axis_size("tp")
    devices = lax.axis_size("seq") * tp
    block = tp * seqs * rows

    def by_sequence(value):
        return jnp.swapaxes(value, 0, 1).reshape(seqs * rows, width)

    def by_place(value):
        return jnp.swapaxes(value.reshape(seqs, rows, width), 0, 1)

    own_stream = by_sequence(stream)
    own_cot = by_sequence(cotangent)
    row_mean = jnp.mean(own_stream, axis=-1, keepdims=True)
    centred = own_stream - row_mean
    inverse_std = lax.rsqrt(jnp.mean(centred * centred, axis=-1, keepdims=True) + EPS)
    unit_rows = centred * inverse_std
    own_normed = (unit_rows * norm_gain + norm_offset).astype(BF)
    own_grad = own_cot.astype(BF)
    normed = lax.all_gather(own_normed, ("seq", "tp"), axis=0, tiled=True)
    grads = lax.all_gather(own_grad, ("seq", "tp"), axis=0, tiled=True)

    weights = jnp.swapaxes(attend_weight, 0, 1)
    projected = jnp.concatenate(
        [dot(normed, weights[i], (1, 0)) for i in range(3)], axis=1
    )
    up_pre = dot(normed, up_weight, (1, 0)) + up_bias
    up_value, up_slope = gelu_parts(up_pre)
    hidden = up_value.astype(BF)
    ctx_grad = dot(grads, output_weight, (1, 1)).astype(BF)
    pre_grad = dot(grads, down_weight, (1, 1)) * up_slope
    up_bias_grad = jnp.sum(pre_grad, axis=0)
    pre_rounded = pre_grad.astype(BF)
    context, proj_grads, attend_bias_grad = attention(
        projected, ctx_grad, attend_bias, devices, seqs, rows
    )
    start = lax.axis_index("seq") * block

    def own_block(value):
        return lax.dynamic_slice_in_dim(value, start, block, 0)

    summed = dot(own_block(context), output_weight, (1, 0)) + dot(
        own_block(hidden), down_weight, (1, 0)
    )
    branch_total = lax.psum_scatter(summed, "tp", scatter_dimension=0, tiled=True)
    result = by_place(own_stream + branch_total + final_bias)
    back = dot(own_block(pre_rounded), up_weight, (1, 1))
    for i in range(3):
        back = back + dot(own_block(proj_grads[i]), weights[i], (1, 1))
    normed_grad = lax.psum_scatter(back, "tp", scatter_dimension=0, tiled=True)

    output_grad = dot(context, grads, (0, 0))
    down_grad = dot(hidden, grads, (0, 0))
    up_grad = dot(normed, pre_rounded, (0, 0))
    attend_grad = jnp.swapaxes(
        jnp.stack([dot(normed, part, (0, 0)) for part in proj_grads]), 0, 1
    )

    scaled = normed_grad * norm_gain
    stream_grad = own_cot + inverse_std * (
        scaled
        - jnp.mean(scaled, axis=-1, keepdims=True)
        - unit_rows * jnp.mean(scaled * unit_rows, axis=-1, keepdims=True)
    )
    sums = jnp.stack(
        [
            jnp.sum(normed_grad * unit_rows, axis=0),
            jnp.sum(normed_grad, axis=0),
            jnp.sum(own_cot, axis=0),
        ]
    )
    sums = lax.psum(sums, ("seq", "tp"))
    return (
        result,
        by_place(stream_grad),
        sums[0],
        sums[1],
        attend_grad,
        attend_bias_grad,
        output_grad,
        up_grad,
        up_bias_grad,
        down_grad,
        sums[2],
    )


def solution(mesh):
    in_specs = (
        P(("seq", "tp"), None, None),
        P(),
        P(),
        P(None, None, "tp"),
        P(None, "tp"),
        P("tp", None),
        P(None, "tp"),
        P("tp"),
        P("tp", None),
        P(),
        P(("seq", "tp"), None, None),
    )
    out_specs = (
        P(("seq", "tp"), None, None),
        P(("seq", "tp"), None, None),
        P(),
        P(),
        P(None, None, "tp"),
        P(None, "tp"),
        P("tp", None),
        P(None, "tp"),
        P("tp"),
        P("tp", None),
        P(),
    )
    return jax.shard_map(
        per_device, mesh=mesh, in_specs=in_specs, out_specs=out_specs, check_vma=False
    )
```

```python
import functools
import math

import jax
import jax.numpy as jnp
from jax import lax
from jax.experimental import pallas as pl
from jax.experimental.pallas import tpu as pltpu
from jax.sharding import PartitionSpec as P

HEAD_DIM = 64
ROT = 32

EPS = 1e-05
GELU_C = 0.7978845608028654
CUBIC = 0.044715
LOG_BASE = math.log(10000.0)
BF = jnp.bfloat16
F32 = jnp.float32
MESH = pl.DeviceIdType.MESH


def gelu_parts(pre_act):
    inner_arg = GELU_C * (pre_act + CUBIC * pre_act * pre_act * pre_act)
    tanh_value = jnp.tanh(inner_arg)
    gelu_value = 0.5 * pre_act * (1.0 + tanh_value)
    gelu_slope = 0.5 * (1.0 + tanh_value) + 0.5 * pre_act * (
        1.0 - tanh_value * tanh_value
    ) * GELU_C * (1.0 + 3.0 * CUBIC * pre_act * pre_act)
    return (gelu_value, gelu_slope)


def dot(a, b, dims):
    return lax.dot_general(a, b, ((dims[:1], dims[1:]), ((), ())), preferred_element_type=F32)


def flip(index, bit):
    return index + bit - 2 * bit * ((index // bit) % 2)


def head_pass(q_all, k_all, v_all, g_all, heads):
    length = q_all.shape[0]
    scale = HEAD_DIM ** (-0.5)
    block = min(256, length)
    results = ([], [], [], [])
    for head in range(heads):
        lanes = slice(head * HEAD_DIM, (head + 1) * HEAD_DIM)
        q, k, v, g = q_all[:, lanes], k_all[:, lanes], v_all[:, lanes], g_all[:, lanes]
        ctx_rows, dq_rows = [], []
        dk = dv = None
        for start in range(0, length, block):
            stop = start + block
            qb, gb = q[start:stop], g[start:stop]
            s = dot(qb, k[:stop], (1, 1)) * scale
            row = lax.broadcasted_iota(jnp.int32, s.shape, 0) + start
            col = lax.broadcasted_iota(jnp.int32, s.shape, 1)
            s = jnp.where(row >= col, s, -jnp.inf)
            m = jnp.max(s, axis=1, keepdims=True)
            p = jnp.exp(s - m)
            p = p * (1.0 / jnp.sum(p, axis=1, keepdims=True))
            pb = p.astype(BF)
            ctx = dot(pb, v[:stop], (1, 0)).astype(BF)
            delta = jnp.sum(gb.astype(F32) * ctx.astype(F32), axis=1, keepdims=True)
            dp = dot(gb, v[:stop], (1, 1))
            ds = (p * (dp - delta) * scale).astype(BF)
            ctx_rows.append(ctx)
            dq_rows.append(dot(ds, k[:stop], (1, 0)))
            dvb = dot(pb, gb, (0, 0))
            dkb = dot(ds, qb, (0, 0))
            if start == 0:
                dk, dv = dkb, dvb
            else:
                dk = jnp.concatenate([dk + dkb[:start], dkb[start:]], axis=0)
                dv = jnp.concatenate([dv + dvb[:start], dvb[start:]], axis=0)
        results[0].append(jnp.concatenate(ctx_rows, axis=0))
        results[1].append(jnp.concatenate(dq_rows, axis=0))
        results[2].append(dk)
        results[3].append(dv)
    return [jnp.concatenate(parts, axis=1) for parts in results]


def block_kernel(
    dims,
    stream_ref, cot_ref, gain_ref, offset_ref, fbias_ref, abias_ref, ubias_ref,
    wa_hbm, wo_hbm, wu_hbm, wd_hbm,
    norm_out, grad_out, hid_out, pre_out, ctx_out, dproj_out,
    result_ref, sgrad_ref, sums_ref, abg_ref, ubg_ref,
    gat, wa, wo, wu, wd, unit, istd, table, proj, cgrad, hid, pre, ctx, dproj,
    part, parts_in, sum_tp, sum_seq,
    zs, zr, xs, xr, fs, fr, ps, pr, ms, mr, ws, os,
):
    Z, TP, S, R, D = dims
    z, t = lax.axis_index("seq"), lax.axis_index("tp")
    chip, core = t // 2, t % 2
    chips = TP // 2
    levels = chips.bit_length() - 1
    bits = [
        (1 - core) * (1 << i) + core * (1 << (levels - 1 - i)) for i in range(levels)
    ]
    partner = chip * 2 + 1 - core
    L = Z * TP * R
    local = wo.shape[0]
    hidden = wu.shape[1]
    pair = min(128, local)
    own_rows = TP * R

    loads = [
        pltpu.make_async_copy(src, dst, ws.at[i])
        for i, (src, dst) in enumerate(((wa_hbm, wa), (wo_hbm, wo), (wu_hbm, wu), (wd_hbm, wd)))
    ]
    for load in loads:
        load.start()
    barrier = pltpu.get_barrier_semaphore()
    for d in range(1, TP):
        pl.semaphore_signal(barrier, inc=1, device_id={"tp": (t + d) % TP}, device_id_type=MESH)
    for d in range(1, Z):
        pl.semaphore_signal(barrier, inc=1, device_id={"seq": (z + d) % Z}, device_id_type=MESH)

    @pl.loop(0, S)
    def _(s):
        x = stream_ref[:, pl.ds(s, 1), :].reshape(R, D)
        mean = jnp.mean(x, axis=-1, keepdims=True)
        centred = x - mean
        inv = lax.rsqrt(jnp.mean(centred * centred, axis=-1, keepdims=True) + EPS)
        u = centred * inv
        unit[s] = u
        istd[s] = jnp.broadcast_to(inv, (R, 128))
        gat[0, s, z, t] = (u * gain_ref[...] + offset_ref[...]).astype(BF)
        gat[1, s, z, t] = cot_ref[:, pl.ds(s, 1), :].reshape(R, D).astype(BF)

    pl.semaphore_wait(barrier, TP + Z - 2)

    def remote(src, dst, ssem, rsem, dev):
        return pltpu.make_async_remote_copy(
            src_ref=src, dst_ref=dst, send_sem=ssem, recv_sem=rsem,
            device_id=dev, device_id_type=MESH,
        )

    def same(ref, ssem, rsem, dev):
        return remote(ref, ref, ssem, rsem, dev)

    def unit_of(s, zz, tt):
        return gat.at[:, s, zz, tt]

    def column(s, tt):
        return gat.at[:, s, :, tt]

    here = {"tp": t}

    def z_copy(s, d):
        return same(unit_of(s, z, t), zs.at[s, d], zr.at[s, z], {"seq": (z + d) % Z})

    def z_sends(s):
        for d in range(1, Z):
            z_copy(s, d).start()

    def x_copy(s, d, i):
        return same(
            unit_of(s, (z + d) % Z, t), xs.at[s, i, d],
            xr.at[s, t, 0 if d == 0 else 1], {"tp": flip(chip, bits[i]) * 2 + core},
        )

    def f_copy(s, src, slot, to):
        return same(column(s, src), fs.at[s, slot], fr.at[s, src], {"tp": to})

    def source(r):
        c = chip
        for i in range(levels):
            if (r >> i) & 1:
                c = flip(c, bits[i])
        return c * 2 + core

    order = sorted(range(1, chips), key=lambda r: (bin(r).count("1"), r))

    def top(r):
        return max(i for i in range(levels) if (r >> i) & 1)

    def slot_of(r, i):
        return r * (levels + 1) + i

    def own_sends(s):
        for i in range(levels):
            x_copy(s, 0, i).start()

    def z_step(s):
        for d in range(1, Z):
            zz = (z + d) % Z
            same(unit_of(s, zz, t), zs.at[s, 0], zr.at[s, zz], here).wait_recv()
        for d in range(1, Z):
            for i in range(levels):
                x_copy(s, d, i).start()
        f_copy(s, t, slot_of(0, 0), partner).start()

    def f_step(s, level):
        for r in order:
            if bin(r).count("1") != level:
                continue
            src = source(r)
            if level == 1:
                same(unit_of(s, z, src), zs.at[s, 0], xr.at[s, src, 0], here).wait_recv()
                same(
                    gat.at[:, s, pl.ds(0, Z - 1), src], zs.at[s, 0], xr.at[s, src, 1], here
                ).wait_recv()
            else:
                same(column(s, src), zs.at[s, 0], fr.at[s, src], here).wait_recv()
            for i in range(top(r) + 1, levels):
                f_copy(s, src, slot_of(r, i + 1), flip(chip, bits[i]) * 2 + core).start()
            f_copy(s, src, slot_of(r, 0), partner).start()

    def end_step(s):
        for c in range(chips):
            src = ((chip + c) % chips) * 2 + 1 - core
            same(column(s, src), zs.at[s, 0], fr.at[s, src], here).wait_recv()

    def upper_steps(s):
        for level in range(2, levels + 1):
            f_step(s, level)

    def drain_gather(s):
        for d in range(1, Z):
            z_copy(s, d).wait_send()
        for d in range(Z):
            for i in range(levels):
                x_copy(s, d, i).wait_send()
        f_copy(s, t, slot_of(0, 0), partner).wait_send()
        for r in order:
            src = source(r)
            for i in range(top(r) + 1, levels):
                f_copy(s, src, slot_of(r, i + 1), flip(chip, bits[i]) * 2 + core).wait_send()
            f_copy(s, src, slot_of(r, 0), partner).wait_send()

    def p_copy(kind, s, d):
        to = (t + d) % TP
        return remote(
            part.at[kind, s, to], parts_in.at[kind, s, t], ps.at[kind, s, d], pr.at[kind, s],
            {"tp": to},
        )

    def out_copies(s):
        return [
            pltpu.make_async_copy(src, dst, os.at[i])
            for i, (src, dst) in enumerate((
                (gat.at[0, s], norm_out.at[s]), (gat.at[1, s], grad_out.at[s]),
                (hid, hid_out.at[s]), (pre, pre_out.at[s]), (ctx, ctx_out.at[s]),
                (dproj, dproj_out.at[:, s]),
            ))
        ]

    @pl.loop(0, S)
    def _(s):
        z_sends(s)

    own_sends(0)
    if S > 1:
        own_sends(1)

    lane = lax.broadcasted_iota(jnp.int32, (L, pair), 1) % HEAD_DIM
    place = lax.broadcasted_iota(jnp.int32, (L, pair), 0).astype(F32)
    half = ROT // 2
    freq = jnp.exp((lane % half).astype(F32) * (-2.0 * LOG_BASE / ROT))
    angle = place * freq
    cosine, sine = jnp.cos(angle), jnp.sin(angle)
    table[0] = jnp.where(lane < ROT, cosine, 1.0)
    table[1] = jnp.where(lane < half, -sine, 0.0)
    table[2] = jnp.where((lane >= half) & (lane < ROT), sine, 0.0)
    abg_ref[...] = jnp.zeros_like(abg_ref)
    ubg_ref[...] = jnp.zeros_like(ubg_ref)
    for load in loads:
        load.wait()

    z_step(0)
    f_step(0, 1)
    if S > 1:
        z_step(1)
    upper_steps(0)
    end_step(0)

    def turned(x, sign):
        return (
            x * table[0]
            + sign * pltpu.roll(x, pair - half, 1) * table[1]
            + sign * pltpu.roll(x, half, 1) * table[2]
        )

    @pl.loop(0, S)
    def _(s):
        rows_n = gat[0, s].reshape(L, D)
        rows_g = gat[1, s].reshape(L, D)

        @pl.when(s > 0)
        def _():
            for copy in out_copies(s - 1):
                copy.wait()

        @pl.when(s + 2 < S)
        def _():
            own_sends(s + 2)

        @pl.loop(0, 3)
        def _(j):
            proj[j] = dot(rows_n, wa[j], (1, 0)) + abias_ref[j]

        cgrad[...] = dot(rows_g, wo[...], (1, 1)).astype(BF)

        @pl.when(s + 1 < S)
        def _():
            f_step(s + 1, 1)

        @pl.loop(0, local // pair)
        def _(h):
            lanes = pl.ds(pl.multiple_of(h * pair, pair), pair)
            q = turned(proj[0, :, lanes], 1.0).astype(BF)
            k = turned(proj[1, :, lanes], 1.0).astype(BF)
            v = proj[2, :, lanes].astype(BF)
            c, dq, dk, dv = head_pass(q, k, v, cgrad[:, lanes], pair // HEAD_DIM)
            ctx[:, lanes] = c
            for j, value in enumerate((turned(dq, -1.0), turned(dk, -1.0), dv)):
                dproj[j, :, lanes] = value.astype(BF)
                abg_ref[j : j + 1, lanes] += jnp.sum(value, axis=0, keepdims=True)

        @pl.when(s + 2 < S)
        def _():
            z_step(s + 2)

        @pl.when(s + 1 < S)
        def _():
            upper_steps(s + 1)

        tile = min(256, hidden)

        @pl.loop(0, hidden // tile)
        def _(n):
            cols = pl.ds(pl.multiple_of(n * tile, tile), tile)
            value, slope = gelu_parts(dot(rows_n, wu[:, cols], (1, 0)) + ubias_ref[:, cols])
            hid[:, cols] = value.astype(BF)
            grad = dot(rows_g, wd[cols, :], (1, 1)) * slope
            pre[:, cols] = grad.astype(BF)
            ubg_ref[:, cols] += jnp.sum(grad, axis=0, keepdims=True)

        for copy in out_copies(s):
            copy.start()

        mine = pl.ds(pl.multiple_of(z * own_rows, own_rows), own_rows)

        @pl.loop(0, D // 256)
        def _(n):
            cols = pl.ds(pl.multiple_of(n * 256, 256), 256)
            out = dot(ctx[mine, :], wo[:, cols], (1, 0)) + dot(hid[mine, :], wd[:, cols], (1, 0))
            back = dot(pre[mine, :], wu[cols, :], (1, 1))
            for j in range(3):
                back = back + dot(dproj[j, mine, :], wa[j, cols, :], (1, 1))
            part[0, s, :, :, cols] = out.astype(BF).reshape(TP, R, 256)
            part[1, s, :, :, cols] = back.astype(BF).reshape(TP, R, 256)

        for kind in range(2):
            for d in range(1, TP):
                p_copy(kind, s, d).start()

        @pl.when(s + 1 < S)
        def _():
            end_step(s + 1)

    sum_tp[t] = jnp.zeros_like(sum_tp[t])

    @pl.loop(0, S)
    def _(s):
        totals = []
        for kind in range(2):
            remote(
                part.at[kind, s, pl.ds(0, TP - 1)], parts_in.at[kind, s, pl.ds(0, TP - 1)],
                ps.at[kind, s, 0], pr.at[kind, s], here,
            ).wait_recv()
            total = part[kind, s, t].astype(F32)
            for d in range(1, TP):
                total = total + parts_in[kind, s, (t + d) % TP].astype(F32)
            totals.append(total)
        branch, ngrad = totals
        x = stream_ref[:, pl.ds(s, 1), :].reshape(R, D)
        cot = cot_ref[:, pl.ds(s, 1), :].reshape(R, D)
        result_ref[:, pl.ds(s, 1), :] = (x + branch + fbias_ref[...]).reshape(R, 1, D)
        u = unit[s]
        scaled = ngrad * gain_ref[...]
        sgrad_ref[:, pl.ds(s, 1), :] = (
            cot
            + istd[s][:, :1]
            * (
                scaled
                - jnp.mean(scaled, axis=-1, keepdims=True)
                - u * jnp.mean(scaled * u, axis=-1, keepdims=True)
            )
        ).reshape(R, 1, D)
        for i, value in enumerate((ngrad * u, ngrad, cot)):
            sum_tp[t, i : i + 1, :] += jnp.sum(value, axis=0, keepdims=True)

    def m_copy(d):
        return remote(sum_tp.at[t], sum_tp.at[t], ms.at[d], mr.at[0], {"tp": (t + d) % TP})

    def n_copy(d):
        return remote(
            sum_seq.at[z], sum_seq.at[z], ms.at[TP + d], mr.at[1], {"seq": (z + d) % Z}
        )

    for d in range(1, TP):
        m_copy(d).start()
    same(sum_tp.at[pl.ds(0, TP - 1)], ms.at[0], mr.at[0], here).wait_recv()
    total = sum_tp[0]
    for d in range(1, TP):
        total = total + sum_tp[d]
    sum_seq[z] = total
    for d in range(1, Z):
        n_copy(d).start()
    same(sum_seq.at[pl.ds(0, Z - 1)], ms.at[0], mr.at[1], here).wait_recv()
    total = sum_seq[0]
    for d in range(1, Z):
        total = total + sum_seq[d]
    sums_ref[...] = total

    for d in range(1, TP):
        m_copy(d).wait_send()
    for d in range(1, Z):
        n_copy(d).wait_send()
    for copy in out_copies(S - 1):
        copy.wait()

    @pl.loop(0, S)
    def _(s):
        drain_gather(s)
        for kind in range(2):
            for d in range(1, TP):
                p_copy(kind, s, d).wait_send()


def block_call(stream, cotangent, gain, offset, fbias, abias, ubias, wa, wo, wu, wd, Z, TP):
    R, S, D = stream.shape
    local, hidden = wo.shape[0], wu.shape[1]
    L = Z * TP * R
    chips = TP // 2
    levels = chips.bit_length() - 1
    vm = pl.BlockSpec(memory_space=pltpu.VMEM)
    anywhere = pl.BlockSpec(memory_space=pl.ANY)
    shape = jax.ShapeDtypeStruct
    dma = pltpu.SemaphoreType.DMA
    return pl.pallas_call(
        functools.partial(block_kernel, (Z, TP, S, R, D)),
        in_specs=[vm] * 7 + [anywhere] * 4,
        out_specs=[anywhere] * 6 + [vm] * 5,
        out_shape=[
            shape((S, Z, TP, R, D), BF),
            shape((S, Z, TP, R, D), BF),
            shape((S, L, hidden), BF),
            shape((S, L, hidden), BF),
            shape((S, L, local), BF),
            shape((3, S, L, local), BF),
            shape((R, S, D), F32),
            shape((R, S, D), F32),
            shape((8, D), F32),
            shape((3, local), F32),
            shape((1, hidden), F32),
        ],
        scratch_shapes=[
            pltpu.VMEM((2, S, Z, TP, R, D), BF),
            pltpu.VMEM((3, D, local), BF),
            pltpu.VMEM((local, D), BF),
            pltpu.VMEM((D, hidden), BF),
            pltpu.VMEM((hidden, D), BF),
            pltpu.VMEM((S, R, D), F32),
            pltpu.VMEM((S, R, 128), F32),
            pltpu.VMEM((3, L, min(128, local)), F32),
            pltpu.VMEM((3, L, local), F32),
            pltpu.VMEM((L, local), BF),
            pltpu.VMEM((L, hidden), BF),
            pltpu.VMEM((L, hidden), BF),
            pltpu.VMEM((L, local), BF),
            pltpu.VMEM((3, L, local), BF),
            pltpu.VMEM((2, S, TP, R, D), BF),
            pltpu.VMEM((2, S, TP, R, D), BF),
            pltpu.VMEM((TP, 8, D), F32),
            pltpu.VMEM((Z, 8, D), F32),
            dma((S, Z)),
            dma((S, Z)),
            dma((S, levels, Z)),
            dma((S, TP, 2)),
            dma((S, chips * (levels + 1))),
            dma((S, TP)),
            dma((2, S, TP)),
            dma((2, S)),
            dma((TP + Z,)),
            dma((2,)),
            dma((4,)),
            dma((6,)),
        ],
        compiler_params=pltpu.CompilerParams(
            collective_id=0, has_side_effects=True, vmem_limit_bytes=67000000
        ),
        name="block",
    )(stream, cotangent, gain, offset, fbias, abias, ubias, wa, wo, wu, wd)


def per_device(
    stream,
    norm_gain,
    norm_offset,
    attend_weight,
    attend_bias,
    output_weight,
    up_weight,
    up_bias,
    down_weight,
    final_bias,
    cotangent,
):
    R, S, D = stream.shape
    local = attend_weight.shape[2]
    hidden = up_weight.shape[1]
    TP, Z = lax.axis_size("tp"), lax.axis_size("seq")
    tokens = R * S * TP * Z
    weights = jnp.swapaxes(attend_weight, 0, 1)
    (
        normed, grads, hid, pre, ctx, dproj, result, stream_grad, sums, abias_grad, ubias_grad
    ) = block_call(
        stream, cotangent, norm_gain.reshape(1, D), norm_offset.reshape(1, D),
        final_bias.reshape(1, D), attend_bias.reshape(3, 1, local), up_bias.reshape(1, hidden),
        weights, output_weight, up_weight, down_weight, Z, TP,
    )
    normed = normed.reshape(tokens, D)
    grads = grads.reshape(tokens, D)
    output_grad = dot(ctx.reshape(tokens, local), grads, (0, 0))
    down_grad = dot(hid.reshape(tokens, hidden), grads, (0, 0))
    up_grad = dot(normed, pre.reshape(tokens, hidden), (0, 0))
    attend_grad = jnp.swapaxes(
        jnp.stack([dot(normed, dproj[j].reshape(tokens, local), (0, 0)) for j in range(3)]), 0, 1
    )
    return (
        result,
        stream_grad,
        sums[0],
        sums[1],
        attend_grad,
        abias_grad,
        output_grad,
        up_grad,
        ubias_grad.reshape(hidden),
        down_grad,
        sums[2],
    )


def solution(mesh):
    in_specs = (
        P(("seq", "tp"), None, None),
        P(),
        P(),
        P(None, None, "tp"),
        P(None, "tp"),
        P("tp", None),
        P(None, "tp"),
        P("tp"),
        P("tp", None),
        P(),
        P(("seq", "tp"), None, None),
    )
    out_specs = (
        P(("seq", "tp"), None, None),
        P(("seq", "tp"), None, None),
        P(),
        P(),
        P(None, None, "tp"),
        P(None, "tp"),
        P("tp", None),
        P(None, "tp"),
        P("tp"),
        P("tp", None),
        P(),
    )
    return jax.shard_map(
        per_device, mesh=mesh, in_specs=in_specs, out_specs=out_specs, check_vma=False
    )
```

```python
import functools
import math

import jax
import jax.numpy as jnp
from jax import lax
from jax.experimental import pallas as pl
from jax.experimental.pallas import tpu as pltpu
from jax.sharding import PartitionSpec as P

HEAD_DIM = 64
ROT = 32

EPS = 1e-05
GELU_C = 0.7978845608028654
CUBIC = 0.044715
LOG_BASE = math.log(10000.0)
BF = jnp.bfloat16
F32 = jnp.float32
MESH = pl.DeviceIdType.MESH


def gelu_parts(pre_act):
    inner_arg = GELU_C * (pre_act + CUBIC * pre_act * pre_act * pre_act)
    tanh_value = jnp.tanh(inner_arg)
    gelu_value = 0.5 * pre_act * (1.0 + tanh_value)
    gelu_slope = 0.5 * (1.0 + tanh_value) + 0.5 * pre_act * (
        1.0 - tanh_value * tanh_value
    ) * GELU_C * (1.0 + 3.0 * CUBIC * pre_act * pre_act)
    return (gelu_value, gelu_slope)


def dot(a, b, dims):
    return lax.dot_general(a, b, ((dims[:1], dims[1:]), ((), ())), preferred_element_type=F32)


def flip(index, bit):
    return index + bit - 2 * bit * ((index // bit) % 2)


def flip_all(index, mask):
    bit = 1
    while bit <= mask:
        if mask & bit:
            index = flip(index, bit)
        bit *= 2
    return index


def head_pass(q_all, k_all, v_all, g_all, heads):
    length = q_all.shape[0]
    scale = HEAD_DIM ** (-0.5)
    block = min(256, length)
    results = ([], [], [], [])
    for head in range(heads):
        lanes = slice(head * HEAD_DIM, (head + 1) * HEAD_DIM)
        q, k, v, g = q_all[:, lanes], k_all[:, lanes], v_all[:, lanes], g_all[:, lanes]
        ctx_rows, dq_rows = [], []
        dk = dv = None
        for start in range(0, length, block):
            stop = start + block
            qb, gb = q[start:stop], g[start:stop]
            s = dot(qb, k[:stop], (1, 1)) * scale
            row = lax.broadcasted_iota(jnp.int32, s.shape, 0) + start
            col = lax.broadcasted_iota(jnp.int32, s.shape, 1)
            s = jnp.where(row >= col, s, -jnp.inf)
            m = jnp.max(s, axis=1, keepdims=True)
            p = jnp.exp(s - m)
            p = p * (1.0 / jnp.sum(p, axis=1, keepdims=True))
            pb = p.astype(BF)
            ctx = dot(pb, v[:stop], (1, 0)).astype(BF)
            delta = jnp.sum(gb.astype(F32) * ctx.astype(F32), axis=1, keepdims=True)
            dp = dot(gb, v[:stop], (1, 1))
            ds = (p * (dp - delta) * scale).astype(BF)
            ctx_rows.append(ctx)
            dq_rows.append(dot(ds, k[:stop], (1, 0)))
            dvb = dot(pb, gb, (0, 0))
            dkb = dot(ds, qb, (0, 0))
            if start == 0:
                dk, dv = dkb, dvb
            else:
                dk = jnp.concatenate([dk + dkb[:start], dkb[start:]], axis=0)
                dv = jnp.concatenate([dv + dvb[:start], dvb[start:]], axis=0)
        results[0].append(jnp.concatenate(ctx_rows, axis=0))
        results[1].append(jnp.concatenate(dq_rows, axis=0))
        results[2].append(dk)
        results[3].append(dv)
    return [jnp.concatenate(parts, axis=1) for parts in results]


def block_kernel(
    dims,
    stream_ref, cot_ref, gain_ref, offset_ref, fbias_ref, abias_ref, ubias_ref,
    wa_hbm, wo_hbm, wu_hbm, wd_hbm,
    norm_out, grad_out, hid_out, pre_out, ctx_out, dproj_out,
    result_ref, sgrad_ref, sums_ref, abg_ref, ubg_ref,
    gat, wa, wo, wu, wd, unit, istd, table, proj, cgrad, hid, pre, ctx, dproj,
    part, half_in, parts_in, sum_tp, sum_seq,
    zs, zr, xs, xr, fs, fr, ps, hr, pr, ms, mr, ws, os,
):
    Z, TP, S, R, D = dims
    z, t = lax.axis_index("seq"), lax.axis_index("tp")
    chip, core = t // 2, t % 2
    chips = TP // 2
    levels = chips.bit_length() - 1
    bits = [
        (1 - core) * (1 << i) + core * (1 << (levels - 1 - i)) for i in range(levels)
    ]
    partner = chip * 2 + 1 - core
    L = Z * TP * R
    local = wo.shape[0]
    hidden = wu.shape[1]
    pair = min(128, local)
    own_rows = TP * R

    loads = [
        pltpu.make_async_copy(src, dst, ws.at[i])
        for i, (src, dst) in enumerate(((wa_hbm, wa), (wo_hbm, wo), (wu_hbm, wu), (wd_hbm, wd)))
    ]
    for load in loads:
        load.start()
    barrier = pltpu.get_barrier_semaphore()
    for d in range(1, TP):
        pl.semaphore_signal(barrier, inc=1, device_id={"tp": (t + d) % TP}, device_id_type=MESH)
    for d in range(1, Z):
        pl.semaphore_signal(barrier, inc=1, device_id={"seq": (z + d) % Z}, device_id_type=MESH)

    @pl.loop(0, S)
    def _(s):
        x = stream_ref[:, pl.ds(s, 1), :].reshape(R, D)
        mean = jnp.mean(x, axis=-1, keepdims=True)
        centred = x - mean
        inv = lax.rsqrt(jnp.mean(centred * centred, axis=-1, keepdims=True) + EPS)
        u = centred * inv
        unit[s] = u
        istd[s] = jnp.broadcast_to(inv, (R, 128))
        gat[0, s, z, t] = (u * gain_ref[...] + offset_ref[...]).astype(BF)
        gat[1, s, z, t] = cot_ref[:, pl.ds(s, 1), :].reshape(R, D).astype(BF)

    pl.semaphore_wait(barrier, TP + Z - 2)

    def remote(src, dst, ssem, rsem, dev):
        return pltpu.make_async_remote_copy(
            src_ref=src, dst_ref=dst, send_sem=ssem, recv_sem=rsem,
            device_id=dev, device_id_type=MESH,
        )

    def same(ref, ssem, rsem, dev):
        return remote(ref, ref, ssem, rsem, dev)

    def unit_of(s, zz, tt):
        return gat.at[:, s, zz, tt]

    def column(s, tt):
        return gat.at[:, s, :, tt]

    here = {"tp": t}
    other = [z] + [flip_all(z, r) if Z & (Z - 1) == 0 else (z + r) % Z for r in range(1, Z)]
    sender = [z] + [flip_all(z, r) if Z & (Z - 1) == 0 else (z + Z - r) % Z for r in range(1, Z)]

    def z_copy(s, r):
        return same(unit_of(s, z, t), zs.at[s, r], zr.at[s, z], {"seq": other[r]})

    def z_sends(s):
        for r in range(1, Z):
            z_copy(s, r).start()

    def x_copy(s, r, src, slot, i):
        return same(
            unit_of(s, sender[r], src), xs.at[s, slot, r], xr.at[s, src, sender[r]],
            {"tp": flip(chip, bits[i]) * 2 + core},
        )

    def f_copy(s, src, r):
        return same(column(s, src), fs.at[s, r], fr.at[s, src], {"tp": partner})

    def source(mask):
        c = chip
        for i in range(levels):
            if (mask >> i) & 1:
                c = flip(c, bits[i])
        return c * 2 + core

    order = sorted(range(1, chips), key=lambda m: (bin(m).count("1"), m))

    def later(mask):
        first = mask.bit_length()
        return [(mask * levels + i, i) for i in range(first, levels)]

    def own_unit(s, r):
        if r > 0:
            zz = sender[r]
            same(unit_of(s, zz, t), zs.at[s, 0], zr.at[s, zz], here).wait_recv()
        for slot, i in later(0):
            x_copy(s, r, t, slot, i).start()
        if r == Z - 1:
            f_copy(s, t, 0).start()

    def pass_unit(s, r, level):
        for mask in order:
            if bin(mask).count("1") != level:
                continue
            src = source(mask)
            same(unit_of(s, sender[r], src), zs.at[s, 0], xr.at[s, src, sender[r]], here).wait_recv()
            for slot, i in later(mask):
                x_copy(s, r, src, slot, i).start()
            if r == Z - 1:
                f_copy(s, src, mask).start()

    def z_step(s):
        for r in range(1, Z):
            own_unit(s, r)

    def f_step(s, level):
        for r in range(Z):
            pass_unit(s, r, level)

    def end_step(s):
        for c in range(chips):
            src = ((chip + c) % chips) * 2 + 1 - core
            same(column(s, src), zs.at[s, 0], fr.at[s, src], here).wait_recv()

    def upper_steps(s):
        for level in range(2, levels + 1):
            f_step(s, level)

    def drain_gather(s):
        for r in range(1, Z):
            z_copy(s, r).wait_send()
        for mask in [0] + order:
            src = source(mask)
            for slot, i in later(mask):
                for r in range(Z):
                    x_copy(s, r, src, slot, i).wait_send()
            f_copy(s, src, mask).wait_send()

    def half_copy(kind, s):
        return remote(
            part.at[kind, s, :, 1 - core], half_in.at[kind, s], ps.at[kind, s, 0], hr.at[kind, s],
            {"tp": partner},
        )

    def p_copy(kind, s, d):
        to = (chip + d) % chips
        return remote(
            part.at[kind, s, to, core], parts_in.at[kind, s, chip], ps.at[kind, s, d],
            pr.at[kind, s], {"tp": to * 2 + core},
        )

    def half_sends(s):
        for kind in range(2):
            half_copy(kind, s).start()

    def p_sends(s):
        for kind in range(2):
            half_copy(kind, s).wait_recv()
            for d in range(chips):
                c = (chip + d) % chips
                part[kind, s, c, core] = (
                    part[kind, s, c, core].astype(F32) + half_in[kind, s, c].astype(F32)
                ).astype(BF)
            for d in range(1, chips):
                p_copy(kind, s, d).start()

    def out_copies(s):
        return [
            pltpu.make_async_copy(src, dst, os.at[i])
            for i, (src, dst) in enumerate((
                (gat.at[0, s], norm_out.at[s]), (gat.at[1, s], grad_out.at[s]),
                (hid, hid_out.at[s]), (pre, pre_out.at[s]), (ctx, ctx_out.at[s]),
                (dproj, dproj_out.at[:, s]),
            ))
        ]

    z_sends(0)
    own_unit(0, 0)

    lane = lax.broadcasted_iota(jnp.int32, (L, pair), 1) % HEAD_DIM
    place = lax.broadcasted_iota(jnp.int32, (L, pair), 0).astype(F32)
    half = ROT // 2
    freq = jnp.exp((lane % half).astype(F32) * (-2.0 * LOG_BASE / ROT))
    angle = place * freq
    cosine, sine = jnp.cos(angle), jnp.sin(angle)
    table[0] = jnp.where(lane < ROT, cosine, 1.0)
    table[1] = jnp.where(lane < half, -sine, 0.0)
    table[2] = jnp.where((lane >= half) & (lane < ROT), sine, 0.0)
    abg_ref[...] = jnp.zeros_like(abg_ref)
    ubg_ref[...] = jnp.zeros_like(ubg_ref)
    for load in loads:
        load.wait()

    for r in range(1, Z + 3):
        if r < Z:
            own_unit(0, r)
        if r == Z // 2 and S > 1:
            z_sends(1)
            own_unit(1, 0)
        if 1 <= r <= Z:
            pass_unit(0, r - 1, 1)
        for level in range(2, levels + 1):
            if 0 <= r - level < Z:
                pass_unit(0, r - level, level)
    end_step(0)

    @pl.loop(2, S)
    def _(s):
        z_sends(s)
        own_unit(s, 0)

    def turned(x, sign):
        return (
            x * table[0]
            + sign * pltpu.roll(x, pair - half, 1) * table[1]
            + sign * pltpu.roll(x, half, 1) * table[2]
        )

    @pl.loop(0, S)
    def _(s):
        def rows_n():
            return gat[0, s].reshape(L, D)

        def rows_g():
            return gat[1, s].reshape(L, D)

        @pl.when(s > 0)
        def _():
            for copy in out_copies(s - 1):
                copy.wait()

        @pl.loop(0, 3)
        def _(j):
            proj[j] = dot(rows_n(), wa[j], (1, 0)) + abias_ref[j]

        cgrad[...] = dot(rows_g(), wo[...], (1, 1)).astype(BF)

        @pl.when((s == 0) & (s + 1 < S))
        def _():
            z_step(s + 1)

        @pl.when(s > 0)
        def _():
            p_sends(s - 1)

        @pl.loop(0, local // pair)
        def _(h):
            lanes = pl.ds(pl.multiple_of(h * pair, pair), pair)
            q = turned(proj[0, :, lanes], 1.0).astype(BF)
            k = turned(proj[1, :, lanes], 1.0).astype(BF)
            v = proj[2, :, lanes].astype(BF)
            c, dq, dk, dv = head_pass(q, k, v, cgrad[:, lanes], pair // HEAD_DIM)
            ctx[:, lanes] = c
            for j, value in enumerate((turned(dq, -1.0), turned(dk, -1.0), dv)):
                dproj[j, :, lanes] = value.astype(BF)
                abg_ref[j : j + 1, lanes] += jnp.sum(value, axis=0, keepdims=True)

            @pl.when((h == 0) & (s > 0) & (s + 1 < S))
            def _():
                f_step(s + 1, 1)

        tile = min(256, hidden)
        middle = hidden // tile // 2

        def feed_forward(n):
            cols = pl.ds(pl.multiple_of(n * tile, tile), tile)
            value, slope = gelu_parts(dot(rows_n(), wu[:, cols], (1, 0)) + ubias_ref[:, cols])
            hid[:, cols] = value.astype(BF)
            grad = dot(rows_g(), wd[cols, :], (1, 1)) * slope
            pre[:, cols] = grad.astype(BF)
            ubg_ref[:, cols] += jnp.sum(grad, axis=0, keepdims=True)

        @pl.loop(0, hidden // tile)
        def _(n):
            feed_forward(n)

            @pl.when((n == middle) & (s > 0) & (s + 1 < S))
            def _():
                upper_steps(s + 1)

            @pl.when((n == middle) & (s == 0) & (s + 1 < S))
            def _():
                f_step(s + 1, 1)

        @pl.when(s + 2 < S)
        def _():
            z_step(s + 2)

        for copy in out_copies(s):
            copy.start()

        mine = pl.ds(pl.multiple_of(z * own_rows, own_rows), own_rows)

        @pl.loop(0, D // 256)
        def _(n):
            cols = pl.ds(pl.multiple_of(n * 256, 256), 256)
            out = dot(ctx[mine, :], wo[:, cols], (1, 0)) + dot(hid[mine, :], wd[:, cols], (1, 0))
            back = dot(pre[mine, :], wu[cols, :], (1, 1))
            for j in range(3):
                back = back + dot(dproj[j, mine, :], wa[j, cols, :], (1, 1))
            part[0, s, :, :, :, cols] = out.astype(BF).reshape(chips, 2, R, 256)
            part[1, s, :, :, :, cols] = back.astype(BF).reshape(chips, 2, R, 256)

        half_sends(s)

        @pl.when((s == 0) & (s + 1 < S))
        def _():
            upper_steps(s + 1)

        @pl.when(s + 1 < S)
        def _():
            end_step(s + 1)

    p_sends(S - 1)
    sum_tp[t] = jnp.zeros_like(sum_tp[t])

    @pl.loop(0, S)
    def _(s):
        totals = []
        for kind in range(2):
            incoming = parts_in.at[kind, s, pl.ds(0, chips - 1)]
            remote(incoming, incoming, ps.at[kind, s, 0], pr.at[kind, s], here).wait_recv()
            total = part[kind, s, chip, core].astype(F32)
            for d in range(1, chips):
                total = total + parts_in[kind, s, (chip + d) % chips].astype(F32)
            totals.append(total)
        branch, ngrad = totals
        x = stream_ref[:, pl.ds(s, 1), :].reshape(R, D)
        cot = cot_ref[:, pl.ds(s, 1), :].reshape(R, D)
        result_ref[:, pl.ds(s, 1), :] = (x + branch + fbias_ref[...]).reshape(R, 1, D)
        u = unit[s]
        scaled = ngrad * gain_ref[...]
        sgrad_ref[:, pl.ds(s, 1), :] = (
            cot
            + istd[s][:, :1]
            * (
                scaled
                - jnp.mean(scaled, axis=-1, keepdims=True)
                - u * jnp.mean(scaled * u, axis=-1, keepdims=True)
            )
        ).reshape(R, 1, D)
        for i, value in enumerate((ngrad * u, ngrad, cot)):
            sum_tp[t, i] += jnp.sum(value, axis=0, keepdims=True).reshape(D // 128, 128)

    def m_copy(d):
        return remote(sum_tp.at[t], sum_tp.at[t], ms.at[d], mr.at[0], {"tp": (t + d) % TP})

    def n_copy(d):
        return remote(
            sum_seq.at[z], sum_seq.at[z], ms.at[TP + d], mr.at[1], {"seq": (z + d) % Z}
        )

    for d in range(1, TP):
        m_copy(d).start()
    same(sum_tp.at[pl.ds(0, TP - 1)], ms.at[0], mr.at[0], here).wait_recv()
    total = sum_tp[0]
    for d in range(1, TP):
        total = total + sum_tp[d]
    sum_seq[z] = total
    for d in range(1, Z):
        n_copy(d).start()
    same(sum_seq.at[pl.ds(0, Z - 1)], ms.at[0], mr.at[1], here).wait_recv()
    total = sum_seq[0]
    for d in range(1, Z):
        total = total + sum_seq[d]
    sums_ref[...] = total

    for d in range(1, TP):
        m_copy(d).wait_send()
    for d in range(1, Z):
        n_copy(d).wait_send()
    for copy in out_copies(S - 1):
        copy.wait()

    @pl.loop(0, S)
    def _(s):
        drain_gather(s)
        for kind in range(2):
            half_copy(kind, s).wait_send()
            for d in range(1, chips):
                p_copy(kind, s, d).wait_send()


def block_call(stream, cotangent, gain, offset, fbias, abias, ubias, wa, wo, wu, wd, Z, TP):
    R, S, D = stream.shape
    local, hidden = wo.shape[0], wu.shape[1]
    L = Z * TP * R
    chips = TP // 2
    levels = chips.bit_length() - 1
    vm = pl.BlockSpec(memory_space=pltpu.VMEM)
    anywhere = pl.BlockSpec(memory_space=pl.ANY)
    shape = jax.ShapeDtypeStruct
    dma = pltpu.SemaphoreType.DMA
    return pl.pallas_call(
        functools.partial(block_kernel, (Z, TP, S, R, D)),
        in_specs=[vm] * 7 + [anywhere] * 4,
        out_specs=[anywhere] * 6 + [vm] * 5,
        out_shape=[
            shape((S, Z, TP, R, D), BF),
            shape((S, Z, TP, R, D), BF),
            shape((S, L, hidden), BF),
            shape((S, L, hidden), BF),
            shape((S, L, local), BF),
            shape((3, S, L, local), BF),
            shape((R, S, D), F32),
            shape((R, S, D), F32),
            shape((3, D // 128, 128), F32),
            shape((3, local), F32),
            shape((1, hidden), F32),
        ],
        scratch_shapes=[
            pltpu.VMEM((2, S, Z, TP, R, D), BF),
            pltpu.VMEM((3, D, local), BF),
            pltpu.VMEM((local, D), BF),
            pltpu.VMEM((D, hidden), BF),
            pltpu.VMEM((hidden, D), BF),
            pltpu.VMEM((S, R, D), F32),
            pltpu.VMEM((S, R, 128), F32),
            pltpu.VMEM((3, L, min(128, local)), F32),
            pltpu.VMEM((3, L, local), F32),
            pltpu.VMEM((L, local), BF),
            pltpu.VMEM((L, hidden), BF),
            pltpu.VMEM((L, hidden), BF),
            pltpu.VMEM((L, local), BF),
            pltpu.VMEM((3, L, local), BF),
            pltpu.VMEM((2, S, chips, 2, R, D), BF),
            pltpu.VMEM((2, S, chips, R, D), BF),
            pltpu.VMEM((2, S, chips, R, D), BF),
            pltpu.VMEM((TP, 3, D // 128, 128), F32),
            pltpu.VMEM((Z, 3, D // 128, 128), F32),
            dma((S, Z)),
            dma((S, Z)),
            dma((S, chips * levels, Z)),
            dma((S, TP, Z)),
            dma((S, chips)),
            dma((S, TP)),
            dma((2, S, chips)),
            dma((2, S)),
            dma((2, S)),
            dma((TP + Z,)),
            dma((2,)),
            dma((4,)),
            dma((6,)),
        ],
        compiler_params=pltpu.CompilerParams(
            collective_id=0, has_side_effects=True, vmem_limit_bytes=67000000
        ),
        name="block",
    )(stream, cotangent, gain, offset, fbias, abias, ubias, wa, wo, wu, wd)


def weight_kernel(steps, normed, grads, pre, dproj, hid_hbm, ctx_hbm, up, attend, down, output, hid, ctx, sem):
    i = pl.program_id(0)
    loads = [
        pltpu.make_async_copy(hid_hbm, hid, sem.at[0]),
        pltpu.make_async_copy(ctx_hbm, ctx, sem.at[1]),
    ]

    @pl.when(i == 0)
    def _():
        for load in loads:
            load.start()

    @pl.when(i < steps)
    def _():
        up[...] = dot(normed[...], pre[...], (0, 0))
        for j in range(3):
            attend[j] = dot(normed[...], dproj[j], (0, 0))

    @pl.when(i == steps)
    def _():
        for load in loads:
            load.wait()

    @pl.when(i >= steps)
    def _():
        down[...] = dot(hid[...], grads[...], (0, 0))
        output[...] = dot(ctx[...], grads[...], (0, 0))


def weight_call(normed, grads, pre, dproj, hid, ctx):
    tokens, D = normed.shape
    hidden, local = pre.shape[1], ctx.shape[1]
    tile = 512 if tokens * 512 * 2 <= (2 << 20) else 256
    steps = D // tile
    whole = lambda *shape: pl.BlockSpec(shape, lambda i: (0,) * len(shape), pipeline_mode=pl.Buffered(1))
    first = lambda i: jnp.minimum(i, steps - 1)
    second = lambda i: jnp.maximum(i - steps, 0)
    anywhere = pl.BlockSpec(memory_space=pl.ANY)
    shape = jax.ShapeDtypeStruct
    return pl.pallas_call(
        functools.partial(weight_kernel, steps),
        grid=(2 * steps,),
        in_specs=[
            pl.BlockSpec((tokens, tile), lambda i: (0, first(i))),
            pl.BlockSpec((tokens, tile), lambda i: (0, second(i))),
            whole(tokens, hidden),
            whole(3, tokens, local),
            anywhere,
            anywhere,
        ],
        out_specs=[
            pl.BlockSpec((tile, hidden), lambda i: (first(i), 0)),
            pl.BlockSpec((3, tile, local), lambda i: (0, first(i), 0)),
            pl.BlockSpec((hidden, tile), lambda i: (0, second(i))),
            pl.BlockSpec((local, tile), lambda i: (0, second(i))),
        ],
        out_shape=[
            shape((D, hidden), F32),
            shape((3, D, local), F32),
            shape((hidden, D), F32),
            shape((local, D), F32),
        ],
        scratch_shapes=[
            pltpu.VMEM((tokens, hidden), BF),
            pltpu.VMEM((tokens, local), BF),
            pltpu.SemaphoreType.DMA((2,)),
        ],
        compiler_params=pltpu.CompilerParams(vmem_limit_bytes=67000000),
        name="weights",
    )(normed, grads, pre, dproj, hid, ctx)


def per_device(
    stream,
    norm_gain,
    norm_offset,
    attend_weight,
    attend_bias,
    output_weight,
    up_weight,
    up_bias,
    down_weight,
    final_bias,
    cotangent,
):
    R, S, D = stream.shape
    local = attend_weight.shape[2]
    hidden = up_weight.shape[1]
    TP, Z = lax.axis_size("tp"), lax.axis_size("seq")
    tokens = R * S * TP * Z
    weights = jnp.swapaxes(attend_weight, 0, 1)
    (
        normed, grads, hid, pre, ctx, dproj, result, stream_grad, sums, abias_grad, ubias_grad
    ) = block_call(
        stream, cotangent, norm_gain.reshape(1, D), norm_offset.reshape(1, D),
        final_bias.reshape(1, D), attend_bias.reshape(3, 1, local), up_bias.reshape(1, hidden),
        weights, output_weight, up_weight, down_weight, Z, TP,
    )
    up_grad, attend_grad, down_grad, output_grad = weight_call(
        normed.reshape(tokens, D), grads.reshape(tokens, D), pre.reshape(tokens, hidden),
        dproj.reshape(3, tokens, local), hid.reshape(tokens, hidden), ctx.reshape(tokens, local),
    )
    return (
        result,
        stream_grad,
        sums[0].reshape(D),
        sums[1].reshape(D),
        jnp.swapaxes(attend_grad, 0, 1),
        abias_grad,
        output_grad,
        up_grad,
        ubias_grad.reshape(hidden),
        down_grad,
        sums[2].reshape(D),
    )


def solution(mesh):
    in_specs = (
        P(("seq", "tp"), None, None),
        P(),
        P(),
        P(None, None, "tp"),
        P(None, "tp"),
        P("tp", None),
        P(None, "tp"),
        P("tp"),
        P("tp", None),
        P(),
        P(("seq", "tp"), None, None),
    )
    out_specs = (
        P(("seq", "tp"), None, None),
        P(("seq", "tp"), None, None),
        P(),
        P(),
        P(None, None, "tp"),
        P(None, "tp"),
        P("tp", None),
        P(None, "tp"),
        P("tp"),
        P("tp", None),
        P(),
    )
    return jax.shard_map(
        per_device, mesh=mesh, in_specs=in_specs, out_specs=out_specs, check_vma=False
    )
```

```python
import functools
import math

import jax
import jax.numpy as jnp
from jax import lax
from jax.experimental import pallas as pl
from jax.experimental.pallas import tpu as pltpu
from jax.sharding import PartitionSpec as P

HEAD_DIM = 64
ROT = 32

EPS = 1e-05
GELU_C = 0.7978845608028654
CUBIC = 0.044715
LOG_BASE = math.log(10000.0)
BF = jnp.bfloat16
F32 = jnp.float32
MESH = pl.DeviceIdType.MESH


def gelu_parts(pre_act):
    inner_arg = GELU_C * (pre_act + CUBIC * pre_act * pre_act * pre_act)
    tanh_value = jnp.tanh(inner_arg)
    gelu_value = 0.5 * pre_act * (1.0 + tanh_value)
    gelu_slope = 0.5 * (1.0 + tanh_value) + 0.5 * pre_act * (
        1.0 - tanh_value * tanh_value
    ) * GELU_C * (1.0 + 3.0 * CUBIC * pre_act * pre_act)
    return (gelu_value, gelu_slope)


def dot(a, b, dims):
    return lax.dot_general(a, b, ((dims[:1], dims[1:]), ((), ())), preferred_element_type=F32)


def flip(index, bit):
    return index + bit - 2 * bit * ((index // bit) % 2)


def flip_all(index, mask):
    bit = 1
    while bit <= mask:
        if mask & bit:
            index = flip(index, bit)
        bit *= 2
    return index


def head_pass(q_all, k_all, v_all, g_all, heads, block=256):
    length, width = q_all.shape
    scale = jnp.asarray(HEAD_DIM ** (-0.5), BF)
    block = min(block, length)
    lane = lax.broadcasted_iota(jnp.int32, (1, width), 1) // HEAD_DIM
    zero = jnp.zeros((), BF)
    parts = [(start, head) for start in range(0, length, block) for head in range(heads)]

    def masked(x, start, head):
        return jnp.where(lane == head, x[start : start + block], zero)

    qs = [masked(q_all, a, h) * scale for a, h in parts]
    gs = [masked(g_all, a, h) for a, h in parts]

    def weights(s, start):
        diag = s[:, start:]
        row = lax.broadcasted_iota(jnp.int32, diag.shape, 0)
        col = lax.broadcasted_iota(jnp.int32, diag.shape, 1)
        diag = jnp.where(row >= col, diag, -jnp.inf)
        s = diag if start == 0 else jnp.concatenate([s[:, :start], diag], axis=1)
        p = jnp.exp(s - jnp.max(s, axis=1, keepdims=True))
        return p * (1.0 / jnp.sum(p, axis=1, keepdims=True))

    cs, dqs, dks, dvs = [], [], [], []
    together = len(parts) if length <= 512 else heads
    for first in range(0, len(parts), together):
        group = slice(first, first + together)
        stops = [a + block for a, h in parts[group]]
        gq, gg = qs[group], gs[group]
        ss = [dot(q, k_all[:n], (1, 1)) for q, n in zip(gq, stops)]
        dps = [dot(g, v_all[:n], (1, 1)) for g, n in zip(gg, stops)]
        ps = [weights(s, a) for s, (a, h) in zip(ss, parts[group])]
        pbs = [p.astype(BF) for p in ps]
        gc = [dot(p, v_all[:n], (1, 0)).astype(BF) for p, n in zip(pbs, stops)]
        dvs += [dot(g, p, (0, 0)) for g, p in zip(gg, pbs)]
        deltas = [
            jnp.sum(g.astype(F32) * c.astype(F32), axis=1, keepdims=True) for g, c in zip(gg, gc)
        ]
        dss = [(p * (dp - delta)).astype(BF) for p, dp, delta in zip(ps, dps, deltas)]
        dqs += [dot(ds, k_all[:n], (1, 0)) for ds, n in zip(dss, stops)]
        dks += [dot(q, ds, (0, 0)) for q, ds in zip(gq, dss)]
        cs += gc

    def rows(values):
        blocks = []
        for n in range(0, len(parts), heads):
            value = values[n]
            for h in range(1, heads):
                value = jnp.where(lane == h, values[n + h], value)
            blocks.append(value)
        return jnp.concatenate(blocks, axis=0)

    def columns(values):
        total = None
        for n in range(0, len(parts), heads):
            value = values[n]
            for h in range(1, heads):
                value = value + values[n + h]
            if total is None:
                total = value
            else:
                old = total.shape[1]
                total = jnp.concatenate([total + value[:, :old], value[:, old:]], axis=1)
        return total.T

    return [rows(cs), rows(dqs) * scale.astype(F32), columns(dks), columns(dvs)]


def block_kernel(
    dims,
    stream_ref, cot_ref, gain_ref, offset_ref, fbias_ref, abias_ref, ubias_ref,
    wa_hbm, wo_hbm, wu_hbm, wd_hbm,
    norm_out, grad_out, hid_out, pre_out, ctx_out, dproj_out,
    result_ref, sgrad_ref, gsum_ref, osum_ref, fsum_ref, abg_ref, ubg_ref,
    gat, wa, wo, wu, wd, unit, istd, table, proj, cgrad, hid, pre, ctx, dproj,
    part, half_in, parts_in, sum_tp, sum_seq, ubg,
    zs, zr, xs, xr, fs, fr, ps, hr, pr, ms, mr, ws, os,
):
    Z, TP, S, R, D = dims
    z, t = lax.axis_index("seq"), lax.axis_index("tp")
    chip, core = t // 2, t % 2
    chips = TP // 2
    levels = chips.bit_length() - 1
    bits = [
        (1 - core) * (1 << i) + core * (1 << (levels - 1 - i)) for i in range(levels)
    ]
    partner = chip * 2 + 1 - core
    L = Z * TP * R
    local = wo.shape[0]
    hidden = wu.shape[1]
    pair = min(128, local)
    own_rows = TP * R

    loads = [
        pltpu.make_async_copy(src, dst, ws.at[i])
        for i, (src, dst) in enumerate(((wa_hbm, wa), (wo_hbm, wo), (wu_hbm, wu), (wd_hbm, wd)))
    ]
    for load in loads:
        load.start()
    barrier = pltpu.get_barrier_semaphore()
    for d in range(1, TP):
        pl.semaphore_signal(barrier, inc=1, device_id={"tp": (t + d) % TP}, device_id_type=MESH)
    for d in range(1, Z):
        pl.semaphore_signal(barrier, inc=1, device_id={"seq": (z + d) % Z}, device_id_type=MESH)

    def normalize(s):
        x = stream_ref[:, pl.ds(s, 1), :].reshape(R, D)
        mean = jnp.mean(x, axis=-1, keepdims=True)
        centred = x - mean
        inv = lax.rsqrt(jnp.mean(centred * centred, axis=-1, keepdims=True) + EPS)
        u = centred * inv
        unit[s] = u
        istd[s] = jnp.broadcast_to(inv, (R, 128))
        gat[0, s, z, t] = (u * gain_ref[...] + offset_ref[...]).astype(BF)
        gat[1, s, z, t] = cot_ref[:, pl.ds(s, 1), :].reshape(R, D).astype(BF)

    normalize(0)
    pl.semaphore_wait(barrier, TP + Z - 2)

    def remote(src, dst, ssem, rsem, dev):
        return pltpu.make_async_remote_copy(
            src_ref=src, dst_ref=dst, send_sem=ssem, recv_sem=rsem,
            device_id=dev, device_id_type=MESH,
        )

    def same(ref, ssem, rsem, dev):
        return remote(ref, ref, ssem, rsem, dev)

    def unit_of(s, zz, tt):
        return gat.at[:, s, zz, tt]

    def column(s, tt):
        return gat.at[:, s, :, tt]

    here = {"tp": t}
    other = [z] + [flip_all(z, r) if Z & (Z - 1) == 0 else (z + r) % Z for r in range(1, Z)]
    sender = [z] + [flip_all(z, r) if Z & (Z - 1) == 0 else (z + Z - r) % Z for r in range(1, Z)]

    def z_copy(s, r):
        return same(unit_of(s, z, t), zs.at[s, r], zr.at[s, z], {"seq": other[r]})

    def z_sends(s):
        for r in range(1, Z):
            z_copy(s, r).start()

    def x_copy(s, r, src, slot, i):
        return same(
            unit_of(s, sender[r], src), xs.at[s, slot, r], xr.at[s, src, sender[r]],
            {"tp": flip(chip, bits[i]) * 2 + core},
        )

    def f_copy(s, src, r):
        return same(column(s, src), fs.at[s, r], fr.at[s, src], {"tp": partner})

    def source(mask):
        c = chip
        for i in range(levels):
            if (mask >> i) & 1:
                c = flip(c, bits[i])
        return c * 2 + core

    order = sorted(range(1, chips), key=lambda m: (bin(m).count("1"), m))

    def later(mask):
        first = mask.bit_length()
        return [(mask * levels + i, i) for i in range(first, levels)]

    def own_unit(s, r):
        if r > 0:
            zz = sender[r]
            same(unit_of(s, zz, t), zs.at[s, 0], zr.at[s, zz], here).wait_recv()
        for slot, i in later(0):
            x_copy(s, r, t, slot, i).start()
        if r == Z - 1:
            f_copy(s, t, 0).start()

    def pass_unit(s, r, level):
        for mask in order:
            if bin(mask).count("1") != level:
                continue
            src = source(mask)
            same(unit_of(s, sender[r], src), zs.at[s, 0], xr.at[s, src, sender[r]], here).wait_recv()
            for slot, i in later(mask):
                x_copy(s, r, src, slot, i).start()
            if r == Z - 1:
                f_copy(s, src, mask).start()

    def end_step(s):
        for c in range(chips):
            src = ((chip + c) % chips) * 2 + 1 - core
            same(column(s, src), zs.at[s, 0], fr.at[s, src], here).wait_recv()

    def drain_gather(s):
        for r in range(1, Z):
            z_copy(s, r).wait_send()
        for mask in [0] + order:
            src = source(mask)
            for slot, i in later(mask):
                for r in range(Z):
                    x_copy(s, r, src, slot, i).wait_send()
            f_copy(s, src, mask).wait_send()

    def half_copy(kind, s):
        return remote(
            part.at[kind, s, :, 1 - core], half_in.at[kind, s], ps.at[kind, s, 0], hr.at[kind, s],
            {"tp": partner},
        )

    def p_copy(kind, s, d):
        to = (chip + d) % chips
        return remote(
            part.at[kind, s, to, core], parts_in.at[kind, s, chip], ps.at[kind, s, d],
            pr.at[kind, s], {"tp": to * 2 + core},
        )

    def half_sends(s):
        for kind in range(2):
            half_copy(kind, s).start()

    def p_sends(s):
        for kind in range(2):
            half_copy(kind, s).wait_recv()
            for d in range(chips):
                c = (chip + d) % chips
                part[kind, s, c, core] = (
                    part[kind, s, c, core].astype(F32) + half_in[kind, s, c].astype(F32)
                ).astype(BF)
            for d in range(1, chips):
                p_copy(kind, s, d).start()

    def out_copies(s):
        return [
            pltpu.make_async_copy(src, dst, os.at[i])
            for i, (src, dst) in enumerate((
                (gat.at[0, s], norm_out.at[s]), (gat.at[1, s], grad_out.at[s]),
                (hid, hid_out.at[s]), (pre, pre_out.at[s]), (ctx, ctx_out.at[s]),
                (dproj, dproj_out.at[:, s]),
            ))
        ]

    def group_steps(n):
        steps = []
        if n % Z == 1:
            steps.append((n // Z + 1, z_sends))
        for level in range(levels + 1):
            m = n - 2 * level
            if m > 0 and level == 0:
                steps.append((m // Z, functools.partial(own_unit, r=m % Z)))
            elif m >= 0 and level > 0:
                steps.append((m // Z, functools.partial(pass_unit, r=m % Z, level=level)))
        return steps

    lead = 2 * levels

    def run_groups(s, part):
        for k in range(Z * part // 4, Z * (part + 1) // 4):
            for i, step in group_steps(Z + lead + k):

                @pl.when(s + i < S)
                def _(step=step, i=i):
                    step(s + i)

    z_sends(0)
    own_unit(0, 0)

    @pl.loop(1, S)
    def _(s):
        normalize(s)

    lane = lax.broadcasted_iota(jnp.int32, (L, pair), 1) % HEAD_DIM
    place = lax.broadcasted_iota(jnp.int32, (L, pair), 0).astype(F32)
    half = ROT // 2
    freq = jnp.exp((lane % half).astype(F32) * (-2.0 * LOG_BASE / ROT))
    angle = place * freq
    cosine, sine = jnp.cos(angle), jnp.sin(angle)
    table[0] = jnp.where(lane < ROT, cosine, 1.0)
    table[1] = jnp.where(lane < half, -sine, jnp.where(lane < ROT, sine, 0.0))
    abg_ref[...] = jnp.zeros_like(abg_ref)
    ubg[...] = jnp.zeros_like(ubg)
    for load in loads:
        load.wait()

    for n in range(1, Z + lead):
        for i, step in group_steps(n):
            if i < S:
                step(i)
    end_step(0)

    def turned(x, sign):
        first = lax.broadcasted_iota(jnp.int32, (1, pair), 1) % HEAD_DIM < half
        crossed = jnp.where(first, pltpu.roll(x, pair - half, 1), pltpu.roll(x, half, 1))
        return x * table[0] + sign * (crossed * table[1])

    @pl.loop(0, S)
    def _(s):
        def rows_n():
            return gat[0, s].reshape(L, D)

        def rows_g():
            return gat[1, s].reshape(L, D)

        @pl.when(s > 0)
        def _():
            for copy in out_copies(s - 1):
                copy.wait()

        @pl.loop(0, 3)
        def _(j):
            proj[j] = dot(rows_n(), wa[j], (1, 0)) + abias_ref[pl.ds(j, 1), :]

        cgrad[...] = dot(rows_g(), wo[...], (1, 1)).astype(BF)

        @pl.when(s > 0)
        def _():
            p_sends(s - 1)

        @pl.loop(0, local // pair)
        def _(h):
            lanes = pl.ds(pl.multiple_of(h * pair, pair), pair)
            q = turned(proj[0, :, lanes], 1.0).astype(BF)
            k = turned(proj[1, :, lanes], 1.0).astype(BF)
            v = proj[2, :, lanes].astype(BF)
            c, dq, dk, dv = head_pass(q, k, v, cgrad[:, lanes], pair // HEAD_DIM)
            ctx[:, lanes] = c
            for j, value in enumerate((turned(dq, -1.0), turned(dk, -1.0), dv)):
                dproj[j, :, lanes] = value.astype(BF)
                abg_ref[j : j + 1, lanes] += jnp.sum(value, axis=0, keepdims=True)

            @pl.when(h == 0)
            def _():
                run_groups(s, 0)

        tile = 256 if L <= 512 else 128
        middle = hidden // tile // 2

        def feed_forward(n):
            cols = pl.ds(pl.multiple_of(n * tile, tile), tile)
            value, slope = gelu_parts(dot(rows_n(), wu[:, cols], (1, 0)) + ubias_ref[:, cols])
            hid[:, cols] = value.astype(BF)
            grad = dot(rows_g(), wd[cols, :], (1, 1)) * slope
            pre[:, cols] = grad.astype(BF)
            ubg[:, cols] += jnp.sum(grad, axis=0, keepdims=True)

        @pl.loop(0, hidden // tile)
        def _(n):
            feed_forward(n)

            @pl.when(n == 0)
            def _():
                run_groups(s, 1)

            @pl.when(n == middle)
            def _():
                run_groups(s, 2)

        for copy in out_copies(s):
            copy.start()

        mine = pl.ds(pl.multiple_of(z * own_rows, own_rows), own_rows)

        @pl.loop(0, D // 256)
        def _(n):
            cols = pl.ds(pl.multiple_of(n * 256, 256), 256)
            out = dot(ctx[mine, :], wo[:, cols], (1, 0)) + dot(hid[mine, :], wd[:, cols], (1, 0))
            back = dot(pre[mine, :], wu[cols, :], (1, 1))
            for j in range(3):
                back = back + dot(dproj[j, mine, :], wa[j, cols, :], (1, 1))
            part[0, s, :, :, :, cols] = out.astype(BF).reshape(chips, 2, R, 256)
            part[1, s, :, :, :, cols] = back.astype(BF).reshape(chips, 2, R, 256)

        half_sends(s)

        run_groups(s, 3)

        @pl.when(s + 1 < S)
        def _():
            end_step(s + 1)

    p_sends(S - 1)
    sum_tp[t] = jnp.zeros_like(sum_tp[t])

    @pl.loop(0, S)
    def _(s):
        totals = []
        for kind in range(2):
            incoming = parts_in.at[kind, s, pl.ds(0, chips - 1)]
            remote(incoming, incoming, ps.at[kind, s, 0], pr.at[kind, s], here).wait_recv()
            total = part[kind, s, chip, core].astype(F32)
            for d in range(1, chips):
                total = total + parts_in[kind, s, (chip + d) % chips].astype(F32)
            totals.append(total)
        branch, ngrad = totals
        x = stream_ref[:, pl.ds(s, 1), :].reshape(R, D)
        cot = cot_ref[:, pl.ds(s, 1), :].reshape(R, D)
        result_ref[:, pl.ds(s, 1), :] = (x + branch + fbias_ref[...]).reshape(R, 1, D)
        u = unit[s]
        scaled = ngrad * gain_ref[...]
        sgrad_ref[:, pl.ds(s, 1), :] = (
            cot
            + istd[s][:, :1]
            * (
                scaled
                - jnp.mean(scaled, axis=-1, keepdims=True)
                - u * jnp.mean(scaled * u, axis=-1, keepdims=True)
            )
        ).reshape(R, 1, D)
        for i, value in enumerate((ngrad * u, ngrad, cot)):
            sum_tp[t, i] += jnp.sum(value, axis=0, keepdims=True).reshape(D // 128, 128)

    def m_copy(d):
        return remote(sum_tp.at[t], sum_tp.at[t], ms.at[d], mr.at[0], {"tp": (t + d) % TP})

    def n_copy(d):
        return remote(
            sum_seq.at[z], sum_seq.at[z], ms.at[TP + d], mr.at[1], {"seq": (z + d) % Z}
        )

    for d in range(1, TP):
        m_copy(d).start()
    same(sum_tp.at[pl.ds(0, TP - 1)], ms.at[0], mr.at[0], here).wait_recv()
    total = sum_tp[0]
    for d in range(1, TP):
        total = total + sum_tp[d]
    sum_seq[z] = total
    for d in range(1, Z):
        n_copy(d).start()
    same(sum_seq.at[pl.ds(0, Z - 1)], ms.at[0], mr.at[1], here).wait_recv()
    total = sum_seq[0]
    for d in range(1, Z):
        total = total + sum_seq[d]
    gsum_ref[...], osum_ref[...], fsum_ref[...] = total[0], total[1], total[2]
    ubg_ref[...] = ubg[...].reshape(hidden // 128, 128)

    for d in range(1, TP):
        m_copy(d).wait_send()
    for d in range(1, Z):
        n_copy(d).wait_send()
    for copy in out_copies(S - 1):
        copy.wait()

    @pl.loop(0, S)
    def _(s):
        drain_gather(s)
        for kind in range(2):
            half_copy(kind, s).wait_send()
            for d in range(1, chips):
                p_copy(kind, s, d).wait_send()


def block_call(stream, cotangent, gain, offset, fbias, abias, ubias, wa, wo, wu, wd, Z, TP):
    R, S, D = stream.shape
    local, hidden = wo.shape[0], wu.shape[1]
    L = Z * TP * R
    chips = TP // 2
    levels = chips.bit_length() - 1
    vm = pl.BlockSpec(memory_space=pltpu.VMEM)
    anywhere = pl.BlockSpec(memory_space=pl.ANY)
    shape = jax.ShapeDtypeStruct
    dma = pltpu.SemaphoreType.DMA
    return pl.pallas_call(
        functools.partial(block_kernel, (Z, TP, S, R, D)),
        in_specs=[vm] * 7 + [anywhere] * 4,
        out_specs=[anywhere] * 6 + [vm] * 7,
        out_shape=[
            shape((S, Z, TP, R, D), BF),
            shape((S, Z, TP, R, D), BF),
            shape((S, L, hidden), BF),
            shape((S, L, hidden), BF),
            shape((S, L, local), BF),
            shape((3, S, L, local), BF),
            shape((R, S, D), F32),
            shape((R, S, D), F32),
            shape((D // 128, 128), F32),
            shape((D // 128, 128), F32),
            shape((D // 128, 128), F32),
            shape((3, local), F32),
            shape((hidden // 128, 128), F32),
        ],
        scratch_shapes=[
            pltpu.VMEM((2, S, Z, TP, R, D), BF),
            pltpu.VMEM((3, D, local), BF),
            pltpu.VMEM((local, D), BF),
            pltpu.VMEM((D, hidden), BF),
            pltpu.VMEM((hidden, D), BF),
            pltpu.VMEM((S, R, D), F32),
            pltpu.VMEM((S, R, 128), F32),
            pltpu.VMEM((2, L, min(128, local)), F32),
            pltpu.VMEM((3, L, local), F32),
            pltpu.VMEM((L, local), BF),
            pltpu.VMEM((L, hidden), BF),
            pltpu.VMEM((L, hidden), BF),
            pltpu.VMEM((L, local), BF),
            pltpu.VMEM((3, L, local), BF),
            pltpu.VMEM((2, S, chips, 2, R, D), BF),
            pltpu.VMEM((2, S, chips, R, D), BF),
            pltpu.VMEM((2, S, chips, R, D), BF),
            pltpu.VMEM((TP, 3, D // 128, 128), F32),
            pltpu.VMEM((Z, 3, D // 128, 128), F32),
            pltpu.VMEM((1, hidden), F32),
            dma((S, Z)),
            dma((S, Z)),
            dma((S, chips * levels, Z)),
            dma((S, TP, Z)),
            dma((S, chips)),
            dma((S, TP)),
            dma((2, S, chips)),
            dma((2, S)),
            dma((2, S)),
            dma((TP + Z,)),
            dma((2,)),
            dma((4,)),
            dma((6,)),
        ],
        compiler_params=pltpu.CompilerParams(
            collective_id=0, has_side_effects=True, vmem_limit_bytes=67000000
        ),
        name="block",
    )(stream, cotangent, gain, offset, fbias, abias, ubias, wa, wo, wu, wd)


def weight_kernel(steps, normed, grads, pre, dproj, hid_hbm, ctx_hbm, *rest):
    smalls = (len(rest) - 7) // 2
    given, rest = rest[:smalls], rest[smalls:]
    up, attend, down, output = rest[:4]
    handed, (hid, ctx, sem) = rest[4 : 4 + smalls], rest[4 + smalls :]
    i = pl.program_id(0)
    loads = [
        pltpu.make_async_copy(hid_hbm, hid, sem.at[0]),
        pltpu.make_async_copy(ctx_hbm, ctx, sem.at[1]),
    ]

    @pl.when(i == 0)
    def _():
        for load in loads:
            load.start()
        for source, target in zip(given, handed):
            target[...] = source[...]

    @pl.when(i < steps)
    def _():
        up[...] = dot(normed[...], pre[...], (0, 0))
        for j in range(3):
            attend[j] = dot(normed[...], dproj[j], (0, 0))

    @pl.when(i == steps)
    def _():
        for load in loads:
            load.wait()

    @pl.when(i >= steps)
    def _():
        down[...] = dot(hid[...], grads[...], (0, 0))
        output[...] = dot(ctx[...], grads[...], (0, 0))


def weight_call(normed, grads, pre, dproj, hid, ctx, smalls):
    tokens, D = normed.shape
    hidden, local = pre.shape[1], ctx.shape[1]
    tile = 512 if tokens * 512 * 2 <= (2 << 20) else 256
    steps = D // tile
    whole = lambda *shape: pl.BlockSpec(shape, lambda i: (0,) * len(shape), pipeline_mode=pl.Buffered(1))
    first = lambda i: jnp.minimum(i, steps - 1)
    second = lambda i: jnp.maximum(i - steps, 0)
    anywhere = pl.BlockSpec(memory_space=pl.ANY)
    shape = jax.ShapeDtypeStruct
    return pl.pallas_call(
        functools.partial(weight_kernel, steps),
        grid=(2 * steps,),
        in_specs=[
            pl.BlockSpec((tokens, tile), lambda i: (0, first(i))),
            pl.BlockSpec((tokens, tile), lambda i: (0, second(i))),
            whole(tokens, hidden),
            whole(3, tokens, local),
            anywhere,
            anywhere,
        ]
        + [whole(*small.shape) for small in smalls],
        out_specs=[
            pl.BlockSpec((tile, hidden), lambda i: (first(i), 0)),
            pl.BlockSpec((3, tile, local), lambda i: (0, first(i), 0)),
            pl.BlockSpec((hidden, tile), lambda i: (0, second(i))),
            pl.BlockSpec((local, tile), lambda i: (0, second(i))),
        ]
        + [whole(*small.shape) for small in smalls],
        out_shape=[
            shape((D, hidden), F32),
            shape((3, D, local), F32),
            shape((hidden, D), F32),
            shape((local, D), F32),
        ]
        + [shape(small.shape, F32) for small in smalls],
        scratch_shapes=[
            pltpu.VMEM((tokens, hidden), BF),
            pltpu.VMEM((tokens, local), BF),
            pltpu.SemaphoreType.DMA((2,)),
        ],
        compiler_params=pltpu.CompilerParams(vmem_limit_bytes=67000000),
        name="weights",
    )(normed, grads, pre, dproj, hid, ctx, *smalls)


def per_device(
    stream,
    norm_gain,
    norm_offset,
    attend_weight,
    attend_bias,
    output_weight,
    up_weight,
    up_bias,
    down_weight,
    final_bias,
    cotangent,
):
    R, S, D = stream.shape
    local = attend_weight.shape[2]
    hidden = up_weight.shape[1]
    TP, Z = lax.axis_size("tp"), lax.axis_size("seq")
    tokens = R * S * TP * Z
    weights = jnp.swapaxes(attend_weight, 0, 1)
    (
        normed, grads, hid, pre, ctx, dproj, *smalls
    ) = block_call(
        stream, cotangent, norm_gain.reshape(1, D), norm_offset.reshape(1, D),
        final_bias.reshape(1, D), attend_bias, up_bias.reshape(1, hidden),
        weights, output_weight, up_weight, down_weight, Z, TP,
    )
    (
        up_grad, attend_grad, down_grad, output_grad,
        result, stream_grad, gain_grad, offset_grad, fbias_grad, abias_grad, ubias_grad,
    ) = weight_call(
        normed.reshape(tokens, D), grads.reshape(tokens, D), pre.reshape(tokens, hidden),
        dproj.reshape(3, tokens, local), hid.reshape(tokens, hidden), ctx.reshape(tokens, local),
        smalls,
    )
    return (
        result,
        stream_grad,
        gain_grad.reshape(D),
        offset_grad.reshape(D),
        jnp.swapaxes(attend_grad, 0, 1),
        abias_grad,
        output_grad,
        up_grad,
        ubias_grad.reshape(hidden),
        down_grad,
        fbias_grad.reshape(D),
    )


def solution(mesh):
    in_specs = (
        P(("seq", "tp"), None, None),
        P(),
        P(),
        P(None, None, "tp"),
        P(None, "tp"),
        P("tp", None),
        P(None, "tp"),
        P("tp"),
        P("tp", None),
        P(),
        P(("seq", "tp"), None, None),
    )
    out_specs = (
        P(("seq", "tp"), None, None),
        P(("seq", "tp"), None, None),
        P(),
        P(),
        P(None, None, "tp"),
        P(None, "tp"),
        P("tp", None),
        P(None, "tp"),
        P("tp"),
        P("tp", None),
        P(),
    )
    return jax.shard_map(
        per_device, mesh=mesh, in_specs=in_specs, out_specs=out_specs, check_vma=False
    )
```

```python
import functools
import math

import jax
import jax.numpy as jnp
from jax import lax
from jax.experimental import pallas as pl
from jax.experimental.pallas import tpu as pltpu
from jax.sharding import PartitionSpec as P

HEAD_DIM = 64
ROT = 32

EPS = 1e-05
GELU_C = 0.7978845608028654
CUBIC = 0.044715
LOG_BASE = math.log(10000.0)
BF = jnp.bfloat16
F32 = jnp.float32
MESH = pl.DeviceIdType.MESH


def gelu_parts(pre_act):
    inner_arg = GELU_C * (pre_act + CUBIC * pre_act * pre_act * pre_act)
    tanh_value = jnp.tanh(inner_arg)
    gelu_value = 0.5 * pre_act * (1.0 + tanh_value)
    gelu_slope = 0.5 * (1.0 + tanh_value) + 0.5 * pre_act * (
        1.0 - tanh_value * tanh_value
    ) * GELU_C * (1.0 + 3.0 * CUBIC * pre_act * pre_act)
    return (gelu_value, gelu_slope)


def dot(a, b, dims):
    return lax.dot_general(a, b, ((dims[:1], dims[1:]), ((), ())), preferred_element_type=F32)


def flip(index, bit):
    return index + bit - 2 * bit * ((index // bit) % 2)


def flip_all(index, mask):
    bit = 1
    while bit <= mask:
        if mask & bit:
            index = flip(index, bit)
        bit *= 2
    return index


def head_pass(q_all, k_all, v_all, g_all, heads, block=256):
    length, width = q_all.shape
    scale = jnp.asarray(HEAD_DIM ** (-0.5), BF)
    block = min(block, length)
    lane = lax.broadcasted_iota(jnp.int32, (1, width), 1) // HEAD_DIM
    zero = jnp.zeros((), BF)
    parts = [(start, head) for start in range(0, length, block) for head in range(heads)]

    def masked(x, start, head):
        return jnp.where(lane == head, x[start : start + block], zero)

    qs = [masked(q_all, a, h) * scale for a, h in parts]
    gs = [masked(g_all, a, h) for a, h in parts]

    def weights(s, start):
        diag = s[:, start:]
        row = lax.broadcasted_iota(jnp.int32, diag.shape, 0)
        col = lax.broadcasted_iota(jnp.int32, diag.shape, 1)
        diag = jnp.where(row >= col, diag, -jnp.inf)
        s = diag if start == 0 else jnp.concatenate([s[:, :start], diag], axis=1)
        p = jnp.exp(s - jnp.max(s, axis=1, keepdims=True))
        return p * (1.0 / jnp.sum(p, axis=1, keepdims=True))

    cs, dqs, dks, dvs = [], [], [], []
    together = len(parts) if length <= 512 else heads
    for first in range(0, len(parts), together):
        group = slice(first, first + together)
        stops = [a + block for a, h in parts[group]]
        gq, gg = qs[group], gs[group]
        ss = [dot(q, k_all[:n], (1, 1)) for q, n in zip(gq, stops)]
        dps = [dot(g, v_all[:n], (1, 1)) for g, n in zip(gg, stops)]
        ps = [weights(s, a) for s, (a, h) in zip(ss, parts[group])]
        pbs = [p.astype(BF) for p in ps]
        gc = [dot(p, v_all[:n], (1, 0)).astype(BF) for p, n in zip(pbs, stops)]
        dvs += [dot(g, p, (0, 0)) for g, p in zip(gg, pbs)]
        deltas = [
            jnp.sum(g.astype(F32) * c.astype(F32), axis=1, keepdims=True) for g, c in zip(gg, gc)
        ]
        dss = [(p * (dp - delta)).astype(BF) for p, dp, delta in zip(ps, dps, deltas)]
        dqs += [dot(ds, k_all[:n], (1, 0)) for ds, n in zip(dss, stops)]
        dks += [dot(q, ds, (0, 0)) for q, ds in zip(gq, dss)]
        cs += gc

    def rows(values):
        blocks = []
        for n in range(0, len(parts), heads):
            value = values[n]
            for h in range(1, heads):
                value = jnp.where(lane == h, values[n + h], value)
            blocks.append(value)
        return jnp.concatenate(blocks, axis=0)

    def columns(values):
        total = None
        for n in range(0, len(parts), heads):
            value = values[n]
            for h in range(1, heads):
                value = value + values[n + h]
            if total is None:
                total = value
            else:
                old = total.shape[1]
                total = jnp.concatenate([total + value[:, :old], value[:, old:]], axis=1)
        return total.T

    return [rows(cs), rows(dqs) * scale.astype(F32), columns(dks), columns(dvs)]


def block_kernel(
    dims,
    stream_ref, cot_ref, gain_ref, offset_ref, fbias_ref, abias_ref, ubias_ref,
    wa_hbm, wo_hbm, wu_hbm, wd_hbm,
    norm_out, grad_out, hid_out, pre_out, wide_out, tall_out,
    result_ref, sgrad_ref, gsum_ref, osum_ref, fsum_ref, abg_ref, ubg_ref,
    gat, wa, wo, wu, wd, unit, istd, table, proj, cgrad, hid, pre, ctx, dproj,
    part, half_in, parts_in, sum_tp, sum_seq, ubg, wide, tall,
    zs, zr, xs, xr, fs, fr, ps, hr, pr, ms, mr, ws, os, gs,
):
    Z, TP, S, R, D = dims
    z, t = lax.axis_index("seq"), lax.axis_index("tp")
    chip, core = t // 2, t % 2
    chips = TP // 2
    levels = chips.bit_length() - 1
    bits = [
        (1 - core) * (1 << i) + core * (1 << (levels - 1 - i)) for i in range(levels)
    ]
    partner = chip * 2 + 1 - core
    L = Z * TP * R
    local = wo.shape[0]
    hidden = wu.shape[1]
    pair = min(128, local)
    own_rows = TP * R
    inside = ctx.shape[0] == S

    loads = [
        pltpu.make_async_copy(src, dst, ws.at[i])
        for i, (src, dst) in enumerate(((wa_hbm, wa), (wo_hbm, wo), (wu_hbm, wu), (wd_hbm, wd)))
    ]
    for load in loads:
        load.start()
    barrier = pltpu.get_barrier_semaphore()
    for d in range(1, TP):
        pl.semaphore_signal(barrier, inc=1, device_id={"tp": (t + d) % TP}, device_id_type=MESH)
    for d in range(1, Z):
        pl.semaphore_signal(barrier, inc=1, device_id={"seq": (z + d) % Z}, device_id_type=MESH)

    def normalize(s):
        x = stream_ref[:, pl.ds(s, 1), :].reshape(R, D)
        mean = jnp.mean(x, axis=-1, keepdims=True)
        centred = x - mean
        inv = lax.rsqrt(jnp.mean(centred * centred, axis=-1, keepdims=True) + EPS)
        u = centred * inv
        unit[s] = u
        istd[s] = jnp.broadcast_to(inv, (R, 128))
        gat[0, s, z, t] = (u * gain_ref[...] + offset_ref[...]).astype(BF)
        gat[1, s, z, t] = cot_ref[:, pl.ds(s, 1), :].reshape(R, D).astype(BF)

    normalize(0)
    pl.semaphore_wait(barrier, TP + Z - 2)

    def remote(src, dst, ssem, rsem, dev):
        return pltpu.make_async_remote_copy(
            src_ref=src, dst_ref=dst, send_sem=ssem, recv_sem=rsem,
            device_id=dev, device_id_type=MESH,
        )

    def same(ref, ssem, rsem, dev):
        return remote(ref, ref, ssem, rsem, dev)

    def unit_of(s, zz, tt):
        return gat.at[:, s, zz, tt]

    def column(s, tt):
        return gat.at[:, s, :, tt]

    here = {"tp": t}
    other = [z] + [flip_all(z, r) if Z & (Z - 1) == 0 else (z + r) % Z for r in range(1, Z)]
    sender = [z] + [flip_all(z, r) if Z & (Z - 1) == 0 else (z + Z - r) % Z for r in range(1, Z)]

    def z_copy(s, r):
        return same(unit_of(s, z, t), zs.at[s, r], zr.at[s, z], {"seq": other[r]})

    def z_sends(s):
        for r in range(1, Z):
            z_copy(s, r).start()

    def x_copy(s, r, src, slot, i):
        return same(
            unit_of(s, sender[r], src), xs.at[s, slot, r], xr.at[s, src, sender[r]],
            {"tp": flip(chip, bits[i]) * 2 + core},
        )

    def f_copy(s, src, r):
        return same(column(s, src), fs.at[s, r], fr.at[s, src], {"tp": partner})

    def source(mask):
        c = chip
        for i in range(levels):
            if (mask >> i) & 1:
                c = flip(c, bits[i])
        return c * 2 + core

    order = sorted(range(1, chips), key=lambda m: (bin(m).count("1"), m))

    def later(mask):
        first = mask.bit_length()
        return [(mask * levels + i, i) for i in range(first, levels)]

    def own_unit(s, r):
        if r > 0:
            zz = sender[r]
            same(unit_of(s, zz, t), zs.at[s, 0], zr.at[s, zz], here).wait_recv()
        for slot, i in later(0):
            x_copy(s, r, t, slot, i).start()
        if r == Z - 1:
            f_copy(s, t, 0).start()

    def pass_unit(s, r, level):
        for mask in order:
            if bin(mask).count("1") != level:
                continue
            src = source(mask)
            same(unit_of(s, sender[r], src), zs.at[s, 0], xr.at[s, src, sender[r]], here).wait_recv()
            for slot, i in later(mask):
                x_copy(s, r, src, slot, i).start()
            if r == Z - 1:
                f_copy(s, src, mask).start()

    def end_step(s):
        for c in range(chips):
            src = ((chip + c) % chips) * 2 + 1 - core
            same(column(s, src), zs.at[s, 0], fr.at[s, src], here).wait_recv()

    def drain_gather(s):
        for r in range(1, Z):
            z_copy(s, r).wait_send()
        for mask in [0] + order:
            src = source(mask)
            for slot, i in later(mask):
                for r in range(Z):
                    x_copy(s, r, src, slot, i).wait_send()
            f_copy(s, src, mask).wait_send()

    def half_copy(kind, s):
        return remote(
            part.at[kind, s, :, 1 - core], half_in.at[kind, s], ps.at[kind, s, 0], hr.at[kind, s],
            {"tp": partner},
        )

    def p_copy(kind, s, d):
        to = (chip + d) % chips
        return remote(
            part.at[kind, s, to, core], parts_in.at[kind, s, chip], ps.at[kind, s, d],
            pr.at[kind, s], {"tp": to * 2 + core},
        )

    def half_sends(s):
        for kind in range(2):
            half_copy(kind, s).start()

    def p_sends(s):
        for kind in range(2):
            half_copy(kind, s).wait_recv()
            for d in range(chips):
                c = (chip + d) % chips
                part[kind, s, c, core] = (
                    part[kind, s, c, core].astype(F32) + half_in[kind, s, c].astype(F32)
                ).astype(BF)
            for d in range(1, chips):
                p_copy(kind, s, d).start()

    def out_copies(s):
        pairs = [
            (gat.at[0, s], norm_out.at[s]), (gat.at[1, s], grad_out.at[s]),
            (hid, hid_out.at[s]), (pre, pre_out.at[s]),
        ]
        if not inside:
            pairs += [(ctx.at[0], tall_out.at[s]), (dproj.at[:, 0], wide_out.at[:, s])]
        return [pltpu.make_async_copy(src, dst, os.at[i]) for i, (src, dst) in enumerate(pairs)]

    def group_steps(n):
        steps = []
        if n % Z == 1:
            steps.append((n // Z + 1, z_sends))
        for level in range(levels + 1):
            m = n - 2 * level
            if m > 0 and level == 0:
                steps.append((m // Z, functools.partial(own_unit, r=m % Z)))
            elif m >= 0 and level > 0:
                steps.append((m // Z, functools.partial(pass_unit, r=m % Z, level=level)))
        return steps

    lead = 2 * levels

    def run_groups(s, part):
        for k in range(Z * part // 4, Z * (part + 1) // 4):
            for i, step in group_steps(Z + lead + k):

                @pl.when(s + i < S)
                def _(step=step, i=i):
                    step(s + i)

    z_sends(0)
    own_unit(0, 0)

    @pl.loop(1, S)
    def _(s):
        normalize(s)

    lane = lax.broadcasted_iota(jnp.int32, (L, pair), 1) % HEAD_DIM
    place = lax.broadcasted_iota(jnp.int32, (L, pair), 0).astype(F32)
    half = ROT // 2
    freq = jnp.exp((lane % half).astype(F32) * (-2.0 * LOG_BASE / ROT))
    angle = place * freq
    cosine, sine = jnp.cos(angle), jnp.sin(angle)
    table[0] = jnp.where(lane < ROT, cosine, 1.0)
    table[1] = jnp.where(lane < half, -sine, jnp.where(lane < ROT, sine, 0.0))
    abg_ref[...] = jnp.zeros_like(abg_ref)
    ubg[...] = jnp.zeros_like(ubg)
    for load in loads:
        load.wait()

    for n in range(1, Z + lead):
        for i, step in group_steps(n):
            if i < S:
                step(i)
    end_step(0)

    def turned(x, sign):
        first = lax.broadcasted_iota(jnp.int32, (1, pair), 1) % HEAD_DIM < half
        crossed = jnp.where(first, pltpu.roll(x, pair - half, 1), pltpu.roll(x, half, 1))
        return x * table[0] + sign * (crossed * table[1])

    @pl.loop(0, S)
    def _(s):
        kept = s if inside else 0

        def rows_n():
            return gat[0, s].reshape(L, D)

        def rows_g():
            return gat[1, s].reshape(L, D)

        @pl.when(s > 0)
        def _():
            for copy in out_copies(s - 1):
                copy.wait()

        @pl.loop(0, 3)
        def _(j):
            proj[j] = dot(rows_n(), wa[j], (1, 0)) + abias_ref[pl.ds(j, 1), :]

        cgrad[...] = dot(rows_g(), wo[...], (1, 1)).astype(BF)

        @pl.when(s > 0)
        def _():
            p_sends(s - 1)

        @pl.loop(0, local // pair)
        def _(h):
            lanes = pl.ds(pl.multiple_of(h * pair, pair), pair)
            q = turned(proj[0, :, lanes], 1.0).astype(BF)
            k = turned(proj[1, :, lanes], 1.0).astype(BF)
            v = proj[2, :, lanes].astype(BF)
            c, dq, dk, dv = head_pass(q, k, v, cgrad[:, lanes], pair // HEAD_DIM)
            ctx[kept, :, lanes] = c
            for j, value in enumerate((turned(dq, -1.0), turned(dk, -1.0), dv)):
                dproj[j, kept, :, lanes] = value.astype(BF)
                abg_ref[j : j + 1, lanes] += jnp.sum(value, axis=0, keepdims=True)

            @pl.when(h == 0)
            def _():
                run_groups(s, 0)

        tile = 256 if L <= 512 else 128
        middle = hidden // tile // 2

        def feed_forward(n):
            cols = pl.ds(pl.multiple_of(n * tile, tile), tile)
            value, slope = gelu_parts(dot(rows_n(), wu[:, cols], (1, 0)) + ubias_ref[:, cols])
            hid[:, cols] = value.astype(BF)
            grad = dot(rows_g(), wd[cols, :], (1, 1)) * slope
            pre[:, cols] = grad.astype(BF)
            ubg[:, cols] += jnp.sum(grad, axis=0, keepdims=True)

        @pl.loop(0, hidden // tile)
        def _(n):
            feed_forward(n)

            @pl.when(n == 0)
            def _():
                run_groups(s, 1)

            @pl.when(n == middle)
            def _():
                run_groups(s, 2)

        for copy in out_copies(s):
            copy.start()

        mine = pl.ds(pl.multiple_of(z * own_rows, own_rows), own_rows)

        @pl.loop(0, D // 256)
        def _(n):
            cols = pl.ds(pl.multiple_of(n * 256, 256), 256)
            out = dot(ctx[kept, mine, :], wo[:, cols], (1, 0)) + dot(hid[mine, :], wd[:, cols], (1, 0))
            back = dot(pre[mine, :], wu[cols, :], (1, 1))
            for j in range(3):
                back = back + dot(dproj[j, kept, mine, :], wa[j, cols, :], (1, 1))
            part[0, s, :, :, :, cols] = out.astype(BF).reshape(chips, 2, R, 256)
            part[1, s, :, :, :, cols] = back.astype(BF).reshape(chips, 2, R, 256)

        half_sends(s)

        run_groups(s, 3)

        @pl.when(s + 1 < S)
        def _():
            end_step(s + 1)

    strip = D // 4

    def strip_of(n):
        return pl.ds(pl.multiple_of(n * strip, strip), strip)

    def tall_copy():
        return pltpu.make_async_copy(tall, tall_out, gs.at[2])

    def wide_copy(n, slot):
        return pltpu.make_async_copy(wide.at[slot], wide_out.at[:, strip_of(n), :], gs.at[slot])

    def output_grads():
        if inside:

            @pl.loop(0, 4)
            def _(n):
                rows = gat[1, :, :, :, :, strip_of(n)].reshape(S * L, strip)
                tall[:, strip_of(n)] = dot(ctx[...].reshape(S * L, local), rows, (0, 0))

            tall_copy().start()

    def attend_grads(n, slot):
        if inside:

            @pl.loop(0, 3)
            def _(j):
                rows = gat[0, :, :, :, :, strip_of(n)].reshape(S * L, strip)
                wide[slot, j] = dot(rows, dproj[j].reshape(S * L, local), (0, 0))

            wide_copy(n, slot).start()

    output_grads()
    p_sends(S - 1)

    @pl.loop(0, 2)
    def _(n):
        attend_grads(n, n)

    sum_tp[t] = jnp.zeros_like(sum_tp[t])

    @pl.loop(0, S)
    def _(s):
        totals = []
        for kind in range(2):
            incoming = parts_in.at[kind, s, pl.ds(0, chips - 1)]
            remote(incoming, incoming, ps.at[kind, s, 0], pr.at[kind, s], here).wait_recv()
            total = part[kind, s, chip, core].astype(F32)
            for d in range(1, chips):
                total = total + parts_in[kind, s, (chip + d) % chips].astype(F32)
            totals.append(total)
        branch, ngrad = totals
        x = stream_ref[:, pl.ds(s, 1), :].reshape(R, D)
        cot = cot_ref[:, pl.ds(s, 1), :].reshape(R, D)
        result_ref[:, pl.ds(s, 1), :] = (x + branch + fbias_ref[...]).reshape(R, 1, D)
        u = unit[s]
        scaled = ngrad * gain_ref[...]
        sgrad_ref[:, pl.ds(s, 1), :] = (
            cot
            + istd[s][:, :1]
            * (
                scaled
                - jnp.mean(scaled, axis=-1, keepdims=True)
                - u * jnp.mean(scaled * u, axis=-1, keepdims=True)
            )
        ).reshape(R, 1, D)
        for i, value in enumerate((ngrad * u, ngrad, cot)):
            sum_tp[t, i] += jnp.sum(value, axis=0, keepdims=True).reshape(D // 128, 128)

    def m_copy(d):
        return remote(sum_tp.at[t], sum_tp.at[t], ms.at[d], mr.at[0], {"tp": (t + d) % TP})

    def n_copy(d):
        return remote(
            sum_seq.at[z], sum_seq.at[z], ms.at[TP + d], mr.at[1], {"seq": (z + d) % Z}
        )

    for d in range(1, TP):
        m_copy(d).start()
    if inside:
        wide_copy(0, 0).wait()
    attend_grads(2, 0)
    same(sum_tp.at[pl.ds(0, TP - 1)], ms.at[0], mr.at[0], here).wait_recv()
    total = sum_tp[0]
    for d in range(1, TP):
        total = total + sum_tp[d]
    sum_seq[z] = total
    for d in range(1, Z):
        n_copy(d).start()
    if inside:
        wide_copy(1, 1).wait()
    attend_grads(3, 1)
    same(sum_seq.at[pl.ds(0, Z - 1)], ms.at[0], mr.at[1], here).wait_recv()
    total = sum_seq[0]
    for d in range(1, Z):
        total = total + sum_seq[d]
    gsum_ref[...], osum_ref[...], fsum_ref[...] = total[0], total[1], total[2]
    ubg_ref[...] = ubg[...].reshape(hidden // 128, 128)

    for d in range(1, TP):
        m_copy(d).wait_send()
    for d in range(1, Z):
        n_copy(d).wait_send()
    for copy in out_copies(S - 1):
        copy.wait()
    if inside:
        tall_copy().wait()
        wide_copy(2, 0).wait()
        wide_copy(3, 1).wait()

    @pl.loop(0, S)
    def _(s):
        drain_gather(s)
        for kind in range(2):
            half_copy(kind, s).wait_send()
            for d in range(1, chips):
                p_copy(kind, s, d).wait_send()


def attention_inside(length):
    return length <= 512


def block_call(stream, cotangent, gain, offset, fbias, abias, ubias, wa, wo, wu, wd, Z, TP):
    R, S, D = stream.shape
    local, hidden = wo.shape[0], wu.shape[1]
    L = Z * TP * R
    chips = TP // 2
    levels = chips.bit_length() - 1
    vm = pl.BlockSpec(memory_space=pltpu.VMEM)
    anywhere = pl.BlockSpec(memory_space=pl.ANY)
    shape = jax.ShapeDtypeStruct
    dma = pltpu.SemaphoreType.DMA
    inside = attention_inside(L)
    kept = S if inside else 1
    return pl.pallas_call(
        functools.partial(block_kernel, (Z, TP, S, R, D)),
        in_specs=[vm] * 7 + [anywhere] * 4,
        out_specs=[anywhere] * 6 + [vm] * 7,
        out_shape=[
            shape((S, Z, TP, R, D), BF),
            shape((S, Z, TP, R, D), BF),
            shape((S, L, hidden), BF),
            shape((S, L, hidden), BF),
            shape((3, D, local), F32) if inside else shape((3, S, L, local), BF),
            shape((local, D), F32) if inside else shape((S, L, local), BF),
            shape((R, S, D), F32),
            shape((R, S, D), F32),
            shape((D // 128, 128), F32),
            shape((D // 128, 128), F32),
            shape((D // 128, 128), F32),
            shape((3, local), F32),
            shape((hidden // 128, 128), F32),
        ],
        scratch_shapes=[
            pltpu.VMEM((2, S, Z, TP, R, D), BF),
            pltpu.VMEM((3, D, local), BF),
            pltpu.VMEM((local, D), BF),
            pltpu.VMEM((D, hidden), BF),
            pltpu.VMEM((hidden, D), BF),
            pltpu.VMEM((S, R, D), F32),
            pltpu.VMEM((S, R, 128), F32),
            pltpu.VMEM((2, L, min(128, local)), F32),
            pltpu.VMEM((3, L, local), F32),
            pltpu.VMEM((L, local), BF),
            pltpu.VMEM((L, hidden), BF),
            pltpu.VMEM((L, hidden), BF),
            pltpu.VMEM((kept, L, local), BF),
            pltpu.VMEM((3, kept, L, local), BF),
            pltpu.VMEM((2, S, chips, 2, R, D), BF),
            pltpu.VMEM((2, S, chips, R, D), BF),
            pltpu.VMEM((2, S, chips, R, D), BF),
            pltpu.VMEM((TP, 3, D // 128, 128), F32),
            pltpu.VMEM((Z, 3, D // 128, 128), F32),
            pltpu.VMEM((1, hidden), F32),
            pltpu.VMEM((2, 3, D // 4, local) if inside else (1, 3, 8, 128), F32),
            pltpu.VMEM((local, D) if inside else (8, 128), F32),
            dma((S, Z)),
            dma((S, Z)),
            dma((S, chips * levels, Z)),
            dma((S, TP, Z)),
            dma((S, chips)),
            dma((S, TP)),
            dma((2, S, chips)),
            dma((2, S)),
            dma((2, S)),
            dma((TP + Z,)),
            dma((2,)),
            dma((4,)),
            dma((6,)),
            dma((3,)),
        ],
        compiler_params=pltpu.CompilerParams(
            collective_id=0, has_side_effects=True, vmem_limit_bytes=67000000
        ),
        name="block",
    )(stream, cotangent, gain, offset, fbias, abias, ubias, wa, wo, wu, wd)


def weight_kernel(steps, inside, normed, grads, pre, wide, hid_hbm, tall, *rest):
    smalls = (len(rest) - 7) // 2
    given, rest = rest[:smalls], rest[smalls:]
    up, attend, down, output = rest[:4]
    handed, (hid, ctx, sem) = rest[4 : 4 + smalls], rest[4 + smalls :]
    i = pl.program_id(0)
    loads = [
        pltpu.make_async_copy(hid_hbm, hid, sem.at[0]),
    ]
    if not inside:
        loads.append(pltpu.make_async_copy(tall, ctx, sem.at[1]))

    @pl.when(i == 0)
    def _():
        for load in loads:
            load.start()
        for source, target in zip(given, handed):
            target[...] = source[...]

    @pl.when(i < steps)
    def _():
        up[...] = dot(normed[...], pre[...], (0, 0))
        if inside:
            attend[...] = wide[...]
        else:
            for j in range(3):
                attend[j] = dot(normed[...], wide[j], (0, 0))

    @pl.when(i == steps)
    def _():
        for load in loads:
            load.wait()

    @pl.when(i >= steps)
    def _():
        down[...] = dot(hid[...], grads[...], (0, 0))
        output[...] = tall[...] if inside else dot(ctx[...], grads[...], (0, 0))


def weight_call(normed, grads, pre, wide, hid, tall, smalls, local, inside):
    tokens, D = normed.shape
    hidden = pre.shape[1]
    tile = 512 if tokens * 512 * 2 <= (2 << 20) else 256
    steps = D // tile
    whole = lambda *shape: pl.BlockSpec(shape, lambda i: (0,) * len(shape), pipeline_mode=pl.Buffered(1))
    first = lambda i: jnp.minimum(i, steps - 1)
    second = lambda i: jnp.maximum(i - steps, 0)
    anywhere = pl.BlockSpec(memory_space=pl.ANY)
    shape = jax.ShapeDtypeStruct
    return pl.pallas_call(
        functools.partial(weight_kernel, steps, inside),
        grid=(2 * steps,),
        in_specs=[
            pl.BlockSpec((tokens, tile), lambda i: (0, first(i))),
            pl.BlockSpec((tokens, tile), lambda i: (0, second(i))),
            whole(tokens, hidden),
            pl.BlockSpec((3, tile, local), lambda i: (0, first(i), 0)) if inside else whole(*wide.shape),
            anywhere,
            pl.BlockSpec((local, tile), lambda i: (0, second(i))) if inside else anywhere,
        ]
        + [whole(*small.shape) for small in smalls],
        out_specs=[
            pl.BlockSpec((tile, hidden), lambda i: (first(i), 0)),
            pl.BlockSpec((3, tile, local), lambda i: (0, first(i), 0)),
            pl.BlockSpec((hidden, tile), lambda i: (0, second(i))),
            pl.BlockSpec((local, tile), lambda i: (0, second(i))),
        ]
        + [whole(*small.shape) for small in smalls],
        out_shape=[
            shape((D, hidden), F32),
            shape((3, D, local), F32),
            shape((hidden, D), F32),
            shape((local, D), F32),
        ]
        + [shape(small.shape, F32) for small in smalls],
        scratch_shapes=[
            pltpu.VMEM((tokens, hidden), BF),
            pltpu.VMEM((16, 128) if inside else (tokens, local), BF),
            pltpu.SemaphoreType.DMA((2,)),
        ],
        compiler_params=pltpu.CompilerParams(vmem_limit_bytes=67000000),
        name="weights",
    )(normed, grads, pre, wide, hid, tall, *smalls)


def per_device(
    stream,
    norm_gain,
    norm_offset,
    attend_weight,
    attend_bias,
    output_weight,
    up_weight,
    up_bias,
    down_weight,
    final_bias,
    cotangent,
):
    R, S, D = stream.shape
    local = attend_weight.shape[2]
    hidden = up_weight.shape[1]
    TP, Z = lax.axis_size("tp"), lax.axis_size("seq")
    tokens = R * S * TP * Z
    inside = attention_inside(R * TP * Z)
    weights = jnp.swapaxes(attend_weight, 0, 1)
    (
        normed, grads, hid, pre, wide, tall, *smalls
    ) = block_call(
        stream, cotangent, norm_gain.reshape(1, D), norm_offset.reshape(1, D),
        final_bias.reshape(1, D), attend_bias, up_bias.reshape(1, hidden),
        weights, output_weight, up_weight, down_weight, Z, TP,
    )
    (
        up_grad, attend_grad, down_grad, output_grad,
        result, stream_grad, gain_grad, offset_grad, fbias_grad, abias_grad, ubias_grad,
    ) = weight_call(
        normed.reshape(tokens, D), grads.reshape(tokens, D), pre.reshape(tokens, hidden),
        wide if inside else wide.reshape(3, tokens, local), hid.reshape(tokens, hidden),
        tall if inside else tall.reshape(tokens, local), smalls, local, inside,
    )
    return (
        result,
        stream_grad,
        gain_grad.reshape(D),
        offset_grad.reshape(D),
        jnp.swapaxes(attend_grad, 0, 1),
        abias_grad,
        output_grad,
        up_grad,
        ubias_grad.reshape(hidden),
        down_grad,
        fbias_grad.reshape(D),
    )


def solution(mesh):
    in_specs = (
        P(("seq", "tp"), None, None),
        P(),
        P(),
        P(None, None, "tp"),
        P(None, "tp"),
        P("tp", None),
        P(None, "tp"),
        P("tp"),
        P("tp", None),
        P(),
        P(("seq", "tp"), None, None),
    )
    out_specs = (
        P(("seq", "tp"), None, None),
        P(("seq", "tp"), None, None),
        P(),
        P(),
        P(None, None, "tp"),
        P(None, "tp"),
        P("tp", None),
        P(None, "tp"),
        P("tp"),
        P("tp", None),
        P(),
    )
    return jax.shard_map(
        per_device, mesh=mesh, in_specs=in_specs, out_specs=out_specs, check_vma=False
    )
```

```python
import functools
import math

import jax
import jax.numpy as jnp
from jax import lax
from jax.experimental import pallas as pl
from jax.experimental.pallas import tpu as pltpu
from jax.sharding import PartitionSpec as P

HEAD_DIM = 64
ROT = 32

EPS = 1e-05
GELU_C = 0.7978845608028654
CUBIC = 0.044715
LOG_BASE = math.log(10000.0)
BF = jnp.bfloat16
F32 = jnp.float32
MESH = pl.DeviceIdType.MESH


def gelu_parts(pre_act):
    inner_arg = GELU_C * (pre_act + CUBIC * pre_act * pre_act * pre_act)
    tanh_value = jnp.tanh(inner_arg)
    gelu_value = 0.5 * pre_act * (1.0 + tanh_value)
    gelu_slope = 0.5 * (1.0 + tanh_value) + 0.5 * pre_act * (
        1.0 - tanh_value * tanh_value
    ) * GELU_C * (1.0 + 3.0 * CUBIC * pre_act * pre_act)
    return (gelu_value, gelu_slope)


def dot(a, b, dims):
    return lax.dot_general(a, b, ((dims[:1], dims[1:]), ((), ())), preferred_element_type=F32)


def flip(index, bit):
    return index + bit - 2 * bit * ((index // bit) % 2)


def flip_all(index, mask):
    bit = 1
    while bit <= mask:
        if mask & bit:
            index = flip(index, bit)
        bit *= 2
    return index


def head_pass(q_all, k_all, v_all, g_all, heads, block=256):
    length, width = q_all.shape
    scale = jnp.asarray(HEAD_DIM ** (-0.5), BF)
    block = min(block, length)
    lane = lax.broadcasted_iota(jnp.int32, (1, width), 1) // HEAD_DIM
    zero = jnp.zeros((), BF)
    parts = [(start, head) for start in range(0, length, block) for head in range(heads)]

    def masked(x, start, head):
        return jnp.where(lane == head, x[start : start + block], zero)

    qs = [masked(q_all, a, h) * scale for a, h in parts]
    gs = [masked(g_all, a, h) for a, h in parts]

    def weights(s, start):
        diag = s[:, start:]
        row = lax.broadcasted_iota(jnp.int32, diag.shape, 0)
        col = lax.broadcasted_iota(jnp.int32, diag.shape, 1)
        diag = jnp.where(row >= col, diag, -jnp.inf)
        s = diag if start == 0 else jnp.concatenate([s[:, :start], diag], axis=1)
        p = jnp.exp(s - jnp.max(s, axis=1, keepdims=True))
        return p * (1.0 / jnp.sum(p, axis=1, keepdims=True))

    cs, dqs, dks, dvs = [], [], [], []
    together = len(parts) if length <= 512 else heads
    for first in range(0, len(parts), together):
        group = slice(first, first + together)
        stops = [a + block for a, h in parts[group]]
        gq, gg = qs[group], gs[group]
        ss = [dot(q, k_all[:n], (1, 1)) for q, n in zip(gq, stops)]
        dps = [dot(g, v_all[:n], (1, 1)) for g, n in zip(gg, stops)]
        ps = [weights(s, a) for s, (a, h) in zip(ss, parts[group])]
        pbs = [p.astype(BF) for p in ps]
        gc = [dot(p, v_all[:n], (1, 0)).astype(BF) for p, n in zip(pbs, stops)]
        dvs += [dot(g, p, (0, 0)) for g, p in zip(gg, pbs)]
        deltas = [
            jnp.sum(g.astype(F32) * c.astype(F32), axis=1, keepdims=True) for g, c in zip(gg, gc)
        ]
        dss = [(p * (dp - delta)).astype(BF) for p, dp, delta in zip(ps, dps, deltas)]
        dqs += [dot(ds, k_all[:n], (1, 0)) for ds, n in zip(dss, stops)]
        dks += [dot(q, ds, (0, 0)) for q, ds in zip(gq, dss)]
        cs += gc

    def rows(values):
        blocks = []
        for n in range(0, len(parts), heads):
            value = values[n]
            for h in range(1, heads):
                value = jnp.where(lane == h, values[n + h], value)
            blocks.append(value)
        return jnp.concatenate(blocks, axis=0)

    def columns(values):
        total = None
        for n in range(0, len(parts), heads):
            value = values[n]
            for h in range(1, heads):
                value = value + values[n + h]
            if total is None:
                total = value
            else:
                old = total.shape[1]
                total = jnp.concatenate([total + value[:, :old], value[:, old:]], axis=1)
        return total.T

    return [rows(cs), rows(dqs) * scale.astype(F32), columns(dks), columns(dvs)]


def block_kernel(
    dims,
    stream_ref, cot_ref, gain_ref, offset_ref, fbias_ref, abias_ref, ubias_ref,
    wa_hbm, wo_hbm, wu_hbm, wd_hbm,
    norm_out, grad_out, hid_out, pre_out, wide_out, tall_out,
    result_ref, sgrad_ref, gsum_ref, osum_ref, fsum_ref, abg_ref, ubg_ref,
    gat, wa, wo, wu, wd, unit, istd, table, proj, cgrad, hid, pre, ctx, dproj,
    part, half_in, parts_in, sum_tp, sum_seq, ubg, wide, tall,
    zs, zr, xs, xr, fs, fr, ps, hr, pr, ms, mr, ws, os, gs,
):
    Z, TP, S, R, D = dims
    z, t = lax.axis_index("seq"), lax.axis_index("tp")
    chip, core = t // 2, t % 2
    chips = TP // 2
    levels = chips.bit_length() - 1
    bits = [
        (1 - core) * (1 << i) + core * (1 << (levels - 1 - i)) for i in range(levels)
    ]
    partner = chip * 2 + 1 - core
    L = Z * TP * R
    local = wo.shape[0]
    hidden = wu.shape[1]
    pair = min(128, local)
    own_rows = TP * R
    inside = ctx.shape[0] == S

    loads = [
        pltpu.make_async_copy(src, dst, ws.at[i])
        for i, (src, dst) in enumerate(((wa_hbm, wa), (wo_hbm, wo), (wu_hbm, wu), (wd_hbm, wd)))
    ]
    for load in loads:
        load.start()
    barrier = pltpu.get_barrier_semaphore()
    for d in range(1, TP):
        pl.semaphore_signal(barrier, inc=1, device_id={"tp": (t + d) % TP}, device_id_type=MESH)
    for d in range(1, Z):
        pl.semaphore_signal(barrier, inc=1, device_id={"seq": (z + d) % Z}, device_id_type=MESH)

    def normalize(s):
        x = stream_ref[:, pl.ds(s, 1), :].reshape(R, D)
        mean = jnp.mean(x, axis=-1, keepdims=True)
        centred = x - mean
        inv = lax.rsqrt(jnp.mean(centred * centred, axis=-1, keepdims=True) + EPS)
        u = centred * inv
        unit[s] = u
        istd[s] = jnp.broadcast_to(inv, (R, 128))
        gat[0, s, z, t] = (u * gain_ref[...] + offset_ref[...]).astype(BF)
        gat[1, s, z, t] = cot_ref[:, pl.ds(s, 1), :].reshape(R, D).astype(BF)

    normalize(0)
    pl.semaphore_wait(barrier, TP + Z - 2)

    def remote(src, dst, ssem, rsem, dev):
        return pltpu.make_async_remote_copy(
            src_ref=src, dst_ref=dst, send_sem=ssem, recv_sem=rsem,
            device_id=dev, device_id_type=MESH,
        )

    def same(ref, ssem, rsem, dev):
        return remote(ref, ref, ssem, rsem, dev)

    def unit_of(s, zz, tt):
        return gat.at[:, s, zz, tt]

    def column(s, tt):
        return gat.at[:, s, :, tt]

    here = {"tp": t}
    other = [z] + [flip_all(z, r) if Z & (Z - 1) == 0 else (z + r) % Z for r in range(1, Z)]
    sender = [z] + [flip_all(z, r) if Z & (Z - 1) == 0 else (z + Z - r) % Z for r in range(1, Z)]

    def z_copy(s, r):
        return same(unit_of(s, z, t), zs.at[s, r], zr.at[s, z], {"seq": other[r]})

    def z_sends(s):
        for r in range(1, Z):
            z_copy(s, r).start()

    def x_copy(s, r, src, slot, i):
        return same(
            unit_of(s, sender[r], src), xs.at[s, slot, r], xr.at[s, src, sender[r]],
            {"tp": flip(chip, bits[i]) * 2 + core},
        )

    def f_copy(s, src, r):
        return same(column(s, src), fs.at[s, r], fr.at[s, src], {"tp": partner})

    def source(mask):
        c = chip
        for i in range(levels):
            if (mask >> i) & 1:
                c = flip(c, bits[i])
        return c * 2 + core

    order = sorted(range(1, chips), key=lambda m: (bin(m).count("1"), m))

    def later(mask):
        first = mask.bit_length()
        return [(mask * levels + i, i) for i in range(first, levels)]

    def own_unit(s, r):
        if r > 0:
            zz = sender[r]
            same(unit_of(s, zz, t), zs.at[s, 0], zr.at[s, zz], here).wait_recv()
        for slot, i in later(0):
            x_copy(s, r, t, slot, i).start()
        if r == Z - 1:
            f_copy(s, t, 0).start()

    def pass_unit(s, r, level):
        for mask in order:
            if bin(mask).count("1") != level:
                continue
            src = source(mask)
            same(unit_of(s, sender[r], src), zs.at[s, 0], xr.at[s, src, sender[r]], here).wait_recv()
            for slot, i in later(mask):
                x_copy(s, r, src, slot, i).start()
            if r == Z - 1:
                f_copy(s, src, mask).start()

    def end_step(s):
        for c in range(chips):
            src = ((chip + c) % chips) * 2 + 1 - core
            same(column(s, src), zs.at[s, 0], fr.at[s, src], here).wait_recv()

    def drain_gather(s):
        for r in range(1, Z):
            z_copy(s, r).wait_send()
        for mask in [0] + order:
            src = source(mask)
            for slot, i in later(mask):
                for r in range(Z):
                    x_copy(s, r, src, slot, i).wait_send()
            f_copy(s, src, mask).wait_send()

    def half_copy(kind, s):
        return remote(
            part.at[kind, s, :, 1 - core], half_in.at[kind, s], ps.at[kind, s, 0], hr.at[kind, s],
            {"tp": partner},
        )

    def p_copy(kind, s, d):
        to = (chip + d) % chips
        return remote(
            part.at[kind, s, to, core], parts_in.at[kind, s, chip], ps.at[kind, s, d],
            pr.at[kind, s], {"tp": to * 2 + core},
        )

    def half_sends(s):
        for kind in range(2):
            half_copy(kind, s).start()

    def p_sends(s):
        for kind in range(2):
            half_copy(kind, s).wait_recv()
            for d in range(chips):
                c = (chip + d) % chips
                part[kind, s, c, core] = (
                    part[kind, s, c, core].astype(F32) + half_in[kind, s, c].astype(F32)
                ).astype(BF)
            for d in range(1, chips):
                p_copy(kind, s, d).start()

    def out_copies(s):
        pairs = [
            (gat.at[0, s], norm_out.at[s]), (gat.at[1, s], grad_out.at[s]),
            (hid, hid_out.at[s]), (pre, pre_out.at[s]),
        ]
        if not inside:
            pairs += [(ctx.at[0], tall_out.at[s]), (dproj.at[:, 0], wide_out.at[:, s])]
        return [pltpu.make_async_copy(src, dst, os.at[i]) for i, (src, dst) in enumerate(pairs)]

    def group_steps(n):
        steps = []
        if n % Z == 1:
            steps.append((n // Z + 1, z_sends))
        for level in range(levels + 1):
            m = n - 2 * level
            if m > 0 and level == 0:
                steps.append((m // Z, functools.partial(own_unit, r=m % Z)))
            elif m >= 0 and level > 0:
                steps.append((m // Z, functools.partial(pass_unit, r=m % Z, level=level)))
        return steps

    lead = 2 * levels

    def run_groups(s, part):
        steps = [step for k in range(Z) for step in group_steps(Z + lead + k)]
        for i, step in steps[len(steps) * part // 8 : len(steps) * (part + 1) // 8]:

            @pl.when(s + i < S)
            def _(step=step, i=i):
                step(s + i)

    z_sends(0)
    own_unit(0, 0)

    @pl.loop(1, S)
    def _(s):
        normalize(s)

    lane = lax.broadcasted_iota(jnp.int32, (L, pair), 1) % HEAD_DIM
    place = lax.broadcasted_iota(jnp.int32, (L, pair), 0).astype(F32)
    half = ROT // 2
    freq = jnp.exp((lane % half).astype(F32) * (-2.0 * LOG_BASE / ROT))
    angle = place * freq
    cosine, sine = jnp.cos(angle), jnp.sin(angle)
    table[0] = jnp.where(lane < ROT, cosine, 1.0)
    table[1] = jnp.where(lane < half, -sine, jnp.where(lane < ROT, sine, 0.0))
    abg_ref[...] = jnp.zeros_like(abg_ref)
    ubg[...] = jnp.zeros_like(ubg)
    sum_tp[t] = jnp.zeros_like(sum_tp[t])
    for load in loads:
        load.wait()

    for n in range(1, Z + lead):
        for i, step in group_steps(n):
            if i < S:
                step(i)
    end_step(0)

    def finish_sequence(s):
        totals = []
        for kind in range(2):
            incoming = parts_in.at[kind, s, pl.ds(0, chips - 1)]
            remote(incoming, incoming, ps.at[kind, s, 0], pr.at[kind, s], here).wait_recv()
            total = part[kind, s, chip, core].astype(F32)
            for d in range(1, chips):
                total = total + parts_in[kind, s, (chip + d) % chips].astype(F32)
            totals.append(total)
        branch, ngrad = totals
        x = stream_ref[:, pl.ds(s, 1), :].reshape(R, D)
        cot = cot_ref[:, pl.ds(s, 1), :].reshape(R, D)
        result_ref[:, pl.ds(s, 1), :] = (x + branch + fbias_ref[...]).reshape(R, 1, D)
        u = unit[s]
        scaled = ngrad * gain_ref[...]
        sgrad_ref[:, pl.ds(s, 1), :] = (
            cot
            + istd[s][:, :1]
            * (
                scaled
                - jnp.mean(scaled, axis=-1, keepdims=True)
                - u * jnp.mean(scaled * u, axis=-1, keepdims=True)
            )
        ).reshape(R, 1, D)
        for i, value in enumerate((ngrad * u, ngrad, cot)):
            sum_tp[t, i] += jnp.sum(value, axis=0, keepdims=True).reshape(D // 128, 128)

    def turned(x, sign):
        first = lax.broadcasted_iota(jnp.int32, (1, pair), 1) % HEAD_DIM < half
        crossed = jnp.where(first, pltpu.roll(x, pair - half, 1), pltpu.roll(x, half, 1))
        return x * table[0] + sign * (crossed * table[1])

    @pl.loop(0, S)
    def _(s):
        kept = s if inside else 0

        def rows_n():
            return gat[0, s].reshape(L, D)

        def rows_g():
            return gat[1, s].reshape(L, D)

        @pl.when(s > 0)
        def _():
            for copy in out_copies(s - 1):
                copy.wait()

        @pl.loop(0, 3)
        def _(j):
            proj[j] = dot(rows_n(), wa[j], (1, 0)) + abias_ref[pl.ds(j, 1), :]

        cgrad[...] = dot(rows_g(), wo[...], (1, 1)).astype(BF)

        @pl.when(s > 0)
        def _():
            p_sends(s - 1)

        run_groups(s, 0)

        @pl.loop(0, local // pair)
        def _(h):
            lanes = pl.ds(pl.multiple_of(h * pair, pair), pair)
            q = turned(proj[0, :, lanes], 1.0).astype(BF)
            k = turned(proj[1, :, lanes], 1.0).astype(BF)
            v = proj[2, :, lanes].astype(BF)
            c, dq, dk, dv = head_pass(q, k, v, cgrad[:, lanes], pair // HEAD_DIM)
            ctx[kept, :, lanes] = c
            for j, value in enumerate((turned(dq, -1.0), turned(dk, -1.0), dv)):
                dproj[j, kept, :, lanes] = value.astype(BF)
                abg_ref[j : j + 1, lanes] += jnp.sum(value, axis=0, keepdims=True)

            @pl.when(h == 0)
            def _():
                run_groups(s, 1)

        run_groups(s, 2)
        tile = min(hidden, 512 if L <= 512 else 128)
        tiles = hidden // tile

        def feed_forward(n):
            cols = pl.ds(pl.multiple_of(n * tile, tile), tile)
            value, slope = gelu_parts(dot(rows_n(), wu[:, cols], (1, 0)) + ubias_ref[:, cols])
            hid[:, cols] = value.astype(BF)
            grad = dot(rows_g(), wd[cols, :], (1, 1)) * slope
            pre[:, cols] = grad.astype(BF)
            ubg[:, cols] += jnp.sum(grad, axis=0, keepdims=True)

        @pl.loop(0, tiles)
        def _(n):
            feed_forward(n)

            for q in range(tiles):

                @pl.when(n == q)
                def _(q=q):
                    for part in range(4 * q // tiles, 4 * (q + 1) // tiles):
                        run_groups(s, 3 + part)

        for copy in out_copies(s):
            copy.start()

        mine = pl.ds(pl.multiple_of(z * own_rows, own_rows), own_rows)

        @pl.loop(0, D // 256)
        def _(n):
            cols = pl.ds(pl.multiple_of(n * 256, 256), 256)
            out = dot(ctx[kept, mine, :], wo[:, cols], (1, 0)) + dot(hid[mine, :], wd[:, cols], (1, 0))
            back = dot(pre[mine, :], wu[cols, :], (1, 1))
            for j in range(3):
                back = back + dot(dproj[j, kept, mine, :], wa[j, cols, :], (1, 1))
            part[0, s, :, :, :, cols] = out.astype(BF).reshape(chips, 2, R, 256)
            part[1, s, :, :, :, cols] = back.astype(BF).reshape(chips, 2, R, 256)

        half_sends(s)

        run_groups(s, 7)

        @pl.when(s >= 2)
        def _():
            finish_sequence(s - 2)

        @pl.when(s + 1 < S)
        def _():
            end_step(s + 1)

    strip = D // 4

    def strip_of(n):
        return pl.ds(pl.multiple_of(n * strip, strip), strip)

    def tall_copy():
        return pltpu.make_async_copy(tall, tall_out, gs.at[2])

    def wide_copy(n, slot):
        return pltpu.make_async_copy(wide.at[slot], wide_out.at[:, strip_of(n), :], gs.at[slot])

    def output_grads():
        if inside:

            @pl.loop(0, 4)
            def _(n):
                rows = gat[1, :, :, :, :, strip_of(n)].reshape(S * L, strip)
                tall[:, strip_of(n)] = dot(ctx[...].reshape(S * L, local), rows, (0, 0))

            tall_copy().start()

    def attend_grads(n, slot):
        if inside:

            @pl.loop(0, 3)
            def _(j):
                rows = gat[0, :, :, :, :, strip_of(n)].reshape(S * L, strip)
                wide[slot, j] = dot(rows, dproj[j].reshape(S * L, local), (0, 0))

            wide_copy(n, slot).start()

    output_grads()
    p_sends(S - 1)

    @pl.loop(0, 2)
    def _(n):
        attend_grads(n, n)

    @pl.loop(max(0, S - 2), S)
    def _(s):
        finish_sequence(s)

    def m_copy(d):
        return remote(sum_tp.at[t], sum_tp.at[t], ms.at[d], mr.at[0], {"tp": (t + d) % TP})

    def n_copy(d):
        return remote(
            sum_seq.at[z], sum_seq.at[z], ms.at[TP + d], mr.at[1], {"seq": (z + d) % Z}
        )

    for d in range(1, TP):
        m_copy(d).start()
    if inside:
        wide_copy(0, 0).wait()
    attend_grads(2, 0)
    same(sum_tp.at[pl.ds(0, TP - 1)], ms.at[0], mr.at[0], here).wait_recv()
    total = sum_tp[0]
    for d in range(1, TP):
        total = total + sum_tp[d]
    sum_seq[z] = total
    for d in range(1, Z):
        n_copy(d).start()
    if inside:
        wide_copy(1, 1).wait()
    attend_grads(3, 1)
    same(sum_seq.at[pl.ds(0, Z - 1)], ms.at[0], mr.at[1], here).wait_recv()
    total = sum_seq[0]
    for d in range(1, Z):
        total = total + sum_seq[d]
    gsum_ref[...], osum_ref[...], fsum_ref[...] = total[0], total[1], total[2]
    ubg_ref[...] = ubg[...].reshape(hidden // 128, 128)

    for d in range(1, TP):
        m_copy(d).wait_send()
    for d in range(1, Z):
        n_copy(d).wait_send()
    for copy in out_copies(S - 1):
        copy.wait()
    if inside:
        tall_copy().wait()
        wide_copy(2, 0).wait()
        wide_copy(3, 1).wait()

    @pl.loop(0, S)
    def _(s):
        drain_gather(s)
        for kind in range(2):
            half_copy(kind, s).wait_send()
            for d in range(1, chips):
                p_copy(kind, s, d).wait_send()


def attention_inside(length):
    return length <= 512


def block_call(stream, cotangent, gain, offset, fbias, abias, ubias, wa, wo, wu, wd, Z, TP):
    R, S, D = stream.shape
    local, hidden = wo.shape[0], wu.shape[1]
    L = Z * TP * R
    chips = TP // 2
    levels = chips.bit_length() - 1
    vm = pl.BlockSpec(memory_space=pltpu.VMEM)
    anywhere = pl.BlockSpec(memory_space=pl.ANY)
    shape = jax.ShapeDtypeStruct
    dma = pltpu.SemaphoreType.DMA
    inside = attention_inside(L)
    kept = S if inside else 1
    return pl.pallas_call(
        functools.partial(block_kernel, (Z, TP, S, R, D)),
        in_specs=[vm] * 7 + [anywhere] * 4,
        out_specs=[anywhere] * 6 + [vm] * 7,
        out_shape=[
            shape((S, Z, TP, R, D), BF),
            shape((S, Z, TP, R, D), BF),
            shape((S, L, hidden), BF),
            shape((S, L, hidden), BF),
            shape((3, D, local), F32) if inside else shape((3, S, L, local), BF),
            shape((local, D), F32) if inside else shape((S, L, local), BF),
            shape((R, S, D), F32),
            shape((R, S, D), F32),
            shape((D // 128, 128), F32),
            shape((D // 128, 128), F32),
            shape((D // 128, 128), F32),
            shape((3, local), F32),
            shape((hidden // 128, 128), F32),
        ],
        scratch_shapes=[
            pltpu.VMEM((2, S, Z, TP, R, D), BF),
            pltpu.VMEM((3, D, local), BF),
            pltpu.VMEM((local, D), BF),
            pltpu.VMEM((D, hidden), BF),
            pltpu.VMEM((hidden, D), BF),
            pltpu.VMEM((S, R, D), F32),
            pltpu.VMEM((S, R, 128), F32),
            pltpu.VMEM((2, L, min(128, local)), F32),
            pltpu.VMEM((3, L, local), F32),
            pltpu.VMEM((L, local), BF),
            pltpu.VMEM((L, hidden), BF),
            pltpu.VMEM((L, hidden), BF),
            pltpu.VMEM((kept, L, local), BF),
            pltpu.VMEM((3, kept, L, local), BF),
            pltpu.VMEM((2, S, chips, 2, R, D), BF),
            pltpu.VMEM((2, S, chips, R, D), BF),
            pltpu.VMEM((2, S, chips, R, D), BF),
            pltpu.VMEM((TP, 3, D // 128, 128), F32),
            pltpu.VMEM((Z, 3, D // 128, 128), F32),
            pltpu.VMEM((1, hidden), F32),
            pltpu.VMEM((2, 3, D // 4, local) if inside else (1, 3, 8, 128), F32),
            pltpu.VMEM((local, D) if inside else (8, 128), F32),
            dma((S, Z)),
            dma((S, Z)),
            dma((S, chips * levels, Z)),
            dma((S, TP, Z)),
            dma((S, chips)),
            dma((S, TP)),
            dma((2, S, chips)),
            dma((2, S)),
            dma((2, S)),
            dma((TP + Z,)),
            dma((2,)),
            dma((4,)),
            dma((6,)),
            dma((3,)),
        ],
        compiler_params=pltpu.CompilerParams(
            collective_id=0, has_side_effects=True, vmem_limit_bytes=67000000
        ),
        name="block",
    )(stream, cotangent, gain, offset, fbias, abias, ubias, wa, wo, wu, wd)


def weight_kernel(steps, inside, normed, grads, pre, wide, hid_hbm, tall, *rest):
    smalls = (len(rest) - 7) // 2
    given, rest = rest[:smalls], rest[smalls:]
    up, attend, down, output = rest[:4]
    handed, (hid, ctx, sem) = rest[4 : 4 + smalls], rest[4 + smalls :]
    i = pl.program_id(0)
    loads = [
        pltpu.make_async_copy(hid_hbm, hid, sem.at[0]),
    ]
    if not inside:
        loads.append(pltpu.make_async_copy(tall, ctx, sem.at[1]))

    @pl.when(i == 0)
    def _():
        for load in loads:
            load.start()
        for source, target in zip(given, handed):
            target[...] = source[...]

    @pl.when(i < steps)
    def _():
        up[...] = dot(normed[...], pre[...], (0, 0))
        if inside:
            attend[...] = wide[...]
        else:
            for j in range(3):
                attend[j] = dot(normed[...], wide[j], (0, 0))

    @pl.when(i == steps)
    def _():
        for load in loads:
            load.wait()

    @pl.when(i >= steps)
    def _():
        down[...] = dot(hid[...], grads[...], (0, 0))
        output[...] = tall[...] if inside else dot(ctx[...], grads[...], (0, 0))


def weight_call(normed, grads, pre, wide, hid, tall, smalls, local, inside):
    tokens, D = normed.shape
    hidden = pre.shape[1]
    tile = 512 if tokens * 512 * 2 <= (2 << 20) else 256
    steps = D // tile
    whole = lambda *shape: pl.BlockSpec(shape, lambda i: (0,) * len(shape), pipeline_mode=pl.Buffered(1))
    first = lambda i: jnp.minimum(i, steps - 1)
    second = lambda i: jnp.maximum(i - steps, 0)
    anywhere = pl.BlockSpec(memory_space=pl.ANY)
    shape = jax.ShapeDtypeStruct
    return pl.pallas_call(
        functools.partial(weight_kernel, steps, inside),
        grid=(2 * steps,),
        in_specs=[
            pl.BlockSpec((tokens, tile), lambda i: (0, first(i))),
            pl.BlockSpec((tokens, tile), lambda i: (0, second(i))),
            whole(tokens, hidden),
            pl.BlockSpec((3, tile, local), lambda i: (0, first(i), 0)) if inside else whole(*wide.shape),
            anywhere,
            pl.BlockSpec((local, tile), lambda i: (0, second(i))) if inside else anywhere,
        ]
        + [whole(*small.shape) for small in smalls],
        out_specs=[
            pl.BlockSpec((tile, hidden), lambda i: (first(i), 0)),
            pl.BlockSpec((3, tile, local), lambda i: (0, first(i), 0)),
            pl.BlockSpec((hidden, tile), lambda i: (0, second(i))),
            pl.BlockSpec((local, tile), lambda i: (0, second(i))),
        ]
        + [whole(*small.shape) for small in smalls],
        out_shape=[
            shape((D, hidden), F32),
            shape((3, D, local), F32),
            shape((hidden, D), F32),
            shape((local, D), F32),
        ]
        + [shape(small.shape, F32) for small in smalls],
        scratch_shapes=[
            pltpu.VMEM((tokens, hidden), BF),
            pltpu.VMEM((16, 128) if inside else (tokens, local), BF),
            pltpu.SemaphoreType.DMA((2,)),
        ],
        compiler_params=pltpu.CompilerParams(vmem_limit_bytes=67000000),
        name="weights",
    )(normed, grads, pre, wide, hid, tall, *smalls)


def per_device(
    stream,
    norm_gain,
    norm_offset,
    attend_weight,
    attend_bias,
    output_weight,
    up_weight,
    up_bias,
    down_weight,
    final_bias,
    cotangent,
):
    R, S, D = stream.shape
    local = attend_weight.shape[2]
    hidden = up_weight.shape[1]
    TP, Z = lax.axis_size("tp"), lax.axis_size("seq")
    tokens = R * S * TP * Z
    inside = attention_inside(R * TP * Z)
    weights = jnp.swapaxes(attend_weight, 0, 1)
    (
        normed, grads, hid, pre, wide, tall, *smalls
    ) = block_call(
        stream, cotangent, norm_gain.reshape(1, D), norm_offset.reshape(1, D),
        final_bias.reshape(1, D), attend_bias, up_bias.reshape(1, hidden),
        weights, output_weight, up_weight, down_weight, Z, TP,
    )
    (
        up_grad, attend_grad, down_grad, output_grad,
        result, stream_grad, gain_grad, offset_grad, fbias_grad, abias_grad, ubias_grad,
    ) = weight_call(
        normed.reshape(tokens, D), grads.reshape(tokens, D), pre.reshape(tokens, hidden),
        wide if inside else wide.reshape(3, tokens, local), hid.reshape(tokens, hidden),
        tall if inside else tall.reshape(tokens, local), smalls, local, inside,
    )
    return (
        result,
        stream_grad,
        gain_grad.reshape(D),
        offset_grad.reshape(D),
        jnp.swapaxes(attend_grad, 0, 1),
        abias_grad,
        output_grad,
        up_grad,
        ubias_grad.reshape(hidden),
        down_grad,
        fbias_grad.reshape(D),
    )


def solution(mesh):
    in_specs = (
        P(("seq", "tp"), None, None),
        P(),
        P(),
        P(None, None, "tp"),
        P(None, "tp"),
        P("tp", None),
        P(None, "tp"),
        P("tp"),
        P("tp", None),
        P(),
        P(("seq", "tp"), None, None),
    )
    out_specs = (
        P(("seq", "tp"), None, None),
        P(("seq", "tp"), None, None),
        P(),
        P(),
        P(None, None, "tp"),
        P(None, "tp"),
        P("tp", None),
        P(None, "tp"),
        P("tp"),
        P("tp", None),
        P(),
    )
    return jax.shard_map(
        per_device, mesh=mesh, in_specs=in_specs, out_specs=out_specs, check_vma=False
    )
```

```python
import functools
import math

import jax
import jax.numpy as jnp
from jax import lax
from jax.experimental import pallas as pl
from jax.experimental.pallas import tpu as pltpu
from jax.sharding import PartitionSpec as P

HEAD_DIM = 64
ROT = 32

EPS = 1e-05
GELU_C = 0.7978845608028654
CUBIC = 0.044715
LOG_BASE = math.log(10000.0)
BF = jnp.bfloat16
F32 = jnp.float32
MESH = pl.DeviceIdType.MESH


def gelu_parts(pre_act):
    inner_arg = GELU_C * (pre_act + CUBIC * pre_act * pre_act * pre_act)
    tanh_value = jnp.tanh(inner_arg)
    gelu_value = 0.5 * pre_act * (1.0 + tanh_value)
    gelu_slope = 0.5 * (1.0 + tanh_value) + 0.5 * pre_act * (
        1.0 - tanh_value * tanh_value
    ) * GELU_C * (1.0 + 3.0 * CUBIC * pre_act * pre_act)
    return (gelu_value, gelu_slope)


def dot(a, b, dims):
    return lax.dot_general(a, b, ((dims[:1], dims[1:]), ((), ())), preferred_element_type=F32)


def flip(index, bit):
    return index + bit - 2 * bit * ((index // bit) % 2)


def flip_all(index, mask):
    bit = 1
    while bit <= mask:
        if mask & bit:
            index = flip(index, bit)
        bit *= 2
    return index


def head_pass(q_all, k_all, v_all, g_all, heads, block=256):
    length, width = q_all.shape
    scale = jnp.asarray(HEAD_DIM ** (-0.5), BF)
    block = min(block, length)
    lane = lax.broadcasted_iota(jnp.int32, (1, width), 1) // HEAD_DIM
    zero = jnp.zeros((), BF)
    parts = [(start, head) for start in range(0, length, block) for head in range(heads)]

    def masked(x, start, head):
        return jnp.where(lane == head, x[start : start + block], zero)

    qs = [masked(q_all, a, h) * scale for a, h in parts]
    gs = [masked(g_all, a, h) for a, h in parts]

    def weights(s, start):
        diag = s[:, start:]
        row = lax.broadcasted_iota(jnp.int32, diag.shape, 0)
        col = lax.broadcasted_iota(jnp.int32, diag.shape, 1)
        diag = jnp.where(row >= col, diag, -jnp.inf)
        s = diag if start == 0 else jnp.concatenate([s[:, :start], diag], axis=1)
        p = jnp.exp(s - jnp.max(s, axis=1, keepdims=True))
        return p * (1.0 / jnp.sum(p, axis=1, keepdims=True))

    cs, dqs, dks, dvs = [], [], [], []
    together = len(parts) if length <= 512 else heads
    for first in range(0, len(parts), together):
        group = slice(first, first + together)
        stops = [a + block for a, h in parts[group]]
        gq, gg = qs[group], gs[group]
        ss = [dot(q, k_all[:n], (1, 1)) for q, n in zip(gq, stops)]
        dps = [dot(g, v_all[:n], (1, 1)) for g, n in zip(gg, stops)]
        ps = [weights(s, a) for s, (a, h) in zip(ss, parts[group])]
        pbs = [p.astype(BF) for p in ps]
        gc = [dot(p, v_all[:n], (1, 0)).astype(BF) for p, n in zip(pbs, stops)]
        dvs += [dot(g, p, (0, 0)) for g, p in zip(gg, pbs)]
        deltas = [
            jnp.sum(g.astype(F32) * c.astype(F32), axis=1, keepdims=True) for g, c in zip(gg, gc)
        ]
        dss = [(p * (dp - delta)).astype(BF) for p, dp, delta in zip(ps, dps, deltas)]
        dqs += [dot(ds, k_all[:n], (1, 0)) for ds, n in zip(dss, stops)]
        dks += [dot(q, ds, (0, 0)) for q, ds in zip(gq, dss)]
        cs += gc

    def rows(values):
        blocks = []
        for n in range(0, len(parts), heads):
            value = values[n]
            for h in range(1, heads):
                value = jnp.where(lane == h, values[n + h], value)
            blocks.append(value)
        return jnp.concatenate(blocks, axis=0)

    def columns(values):
        total = None
        for n in range(0, len(parts), heads):
            value = values[n]
            for h in range(1, heads):
                value = value + values[n + h]
            if total is None:
                total = value
            else:
                old = total.shape[1]
                total = jnp.concatenate([total + value[:, :old], value[:, old:]], axis=1)
        return total.T

    return [rows(cs), rows(dqs) * scale.astype(F32), columns(dks), columns(dvs)]


def block_kernel(
    dims,
    stream_ref, cot_ref, gain_ref, offset_ref, fbias_ref, abias_ref, ubias_ref,
    wa_hbm, wo_hbm, wu_hbm, wd_hbm,
    norm_out, grad_out, hid_out, pre_out, wide_out, tall_out,
    result_ref, sgrad_ref, gsum_ref, osum_ref, fsum_ref, abg_ref, ubg_ref,
    gat, wa, wo, wu, wd, unit, istd, table, proj, cgrad, hid, pre, ctx, dproj,
    part, half_in, parts_in, sum_tp, sum_seq, ubg, wide, tall,
    zs, zr, xs, xr, fs, fr, ps, hr, pr, ms, mr, ws, os, gs,
):
    Z, TP, S, R, D = dims
    z, t = lax.axis_index("seq"), lax.axis_index("tp")
    chip, core = t // 2, t % 2
    chips = TP // 2
    levels = chips.bit_length() - 1
    bits = [
        (1 - core) * (1 << i) + core * (1 << (levels - 1 - i)) for i in range(levels)
    ]
    partner = chip * 2 + 1 - core
    L = Z * TP * R
    local = wo.shape[0]
    hidden = wu.shape[1]
    pair = min(128, local)
    own_rows = TP * R
    inside = ctx.shape[0] == S

    loads = [
        pltpu.make_async_copy(src, dst, ws.at[i])
        for i, (src, dst) in enumerate(((wo_hbm, wo), (wu_hbm, wu), (wd_hbm, wd)))
    ] + [
        pltpu.make_async_copy(wa_hbm.at[j], wa.at[:, pl.ds(j * wo.shape[0], wo.shape[0])], ws.at[3 + j])
        for j in range(3)
    ]
    for load in loads:
        load.start()
    barrier = pltpu.get_barrier_semaphore()
    for d in range(1, TP):
        pl.semaphore_signal(barrier, inc=1, device_id={"tp": (t + d) % TP}, device_id_type=MESH)
    for d in range(1, Z):
        pl.semaphore_signal(barrier, inc=1, device_id={"seq": (z + d) % Z}, device_id_type=MESH)

    def normalize(s):
        x = stream_ref[:, pl.ds(s, 1), :].reshape(R, D)
        mean = jnp.mean(x, axis=-1, keepdims=True)
        centred = x - mean
        inv = lax.rsqrt(jnp.mean(centred * centred, axis=-1, keepdims=True) + EPS)
        u = centred * inv
        unit[s] = u
        istd[s] = jnp.broadcast_to(inv, (R, 128))
        gat[0, s, z, t] = (u * gain_ref[...] + offset_ref[...]).astype(BF)
        gat[1, s, z, t] = cot_ref[:, pl.ds(s, 1), :].reshape(R, D).astype(BF)

    normalize(0)
    pl.semaphore_wait(barrier, TP + Z - 2)

    def remote(src, dst, ssem, rsem, dev):
        return pltpu.make_async_remote_copy(
            src_ref=src, dst_ref=dst, send_sem=ssem, recv_sem=rsem,
            device_id=dev, device_id_type=MESH,
        )

    def same(ref, ssem, rsem, dev):
        return remote(ref, ref, ssem, rsem, dev)

    def unit_of(s, zz, tt):
        return gat.at[:, s, zz, tt]

    def column(s, tt):
        return gat.at[:, s, :, tt]

    here = {"tp": t}
    other = [z] + [flip_all(z, r) if Z & (Z - 1) == 0 else (z + r) % Z for r in range(1, Z)]
    sender = [z] + [flip_all(z, r) if Z & (Z - 1) == 0 else (z + Z - r) % Z for r in range(1, Z)]

    def z_copy(s, r):
        return same(unit_of(s, z, t), zs.at[s, r], zr.at[s, z], {"seq": other[r]})

    def z_sends(s):
        for r in range(1, Z):
            z_copy(s, r).start()

    def x_copy(s, r, src, slot, i):
        return same(
            unit_of(s, sender[r], src), xs.at[s, slot, r], xr.at[s, src, sender[r]],
            {"tp": flip(chip, bits[i]) * 2 + core},
        )

    def f_copy(s, src, r):
        return same(column(s, src), fs.at[s, r], fr.at[s, src], {"tp": partner})

    def source(mask):
        c = chip
        for i in range(levels):
            if (mask >> i) & 1:
                c = flip(c, bits[i])
        return c * 2 + core

    order = sorted(range(1, chips), key=lambda m: (bin(m).count("1"), m))

    def later(mask):
        first = mask.bit_length()
        return [(mask * levels + i, i) for i in range(first, levels)]

    def own_unit(s, r):
        if r > 0:
            zz = sender[r]
            same(unit_of(s, zz, t), zs.at[s, 0], zr.at[s, zz], here).wait_recv()
        for slot, i in later(0):
            x_copy(s, r, t, slot, i).start()
        if r == Z - 1:
            f_copy(s, t, 0).start()

    def pass_unit(s, r, level):
        for mask in order:
            if bin(mask).count("1") != level:
                continue
            src = source(mask)
            same(unit_of(s, sender[r], src), zs.at[s, 0], xr.at[s, src, sender[r]], here).wait_recv()
            for slot, i in later(mask):
                x_copy(s, r, src, slot, i).start()
            if r == Z - 1:
                f_copy(s, src, mask).start()

    def end_step(s):
        for c in range(chips):
            src = ((chip + c) % chips) * 2 + 1 - core
            same(column(s, src), zs.at[s, 0], fr.at[s, src], here).wait_recv()

    def drain_gather(s):
        for r in range(1, Z):
            z_copy(s, r).wait_send()
        for mask in [0] + order:
            src = source(mask)
            for slot, i in later(mask):
                for r in range(Z):
                    x_copy(s, r, src, slot, i).wait_send()
            f_copy(s, src, mask).wait_send()

    def half_copy(kind, s):
        return remote(
            part.at[kind, s, :, 1 - core], half_in.at[kind, s], ps.at[kind, s, 0], hr.at[kind, s],
            {"tp": partner},
        )

    def p_copy(kind, s, d):
        to = (chip + d) % chips
        return remote(
            part.at[kind, s, to, core], parts_in.at[kind, s, chip], ps.at[kind, s, d],
            pr.at[kind, s], {"tp": to * 2 + core},
        )

    def half_sends(s):
        for kind in range(2):
            half_copy(kind, s).start()

    def p_sends(s):
        for kind in range(2):
            half_copy(kind, s).wait_recv()
            for d in range(chips):
                c = (chip + d) % chips
                part[kind, s, c, core] = (
                    part[kind, s, c, core].astype(F32) + half_in[kind, s, c].astype(F32)
                ).astype(BF)
            for d in range(1, chips):
                p_copy(kind, s, d).start()

    def out_copies(s):
        pairs = [
            (gat.at[0, s], norm_out.at[s]), (gat.at[1, s], grad_out.at[s]),
            (hid, hid_out.at[s]), (pre, pre_out.at[s]),
        ]
        if not inside:
            pairs += [(ctx.at[0], tall_out.at[s]), (dproj.at[:, 0], wide_out.at[:, s])]
        return [pltpu.make_async_copy(src, dst, os.at[i]) for i, (src, dst) in enumerate(pairs)]

    def group_steps(n):
        steps = []
        if n % Z == 1:
            steps.append((n // Z + 1, z_sends))
        for level in range(levels + 1):
            m = n - 2 * level
            if m > 0 and level == 0:
                steps.append((m // Z, functools.partial(own_unit, r=m % Z)))
            elif m >= 0 and level > 0:
                steps.append((m // Z, functools.partial(pass_unit, r=m % Z, level=level)))
        return steps

    lead = 2 * levels

    def run_groups(s, part):
        steps = [step for k in range(Z) for step in group_steps(Z + lead + k)]
        for i, step in steps[len(steps) * part // 8 : len(steps) * (part + 1) // 8]:

            @pl.when(s + i < S)
            def _(step=step, i=i):
                step(s + i)

    z_sends(0)
    own_unit(0, 0)

    @pl.loop(1, S)
    def _(s):
        normalize(s)

    lane = lax.broadcasted_iota(jnp.int32, (L, pair), 1) % HEAD_DIM
    place = lax.broadcasted_iota(jnp.int32, (L, pair), 0).astype(F32)
    half = ROT // 2
    freq = jnp.exp((lane % half).astype(F32) * (-2.0 * LOG_BASE / ROT))
    angle = place * freq
    cosine, sine = jnp.cos(angle), jnp.sin(angle)
    table[0] = jnp.where(lane < ROT, cosine, 1.0)
    table[1] = jnp.where(lane < half, -sine, jnp.where(lane < ROT, sine, 0.0))
    abg_ref[...] = jnp.zeros_like(abg_ref)
    ubg[...] = jnp.zeros_like(ubg)
    sum_tp[t] = jnp.zeros_like(sum_tp[t])
    for load in loads:
        load.wait()

    for n in range(1, Z + lead):
        for i, step in group_steps(n):
            if i < S:
                step(i)
    end_step(0)

    def finish_sequence(s):
        totals = []
        for kind in range(2):
            incoming = parts_in.at[kind, s, pl.ds(0, chips - 1)]
            remote(incoming, incoming, ps.at[kind, s, 0], pr.at[kind, s], here).wait_recv()
            total = part[kind, s, chip, core].astype(F32)
            for d in range(1, chips):
                total = total + parts_in[kind, s, (chip + d) % chips].astype(F32)
            totals.append(total)
        branch, ngrad = totals
        x = stream_ref[:, pl.ds(s, 1), :].reshape(R, D)
        cot = cot_ref[:, pl.ds(s, 1), :].reshape(R, D)
        result_ref[:, pl.ds(s, 1), :] = (x + branch + fbias_ref[...]).reshape(R, 1, D)
        u = unit[s]
        scaled = ngrad * gain_ref[...]
        sgrad_ref[:, pl.ds(s, 1), :] = (
            cot
            + istd[s][:, :1]
            * (
                scaled
                - jnp.mean(scaled, axis=-1, keepdims=True)
                - u * jnp.mean(scaled * u, axis=-1, keepdims=True)
            )
        ).reshape(R, 1, D)
        for i, value in enumerate((ngrad * u, ngrad, cot)):
            sum_tp[t, i] += jnp.sum(value, axis=0, keepdims=True).reshape(D // 128, 128)

    def turned(x, sign):
        first = lax.broadcasted_iota(jnp.int32, (1, pair), 1) % HEAD_DIM < half
        crossed = jnp.where(first, pltpu.roll(x, pair - half, 1), pltpu.roll(x, half, 1))
        return x * table[0] + sign * (crossed * table[1])

    @pl.loop(0, S)
    def _(s):
        kept = s if inside else 0

        def rows_n():
            return gat[0, s].reshape(L, D)

        def rows_g():
            return gat[1, s].reshape(L, D)

        @pl.when(s > 0)
        def _():
            for copy in out_copies(s - 1):
                copy.wait()

        together = 3 if inside else 1
        for first in range(0, 3, together):
            wide_proj = dot(rows_n(), wa[:, first * local : (first + together) * local], (1, 0))
            for j in range(together):
                proj[first + j] = (
                    wide_proj[:, j * local : (j + 1) * local]
                    + abias_ref[first + j : first + j + 1, :]
                )

        cgrad[...] = dot(rows_g(), wo[...], (1, 1)).astype(BF)

        @pl.when(s > 0)
        def _():
            p_sends(s - 1)

        run_groups(s, 0)

        @pl.loop(0, local // pair)
        def _(h):
            lanes = pl.ds(pl.multiple_of(h * pair, pair), pair)
            q = turned(proj[0, :, lanes], 1.0).astype(BF)
            k = turned(proj[1, :, lanes], 1.0).astype(BF)
            v = proj[2, :, lanes].astype(BF)
            c, dq, dk, dv = head_pass(q, k, v, cgrad[:, lanes], pair // HEAD_DIM)
            ctx[kept, :, lanes] = c
            for j, value in enumerate((turned(dq, -1.0), turned(dk, -1.0), dv)):
                dproj[j, kept, :, lanes] = value.astype(BF)
                abg_ref[j : j + 1, lanes] += jnp.sum(value, axis=0, keepdims=True)

            @pl.when(h == 0)
            def _():
                run_groups(s, 1)

        run_groups(s, 2)
        tile = min(hidden, 512 if L <= 512 else 128)
        tiles = hidden // tile

        def feed_forward(n):
            cols = pl.ds(pl.multiple_of(n * tile, tile), tile)
            value, slope = gelu_parts(dot(rows_n(), wu[:, cols], (1, 0)) + ubias_ref[:, cols])
            hid[:, cols] = value.astype(BF)
            grad = dot(rows_g(), wd[cols, :], (1, 1)) * slope
            pre[:, cols] = grad.astype(BF)
            ubg[:, cols] += jnp.sum(grad, axis=0, keepdims=True)

        @pl.loop(0, tiles)
        def _(n):
            feed_forward(n)

            for q in range(tiles):

                @pl.when(n == q)
                def _(q=q):
                    for part in range(4 * q // tiles, 4 * (q + 1) // tiles):
                        run_groups(s, 3 + part)

        for copy in out_copies(s):
            copy.start()

        mine = pl.ds(pl.multiple_of(z * own_rows, own_rows), own_rows)

        step = 512 if inside else 256

        @pl.loop(0, D // step)
        def _(n):
            cols = pl.ds(pl.multiple_of(n * step, step), step)
            out = dot(ctx[kept, mine, :], wo[:, cols], (1, 0)) + dot(hid[mine, :], wd[:, cols], (1, 0))
            back = dot(pre[mine, :], wu[cols, :], (1, 1))
            for j in range(3):
                back = back + dot(dproj[j, kept, mine, :], wa[cols, j * local : (j + 1) * local], (1, 1))
            part[0, s, :, :, :, cols] = out.astype(BF).reshape(chips, 2, R, step)
            part[1, s, :, :, :, cols] = back.astype(BF).reshape(chips, 2, R, step)

        half_sends(s)

        run_groups(s, 7)

        @pl.when(s >= 2)
        def _():
            finish_sequence(s - 2)

        @pl.when(s + 1 < S)
        def _():
            end_step(s + 1)

    strip = D // 4

    def strip_of(n):
        return pl.ds(pl.multiple_of(n * strip, strip), strip)

    def tall_copy():
        return pltpu.make_async_copy(tall, tall_out, gs.at[2])

    def wide_copy(n, slot):
        return pltpu.make_async_copy(wide.at[slot], wide_out.at[:, strip_of(n), :], gs.at[slot])

    def output_grads():
        if inside:

            @pl.loop(0, 4)
            def _(n):
                rows = gat[1, :, :, :, :, strip_of(n)].reshape(S * L, strip)
                tall[:, strip_of(n)] = dot(ctx[...].reshape(S * L, local), rows, (0, 0))

            tall_copy().start()

    def attend_grads(n, slot):
        if inside:

            @pl.loop(0, 3)
            def _(j):
                rows = gat[0, :, :, :, :, strip_of(n)].reshape(S * L, strip)
                wide[slot, j] = dot(rows, dproj[j].reshape(S * L, local), (0, 0))

            wide_copy(n, slot).start()

    output_grads()
    p_sends(S - 1)

    @pl.loop(0, 2)
    def _(n):
        attend_grads(n, n)

    @pl.loop(max(0, S - 2), S)
    def _(s):
        finish_sequence(s)

    def m_copy(d):
        return remote(sum_tp.at[t], sum_tp.at[t], ms.at[d], mr.at[0], {"tp": (t + d) % TP})

    def n_copy(d):
        return remote(
            sum_seq.at[z], sum_seq.at[z], ms.at[TP + d], mr.at[1], {"seq": (z + d) % Z}
        )

    for d in range(1, TP):
        m_copy(d).start()
    if inside:
        wide_copy(0, 0).wait()
    attend_grads(2, 0)
    same(sum_tp.at[pl.ds(0, TP - 1)], ms.at[0], mr.at[0], here).wait_recv()
    total = sum_tp[0]
    for d in range(1, TP):
        total = total + sum_tp[d]
    sum_seq[z] = total
    for d in range(1, Z):
        n_copy(d).start()
    if inside:
        wide_copy(1, 1).wait()
    attend_grads(3, 1)
    same(sum_seq.at[pl.ds(0, Z - 1)], ms.at[0], mr.at[1], here).wait_recv()
    total = sum_seq[0]
    for d in range(1, Z):
        total = total + sum_seq[d]
    gsum_ref[...], osum_ref[...], fsum_ref[...] = total[0], total[1], total[2]
    ubg_ref[...] = ubg[...].reshape(hidden // 128, 128)

    for d in range(1, TP):
        m_copy(d).wait_send()
    for d in range(1, Z):
        n_copy(d).wait_send()
    for copy in out_copies(S - 1):
        copy.wait()
    if inside:
        tall_copy().wait()
        wide_copy(2, 0).wait()
        wide_copy(3, 1).wait()

    @pl.loop(0, S)
    def _(s):
        drain_gather(s)
        for kind in range(2):
            half_copy(kind, s).wait_send()
            for d in range(1, chips):
                p_copy(kind, s, d).wait_send()


def attention_inside(length):
    return length <= 512


def block_call(stream, cotangent, gain, offset, fbias, abias, ubias, wa, wo, wu, wd, Z, TP):
    R, S, D = stream.shape
    local, hidden = wo.shape[0], wu.shape[1]
    L = Z * TP * R
    chips = TP // 2
    levels = chips.bit_length() - 1
    vm = pl.BlockSpec(memory_space=pltpu.VMEM)
    anywhere = pl.BlockSpec(memory_space=pl.ANY)
    shape = jax.ShapeDtypeStruct
    dma = pltpu.SemaphoreType.DMA
    inside = attention_inside(L)
    kept = S if inside else 1
    return pl.pallas_call(
        functools.partial(block_kernel, (Z, TP, S, R, D)),
        in_specs=[vm] * 7 + [anywhere] * 4,
        out_specs=[anywhere] * 6 + [vm] * 7,
        out_shape=[
            shape((S, Z, TP, R, D), BF),
            shape((S, Z, TP, R, D), BF),
            shape((S, L, hidden), BF),
            shape((S, L, hidden), BF),
            shape((3, D, local), F32) if inside else shape((3, S, L, local), BF),
            shape((local, D), F32) if inside else shape((S, L, local), BF),
            shape((R, S, D), F32),
            shape((R, S, D), F32),
            shape((D // 128, 128), F32),
            shape((D // 128, 128), F32),
            shape((D // 128, 128), F32),
            shape((3, local), F32),
            shape((hidden // 128, 128), F32),
        ],
        scratch_shapes=[
            pltpu.VMEM((2, S, Z, TP, R, D), BF),
            pltpu.VMEM((D, 3 * local), BF),
            pltpu.VMEM((local, D), BF),
            pltpu.VMEM((D, hidden), BF),
            pltpu.VMEM((hidden, D), BF),
            pltpu.VMEM((S, R, D), F32),
            pltpu.VMEM((S, R, 128), F32),
            pltpu.VMEM((2, L, min(128, local)), F32),
            pltpu.VMEM((3, L, local), F32),
            pltpu.VMEM((L, local), BF),
            pltpu.VMEM((L, hidden), BF),
            pltpu.VMEM((L, hidden), BF),
            pltpu.VMEM((kept, L, local), BF),
            pltpu.VMEM((3, kept, L, local), BF),
            pltpu.VMEM((2, S, chips, 2, R, D), BF),
            pltpu.VMEM((2, S, chips, R, D), BF),
            pltpu.VMEM((2, S, chips, R, D), BF),
            pltpu.VMEM((TP, 3, D // 128, 128), F32),
            pltpu.VMEM((Z, 3, D // 128, 128), F32),
            pltpu.VMEM((1, hidden), F32),
            pltpu.VMEM((2, 3, D // 4, local) if inside else (1, 3, 8, 128), F32),
            pltpu.VMEM((local, D) if inside else (8, 128), F32),
            dma((S, Z)),
            dma((S, Z)),
            dma((S, chips * levels, Z)),
            dma((S, TP, Z)),
            dma((S, chips)),
            dma((S, TP)),
            dma((2, S, chips)),
            dma((2, S)),
            dma((2, S)),
            dma((TP + Z,)),
            dma((2,)),
            dma((6,)),
            dma((6,)),
            dma((3,)),
        ],
        compiler_params=pltpu.CompilerParams(
            collective_id=0, has_side_effects=True, vmem_limit_bytes=67000000
        ),
        name="block",
    )(stream, cotangent, gain, offset, fbias, abias, ubias, wa, wo, wu, wd)


def weight_kernel(steps, inside, normed, grads, pre, wide, hid_hbm, tall, *rest):
    smalls = (len(rest) - 7) // 2
    given, rest = rest[:smalls], rest[smalls:]
    up, attend, down, output = rest[:4]
    handed, (hid, ctx, sem) = rest[4 : 4 + smalls], rest[4 + smalls :]
    i = pl.program_id(0)
    loads = [
        pltpu.make_async_copy(hid_hbm, hid, sem.at[0]),
    ]
    if not inside:
        loads.append(pltpu.make_async_copy(tall, ctx, sem.at[1]))

    @pl.when(i == 0)
    def _():
        for load in loads:
            load.start()
        for source, target in zip(given, handed):
            target[...] = source[...]

    @pl.when(i < steps)
    def _():
        up[...] = dot(normed[...], pre[...], (0, 0))
        if inside:
            attend[...] = wide[...]
        else:
            for j in range(3):
                attend[j] = dot(normed[...], wide[j], (0, 0))

    @pl.when(i == steps)
    def _():
        for load in loads:
            load.wait()

    @pl.when(i >= steps)
    def _():
        down[...] = dot(hid[...], grads[...], (0, 0))
        output[...] = tall[...] if inside else dot(ctx[...], grads[...], (0, 0))


def weight_call(normed, grads, pre, wide, hid, tall, smalls, local, inside):
    tokens, D = normed.shape
    hidden = pre.shape[1]
    tile = 512 if tokens * 512 * 2 <= (2 << 20) else 256
    steps = D // tile
    whole = lambda *shape: pl.BlockSpec(shape, lambda i: (0,) * len(shape), pipeline_mode=pl.Buffered(1))
    first = lambda i: jnp.minimum(i, steps - 1)
    second = lambda i: jnp.maximum(i - steps, 0)
    anywhere = pl.BlockSpec(memory_space=pl.ANY)
    shape = jax.ShapeDtypeStruct
    return pl.pallas_call(
        functools.partial(weight_kernel, steps, inside),
        grid=(2 * steps,),
        in_specs=[
            pl.BlockSpec((tokens, tile), lambda i: (0, first(i))),
            pl.BlockSpec((tokens, tile), lambda i: (0, second(i))),
            whole(tokens, hidden),
            pl.BlockSpec((3, tile, local), lambda i: (0, first(i), 0)) if inside else whole(*wide.shape),
            anywhere,
            pl.BlockSpec((local, tile), lambda i: (0, second(i))) if inside else anywhere,
        ]
        + [whole(*small.shape) for small in smalls],
        out_specs=[
            pl.BlockSpec((tile, hidden), lambda i: (first(i), 0)),
            pl.BlockSpec((3, tile, local), lambda i: (0, first(i), 0)),
            pl.BlockSpec((hidden, tile), lambda i: (0, second(i))),
            pl.BlockSpec((local, tile), lambda i: (0, second(i))),
        ]
        + [whole(*small.shape) for small in smalls],
        out_shape=[
            shape((D, hidden), F32),
            shape((3, D, local), F32),
            shape((hidden, D), F32),
            shape((local, D), F32),
        ]
        + [shape(small.shape, F32) for small in smalls],
        scratch_shapes=[
            pltpu.VMEM((tokens, hidden), BF),
            pltpu.VMEM((16, 128) if inside else (tokens, local), BF),
            pltpu.SemaphoreType.DMA((2,)),
        ],
        compiler_params=pltpu.CompilerParams(vmem_limit_bytes=67000000),
        name="weights",
    )(normed, grads, pre, wide, hid, tall, *smalls)


def per_device(
    stream,
    norm_gain,
    norm_offset,
    attend_weight,
    attend_bias,
    output_weight,
    up_weight,
    up_bias,
    down_weight,
    final_bias,
    cotangent,
):
    R, S, D = stream.shape
    local = attend_weight.shape[2]
    hidden = up_weight.shape[1]
    TP, Z = lax.axis_size("tp"), lax.axis_size("seq")
    tokens = R * S * TP * Z
    inside = attention_inside(R * TP * Z)
    weights = jnp.swapaxes(attend_weight, 0, 1)
    (
        normed, grads, hid, pre, wide, tall, *smalls
    ) = block_call(
        stream, cotangent, norm_gain.reshape(1, D), norm_offset.reshape(1, D),
        final_bias.reshape(1, D), attend_bias, up_bias.reshape(1, hidden),
        weights, output_weight, up_weight, down_weight, Z, TP,
    )
    (
        up_grad, attend_grad, down_grad, output_grad,
        result, stream_grad, gain_grad, offset_grad, fbias_grad, abias_grad, ubias_grad,
    ) = weight_call(
        normed.reshape(tokens, D), grads.reshape(tokens, D), pre.reshape(tokens, hidden),
        wide if inside else wide.reshape(3, tokens, local), hid.reshape(tokens, hidden),
        tall if inside else tall.reshape(tokens, local), smalls, local, inside,
    )
    return (
        result,
        stream_grad,
        gain_grad.reshape(D),
        offset_grad.reshape(D),
        jnp.swapaxes(attend_grad, 0, 1),
        abias_grad,
        output_grad,
        up_grad,
        ubias_grad.reshape(hidden),
        down_grad,
        fbias_grad.reshape(D),
    )


def solution(mesh):
    in_specs = (
        P(("seq", "tp"), None, None),
        P(),
        P(),
        P(None, None, "tp"),
        P(None, "tp"),
        P("tp", None),
        P(None, "tp"),
        P("tp"),
        P("tp", None),
        P(),
        P(("seq", "tp"), None, None),
    )
    out_specs = (
        P(("seq", "tp"), None, None),
        P(("seq", "tp"), None, None),
        P(),
        P(),
        P(None, None, "tp"),
        P(None, "tp"),
        P("tp", None),
        P(None, "tp"),
        P("tp"),
        P("tp", None),
        P(),
    )
    return jax.shard_map(
        per_device, mesh=mesh, in_specs=in_specs, out_specs=out_specs, check_vma=False
    )
```

```python
import functools
import math

import jax
import jax.numpy as jnp
from jax import lax
from jax.experimental import pallas as pl
from jax.experimental.pallas import tpu as pltpu
from jax.sharding import PartitionSpec as P

HEAD_DIM = 64
ROT = 32

EPS = 1e-05
GELU_C = 0.7978845608028654
CUBIC = 0.044715
LOG_BASE = math.log(10000.0)
BF = jnp.bfloat16
F32 = jnp.float32
MESH = pl.DeviceIdType.MESH


def gelu_parts(pre_act):
    inner_arg = GELU_C * (pre_act + CUBIC * pre_act * pre_act * pre_act)
    tanh_value = jnp.tanh(inner_arg)
    gelu_value = 0.5 * pre_act * (1.0 + tanh_value)
    gelu_slope = 0.5 * (1.0 + tanh_value) + 0.5 * pre_act * (
        1.0 - tanh_value * tanh_value
    ) * GELU_C * (1.0 + 3.0 * CUBIC * pre_act * pre_act)
    return (gelu_value, gelu_slope)


def dot(a, b, dims):
    return lax.dot_general(a, b, ((dims[:1], dims[1:]), ((), ())), preferred_element_type=F32)


def flip(index, bit):
    return index + bit - 2 * bit * ((index // bit) % 2)


def flip_all(index, mask):
    bit = 1
    while bit <= mask:
        if mask & bit:
            index = flip(index, bit)
        bit *= 2
    return index


def head_pass(q_all, k_all, v_all, g_all, heads, block=256):
    length, width = q_all.shape
    scale = jnp.asarray(HEAD_DIM ** (-0.5), BF)
    block = min(block, length)
    lane = lax.broadcasted_iota(jnp.int32, (1, width), 1) // HEAD_DIM
    zero = jnp.zeros((), BF)
    parts = [(start, head) for start in range(0, length, block) for head in range(heads)]

    def masked(x, start, head):
        return jnp.where(lane == head, x[start : start + block], zero)

    qs = [masked(q_all, a, h) * scale for a, h in parts]
    gs = [masked(g_all, a, h) for a, h in parts]

    def weights(s, start):
        diag = s[:, start:]
        row = lax.broadcasted_iota(jnp.int32, diag.shape, 0)
        col = lax.broadcasted_iota(jnp.int32, diag.shape, 1)
        diag = jnp.where(row >= col, diag, -jnp.inf)
        s = diag if start == 0 else jnp.concatenate([s[:, :start], diag], axis=1)
        p = jnp.exp(s - jnp.max(s, axis=1, keepdims=True))
        return p * (1.0 / jnp.sum(p, axis=1, keepdims=True))

    cs, dqs, dks, dvs = [], [], [], []
    together = len(parts) if length <= 512 else heads
    for first in range(0, len(parts), together):
        group = slice(first, first + together)
        stops = [a + block for a, h in parts[group]]
        gq, gg = qs[group], gs[group]
        ss = [dot(q, k_all[:n], (1, 1)) for q, n in zip(gq, stops)]
        dps = [dot(g, v_all[:n], (1, 1)) for g, n in zip(gg, stops)]
        ps = [weights(s, a) for s, (a, h) in zip(ss, parts[group])]
        pbs = [p.astype(BF) for p in ps]
        gc = [dot(p, v_all[:n], (1, 0)).astype(BF) for p, n in zip(pbs, stops)]
        dvs += [dot(g, p, (0, 0)) for g, p in zip(gg, pbs)]
        deltas = [
            jnp.sum(g.astype(F32) * c.astype(F32), axis=1, keepdims=True) for g, c in zip(gg, gc)
        ]
        dss = [(p * (dp - delta)).astype(BF) for p, dp, delta in zip(ps, dps, deltas)]
        dqs += [dot(ds, k_all[:n], (1, 0)) for ds, n in zip(dss, stops)]
        dks += [dot(q, ds, (0, 0)) for q, ds in zip(gq, dss)]
        cs += gc

    def rows(values):
        blocks = []
        for n in range(0, len(parts), heads):
            value = values[n]
            for h in range(1, heads):
                value = jnp.where(lane == h, values[n + h], value)
            blocks.append(value)
        return jnp.concatenate(blocks, axis=0)

    def columns(values):
        total = None
        for n in range(0, len(parts), heads):
            value = values[n]
            for h in range(1, heads):
                value = value + values[n + h]
            if total is None:
                total = value
            else:
                old = total.shape[1]
                total = jnp.concatenate([total + value[:, :old], value[:, old:]], axis=1)
        return total.T

    return [rows(cs), rows(dqs) * scale.astype(F32), columns(dks), columns(dvs)]


def block_kernel(
    dims,
    stream_ref, cot_ref, gain_ref, offset_ref, fbias_ref, abias_ref, ubias_ref,
    wa_hbm, wo_hbm, wu_hbm, wd_hbm,
    norm_out, grad_out, hid_out, pre_out, wide_out, tall_out,
    result_ref, sgrad_ref, gsum_ref, osum_ref, fsum_ref, abg_ref, ubg_ref,
    gat, wa, wo, wu, wd, unit, istd, table, proj, cgrad, hid, pre, ctx, dproj,
    part, half_in, parts_in, sum_tp, sum_seq, ubg, wide, tall,
    zs, zr, xs, xr, fs, fr, ps, hr, pr, ms, mr, ws, os, gs,
):
    Z, TP, S, R, D = dims
    z, t = lax.axis_index("seq"), lax.axis_index("tp")
    chip, core = t // 2, t % 2
    chips = TP // 2
    levels = chips.bit_length() - 1
    bits = [
        (1 - core) * (1 << i) + core * (1 << (levels - 1 - i)) for i in range(levels)
    ]
    partner = chip * 2 + 1 - core
    L = Z * TP * R
    local = wo.shape[0]
    hidden = wu.shape[1]
    pair = min(128, local)
    own_rows = TP * R
    inside = ctx.shape[0] == S

    loads = [
        pltpu.make_async_copy(src, dst, ws.at[i])
        for i, (src, dst) in enumerate(((wo_hbm, wo), (wu_hbm, wu), (wd_hbm, wd)))
    ] + [
        pltpu.make_async_copy(wa_hbm.at[j], wa.at[:, pl.ds(j * wo.shape[0], wo.shape[0])], ws.at[3 + j])
        for j in range(3)
    ]
    for load in loads:
        load.start()
    barrier = pltpu.get_barrier_semaphore()
    for d in range(1, TP):
        pl.semaphore_signal(barrier, inc=1, device_id={"tp": (t + d) % TP}, device_id_type=MESH)
    for d in range(1, Z):
        pl.semaphore_signal(barrier, inc=1, device_id={"seq": (z + d) % Z}, device_id_type=MESH)

    def normalize(s):
        x = stream_ref[:, pl.ds(s, 1), :].reshape(R, D)
        mean = jnp.mean(x, axis=-1, keepdims=True)
        centred = x - mean
        inv = lax.rsqrt(jnp.mean(centred * centred, axis=-1, keepdims=True) + EPS)
        u = centred * inv
        unit[s] = u
        istd[s] = jnp.broadcast_to(inv, (R, 128))
        gat[0, s, z, t] = (u * gain_ref[...] + offset_ref[...]).astype(BF)
        gat[1, s, z, t] = cot_ref[:, pl.ds(s, 1), :].reshape(R, D).astype(BF)

    normalize(0)
    pl.semaphore_wait(barrier, TP + Z - 2)

    def remote(src, dst, ssem, rsem, dev):
        return pltpu.make_async_remote_copy(
            src_ref=src, dst_ref=dst, send_sem=ssem, recv_sem=rsem,
            device_id=dev, device_id_type=MESH,
        )

    def same(ref, ssem, rsem, dev):
        return remote(ref, ref, ssem, rsem, dev)

    def unit_of(s, zz, tt):
        return gat.at[:, s, zz, tt]

    def column(s, tt):
        return gat.at[:, s, :, tt]

    here = {"tp": t}
    other = [z] + [flip_all(z, r) if Z & (Z - 1) == 0 else (z + r) % Z for r in range(1, Z)]
    sender = [z] + [flip_all(z, r) if Z & (Z - 1) == 0 else (z + Z - r) % Z for r in range(1, Z)]

    def z_copy(s, r):
        return same(unit_of(s, z, t), zs.at[s, r], zr.at[s, z], {"seq": other[r]})

    def z_sends(s):
        for r in range(1, Z):
            z_copy(s, r).start()

    def x_copy(s, r, src, slot, i):
        return same(
            unit_of(s, sender[r], src), xs.at[s, slot, r], xr.at[s, src, sender[r]],
            {"tp": flip(chip, bits[i]) * 2 + core},
        )

    def f_copy(s, src, r):
        return same(column(s, src), fs.at[s, r], fr.at[s, src], {"tp": partner})

    def source(mask):
        c = chip
        for i in range(levels):
            if (mask >> i) & 1:
                c = flip(c, bits[i])
        return c * 2 + core

    order = sorted(range(1, chips), key=lambda m: (bin(m).count("1"), m))

    def later(mask):
        first = mask.bit_length()
        return [(mask * levels + i, i) for i in range(first, levels)]

    def own_unit(s, r):
        if r > 0:
            zz = sender[r]
            same(unit_of(s, zz, t), zs.at[s, 0], zr.at[s, zz], here).wait_recv()
        for slot, i in later(0):
            x_copy(s, r, t, slot, i).start()
        if r == Z - 1:
            f_copy(s, t, 0).start()

    def pass_unit(s, r, level):
        for mask in order:
            if bin(mask).count("1") != level:
                continue
            src = source(mask)
            same(unit_of(s, sender[r], src), zs.at[s, 0], xr.at[s, src, sender[r]], here).wait_recv()
            for slot, i in later(mask):
                x_copy(s, r, src, slot, i).start()
            if r == Z - 1:
                f_copy(s, src, mask).start()

    def end_step(s):
        for c in range(chips):
            src = ((chip + c) % chips) * 2 + 1 - core
            same(column(s, src), zs.at[s, 0], fr.at[s, src], here).wait_recv()

    def drain_gather(s):
        for r in range(1, Z):
            z_copy(s, r).wait_send()
        for mask in [0] + order:
            src = source(mask)
            for slot, i in later(mask):
                for r in range(Z):
                    x_copy(s, r, src, slot, i).wait_send()
            f_copy(s, src, mask).wait_send()

    def half_copy(kind, s):
        return remote(
            part.at[kind, s, :, 1 - core], half_in.at[kind, s], ps.at[kind, s, 0], hr.at[kind, s],
            {"tp": partner},
        )

    def p_copy(kind, s, d):
        to = (chip + d) % chips
        return remote(
            part.at[kind, s, to, core], parts_in.at[kind, s, chip], ps.at[kind, s, d],
            pr.at[kind, s], {"tp": to * 2 + core},
        )

    def half_sends(s):
        for kind in range(2):
            half_copy(kind, s).start()

    def p_sends(s):
        for kind in range(2):
            half_copy(kind, s).wait_recv()
            for d in range(chips):
                c = (chip + d) % chips
                part[kind, s, c, core] = (
                    part[kind, s, c, core].astype(F32) + half_in[kind, s, c].astype(F32)
                ).astype(BF)
            for d in range(1, chips):
                p_copy(kind, s, d).start()

    def out_copies(s):
        pairs = [
            (gat.at[0, s], norm_out.at[s]), (gat.at[1, s], grad_out.at[s]),
            (hid, hid_out.at[s]), (pre, pre_out.at[s]),
        ]
        if not inside:
            pairs += [(ctx.at[0], tall_out.at[s]), (dproj.at[:, 0], wide_out.at[:, s])]
        return [pltpu.make_async_copy(src, dst, os.at[i]) for i, (src, dst) in enumerate(pairs)]

    def group_steps(n):
        steps = []
        if n % Z == 1:
            steps.append((n // Z + 1, z_sends))
        for level in range(levels + 1):
            m = n - 2 * level
            if m > 0 and level == 0:
                steps.append((m // Z, functools.partial(own_unit, r=m % Z)))
            elif m >= 0 and level > 0:
                steps.append((m // Z, functools.partial(pass_unit, r=m % Z, level=level)))
        return steps

    lead = 2 * levels

    def run_groups(s, part):
        steps = [step for k in range(Z) for step in group_steps(Z + lead + k)]
        for i, step in steps[len(steps) * part // 8 : len(steps) * (part + 1) // 8]:

            @pl.when(s + i < S)
            def _(step=step, i=i):
                step(s + i)

    z_sends(0)
    own_unit(0, 0)

    @pl.loop(1, S)
    def _(s):
        normalize(s)

    lane = lax.broadcasted_iota(jnp.int32, (L, pair), 1) % HEAD_DIM
    place = lax.broadcasted_iota(jnp.int32, (L, pair), 0).astype(F32)
    half = ROT // 2
    freq = jnp.exp((lane % half).astype(F32) * (-2.0 * LOG_BASE / ROT))
    angle = place * freq
    cosine, sine = jnp.cos(angle), jnp.sin(angle)
    table[0] = jnp.where(lane < ROT, cosine, 1.0)
    table[1] = jnp.where(lane < half, -sine, jnp.where(lane < ROT, sine, 0.0))
    abg_ref[...] = jnp.zeros_like(abg_ref)
    ubg[...] = jnp.zeros_like(ubg)
    sum_tp[t] = jnp.zeros_like(sum_tp[t])
    for load in loads:
        load.wait()

    for n in range(1, Z + lead):
        for i, step in group_steps(n):
            if i < S:
                step(i)
    end_step(0)

    def finish_sequence(s):
        totals = []
        for kind in range(2):
            incoming = parts_in.at[kind, s, pl.ds(0, chips - 1)]
            remote(incoming, incoming, ps.at[kind, s, 0], pr.at[kind, s], here).wait_recv()
            total = part[kind, s, chip, core].astype(F32)
            for d in range(1, chips):
                total = total + parts_in[kind, s, (chip + d) % chips].astype(F32)
            totals.append(total)
        branch, ngrad = totals
        x = stream_ref[:, pl.ds(s, 1), :].reshape(R, D)
        cot = cot_ref[:, pl.ds(s, 1), :].reshape(R, D)
        result_ref[:, pl.ds(s, 1), :] = (x + branch + fbias_ref[...]).reshape(R, 1, D)
        u = unit[s]
        scaled = ngrad * gain_ref[...]
        sgrad_ref[:, pl.ds(s, 1), :] = (
            cot
            + istd[s][:, :1]
            * (
                scaled
                - jnp.mean(scaled, axis=-1, keepdims=True)
                - u * jnp.mean(scaled * u, axis=-1, keepdims=True)
            )
        ).reshape(R, 1, D)
        for i, value in enumerate((ngrad * u, ngrad, cot)):
            sum_tp[t, i] += jnp.sum(value, axis=0, keepdims=True).reshape(D // 128, 128)

    def turned(x, sign):
        first = lax.broadcasted_iota(jnp.int32, (1, pair), 1) % HEAD_DIM < half
        crossed = jnp.where(first, pltpu.roll(x, pair - half, 1), pltpu.roll(x, half, 1))
        return x * table[0] + sign * (crossed * table[1])

    @pl.loop(0, S)
    def _(s):
        kept = s if inside else 0

        def rows_n():
            return gat[0, s].reshape(L, D)

        def rows_g():
            return gat[1, s].reshape(L, D)

        @pl.when(s > 0)
        def _():
            for copy in out_copies(s - 1):
                copy.wait()

        together = 3 if inside else 1
        for first in range(0, 3, together):
            wide_proj = dot(rows_n(), wa[:, first * local : (first + together) * local], (1, 0))
            for j in range(together):
                proj[first + j] = (
                    wide_proj[:, j * local : (j + 1) * local]
                    + abias_ref[first + j : first + j + 1, :]
                )

        cgrad[...] = dot(rows_g(), wo[...], (1, 1)).astype(BF)

        @pl.when(s > 0)
        def _():
            p_sends(s - 1)

        run_groups(s, 0)

        @pl.loop(0, local // pair)
        def _(h):
            lanes = pl.ds(pl.multiple_of(h * pair, pair), pair)
            q = turned(proj[0, :, lanes], 1.0).astype(BF)
            k = turned(proj[1, :, lanes], 1.0).astype(BF)
            v = proj[2, :, lanes].astype(BF)
            c, dq, dk, dv = head_pass(q, k, v, cgrad[:, lanes], pair // HEAD_DIM)
            ctx[kept, :, lanes] = c
            for j, value in enumerate((turned(dq, -1.0), turned(dk, -1.0), dv)):
                dproj[j, kept, :, lanes] = value.astype(BF)
                abg_ref[j : j + 1, lanes] += jnp.sum(value, axis=0, keepdims=True)

            @pl.when(h == 0)
            def _():
                run_groups(s, 1)

        run_groups(s, 2)
        tile = min(hidden, 512 if L <= 512 else 128)
        tiles = hidden // tile

        def feed_forward(n):
            cols = pl.ds(pl.multiple_of(n * tile, tile), tile)
            value, slope = gelu_parts(dot(rows_n(), wu[:, cols], (1, 0)) + ubias_ref[:, cols])
            hid[:, cols] = value.astype(BF)
            grad = dot(rows_g(), wd[cols, :], (1, 1)) * slope
            pre[:, cols] = grad.astype(BF)
            ubg[:, cols] += jnp.sum(grad, axis=0, keepdims=True)

        @pl.loop(0, tiles)
        def _(n):
            feed_forward(n)

            for q in range(tiles):

                @pl.when(n == q)
                def _(q=q):
                    for part in range(4 * q // tiles, 4 * (q + 1) // tiles):
                        run_groups(s, 3 + part)

        for copy in out_copies(s):
            copy.start()

        mine = pl.ds(pl.multiple_of(z * own_rows, own_rows), own_rows)

        step = 512 if inside else 256

        @pl.loop(0, D // step)
        def _(n):
            cols = pl.ds(pl.multiple_of(n * step, step), step)
            out = dot(ctx[kept, mine, :], wo[:, cols], (1, 0)) + dot(hid[mine, :], wd[:, cols], (1, 0))
            back = dot(pre[mine, :], wu[cols, :], (1, 1))
            for j in range(3):
                back = back + dot(dproj[j, kept, mine, :], wa[cols, j * local : (j + 1) * local], (1, 1))
            part[0, s, :, :, :, cols] = out.astype(BF).reshape(chips, 2, R, step)
            part[1, s, :, :, :, cols] = back.astype(BF).reshape(chips, 2, R, step)

        half_sends(s)

        run_groups(s, 7)

        @pl.when(s >= 2)
        def _():
            finish_sequence(s - 2)

        @pl.when(s + 1 < S)
        def _():
            end_step(s + 1)

    strip = D // 4

    def strip_of(n):
        return pl.ds(pl.multiple_of(n * strip, strip), strip)

    def tall_copy():
        return pltpu.make_async_copy(tall, tall_out, gs.at[2])

    def wide_copy(n, slot):
        return pltpu.make_async_copy(wide.at[slot], wide_out.at[:, strip_of(n), :], gs.at[slot])

    def output_grads(first, last):
        if inside:

            @pl.loop(first, last)
            def _(n):
                rows = gat[1, :, :, :, :, strip_of(n)].reshape(S * L, strip)
                tall[:, strip_of(n)] = dot(ctx[...].reshape(S * L, local), rows, (0, 0))

    def attend_grads(n, slot):
        if inside:

            @pl.loop(0, 3)
            def _(j):
                rows = gat[0, :, :, :, :, strip_of(n)].reshape(S * L, strip)
                wide[slot, j] = dot(rows, dproj[j].reshape(S * L, local), (0, 0))

            wide_copy(n, slot).start()

    output_grads(0, 2)
    p_sends(S - 1)
    output_grads(2, 4)
    if inside:
        tall_copy().start()

    @pl.loop(0, 2)
    def _(n):
        attend_grads(n, n)

    @pl.loop(max(0, S - 2), S)
    def _(s):
        finish_sequence(s)

    def m_copy(d):
        return remote(sum_tp.at[t], sum_tp.at[t], ms.at[d], mr.at[0], {"tp": (t + d) % TP})

    def n_copy(d):
        return remote(
            sum_seq.at[z], sum_seq.at[z], ms.at[TP + d], mr.at[1], {"seq": (z + d) % Z}
        )

    for d in range(1, TP):
        m_copy(d).start()
    if inside:
        wide_copy(0, 0).wait()
    attend_grads(2, 0)
    same(sum_tp.at[pl.ds(0, TP - 1)], ms.at[0], mr.at[0], here).wait_recv()
    total = sum_tp[0]
    for d in range(1, TP):
        total = total + sum_tp[d]
    sum_seq[z] = total
    for d in range(1, Z):
        n_copy(d).start()
    if inside:
        wide_copy(1, 1).wait()
    attend_grads(3, 1)
    same(sum_seq.at[pl.ds(0, Z - 1)], ms.at[0], mr.at[1], here).wait_recv()
    total = sum_seq[0]
    for d in range(1, Z):
        total = total + sum_seq[d]
    gsum_ref[...], osum_ref[...], fsum_ref[...] = total[0], total[1], total[2]
    ubg_ref[...] = ubg[...].reshape(hidden // 128, 128)

    for d in range(1, TP):
        m_copy(d).wait_send()
    for d in range(1, Z):
        n_copy(d).wait_send()
    for copy in out_copies(S - 1):
        copy.wait()
    if inside:
        tall_copy().wait()
        wide_copy(2, 0).wait()
        wide_copy(3, 1).wait()

    @pl.loop(0, S)
    def _(s):
        drain_gather(s)
        for kind in range(2):
            half_copy(kind, s).wait_send()
            for d in range(1, chips):
                p_copy(kind, s, d).wait_send()


def attention_inside(length):
    return length <= 512


def block_call(stream, cotangent, gain, offset, fbias, abias, ubias, wa, wo, wu, wd, Z, TP):
    R, S, D = stream.shape
    local, hidden = wo.shape[0], wu.shape[1]
    L = Z * TP * R
    chips = TP // 2
    levels = chips.bit_length() - 1
    vm = pl.BlockSpec(memory_space=pltpu.VMEM)
    anywhere = pl.BlockSpec(memory_space=pl.ANY)
    shape = jax.ShapeDtypeStruct
    dma = pltpu.SemaphoreType.DMA
    inside = attention_inside(L)
    kept = S if inside else 1
    return pl.pallas_call(
        functools.partial(block_kernel, (Z, TP, S, R, D)),
        in_specs=[vm] * 7 + [anywhere] * 4,
        out_specs=[anywhere] * 6 + [vm] * 7,
        out_shape=[
            shape((S, Z, TP, R, D), BF),
            shape((S, Z, TP, R, D), BF),
            shape((S, L, hidden), BF),
            shape((S, L, hidden), BF),
            shape((3, D, local), F32) if inside else shape((3, S, L, local), BF),
            shape((local, D), F32) if inside else shape((S, L, local), BF),
            shape((R, S, D), F32),
            shape((R, S, D), F32),
            shape((D // 128, 128), F32),
            shape((D // 128, 128), F32),
            shape((D // 128, 128), F32),
            shape((3, local), F32),
            shape((hidden // 128, 128), F32),
        ],
        scratch_shapes=[
            pltpu.VMEM((2, S, Z, TP, R, D), BF),
            pltpu.VMEM((D, 3 * local), BF),
            pltpu.VMEM((local, D), BF),
            pltpu.VMEM((D, hidden), BF),
            pltpu.VMEM((hidden, D), BF),
            pltpu.VMEM((S, R, D), F32),
            pltpu.VMEM((S, R, 128), F32),
            pltpu.VMEM((2, L, min(128, local)), F32),
            pltpu.VMEM((3, L, local), F32),
            pltpu.VMEM((L, local), BF),
            pltpu.VMEM((L, hidden), BF),
            pltpu.VMEM((L, hidden), BF),
            pltpu.VMEM((kept, L, local), BF),
            pltpu.VMEM((3, kept, L, local), BF),
            pltpu.VMEM((2, S, chips, 2, R, D), BF),
            pltpu.VMEM((2, S, chips, R, D), BF),
            pltpu.VMEM((2, S, chips, R, D), BF),
            pltpu.VMEM((TP, 3, D // 128, 128), F32),
            pltpu.VMEM((Z, 3, D // 128, 128), F32),
            pltpu.VMEM((1, hidden), F32),
            pltpu.VMEM((2, 3, D // 4, local) if inside else (1, 3, 8, 128), F32),
            pltpu.VMEM((local, D) if inside else (8, 128), F32),
            dma((S, Z)),
            dma((S, Z)),
            dma((S, chips * levels, Z)),
            dma((S, TP, Z)),
            dma((S, chips)),
            dma((S, TP)),
            dma((2, S, chips)),
            dma((2, S)),
            dma((2, S)),
            dma((TP + Z,)),
            dma((2,)),
            dma((6,)),
            dma((6,)),
            dma((3,)),
        ],
        compiler_params=pltpu.CompilerParams(
            collective_id=0, has_side_effects=True, vmem_limit_bytes=67000000
        ),
        name="block",
    )(stream, cotangent, gain, offset, fbias, abias, ubias, wa, wo, wu, wd)


def weight_kernel(steps, inside, normed, grads, pre, wide, hid_hbm, tall, *rest):
    smalls = (len(rest) - 7) // 2
    given, rest = rest[:smalls], rest[smalls:]
    up, attend, down, output = rest[:4]
    handed, (hid, ctx, sem) = rest[4 : 4 + smalls], rest[4 + smalls :]
    i = pl.program_id(0)
    loads = [
        pltpu.make_async_copy(hid_hbm, hid, sem.at[0]),
    ]
    if not inside:
        loads.append(pltpu.make_async_copy(tall, ctx, sem.at[1]))

    @pl.when(i == 0)
    def _():
        for load in loads:
            load.start()
        for source, target in zip(given, handed):
            target[...] = source[...]

    @pl.when(i < steps)
    def _():
        up[...] = dot(normed[...], pre[...], (0, 0))
        if inside:
            attend[...] = wide[...]
        else:
            for j in range(3):
                attend[j] = dot(normed[...], wide[j], (0, 0))

    @pl.when(i == steps)
    def _():
        for load in loads:
            load.wait()

    @pl.when(i >= steps)
    def _():
        down[...] = dot(hid[...], grads[...], (0, 0))
        output[...] = tall[...] if inside else dot(ctx[...], grads[...], (0, 0))


def weight_call(normed, grads, pre, wide, hid, tall, smalls, local, inside):
    tokens, D = normed.shape
    hidden = pre.shape[1]
    tile = 512 if tokens * 512 * 2 <= (2 << 20) else 256
    steps = D // tile
    whole = lambda *shape: pl.BlockSpec(shape, lambda i: (0,) * len(shape), pipeline_mode=pl.Buffered(1))
    first = lambda i: jnp.minimum(i, steps - 1)
    second = lambda i: jnp.maximum(i - steps, 0)
    anywhere = pl.BlockSpec(memory_space=pl.ANY)
    shape = jax.ShapeDtypeStruct
    return pl.pallas_call(
        functools.partial(weight_kernel, steps, inside),
        grid=(2 * steps,),
        in_specs=[
            pl.BlockSpec((tokens, tile), lambda i: (0, first(i))),
            pl.BlockSpec((tokens, tile), lambda i: (0, second(i))),
            whole(tokens, hidden),
            pl.BlockSpec((3, tile, local), lambda i: (0, first(i), 0)) if inside else whole(*wide.shape),
            anywhere,
            pl.BlockSpec((local, tile), lambda i: (0, second(i))) if inside else anywhere,
        ]
        + [whole(*small.shape) for small in smalls],
        out_specs=[
            pl.BlockSpec((tile, hidden), lambda i: (first(i), 0)),
            pl.BlockSpec((3, tile, local), lambda i: (0, first(i), 0)),
            pl.BlockSpec((hidden, tile), lambda i: (0, second(i))),
            pl.BlockSpec((local, tile), lambda i: (0, second(i))),
        ]
        + [whole(*small.shape) for small in smalls],
        out_shape=[
            shape((D, hidden), F32),
            shape((3, D, local), F32),
            shape((hidden, D), F32),
            shape((local, D), F32),
        ]
        + [shape(small.shape, F32) for small in smalls],
        scratch_shapes=[
            pltpu.VMEM((tokens, hidden), BF),
            pltpu.VMEM((16, 128) if inside else (tokens, local), BF),
            pltpu.SemaphoreType.DMA((2,)),
        ],
        compiler_params=pltpu.CompilerParams(vmem_limit_bytes=67000000),
        name="weights",
    )(normed, grads, pre, wide, hid, tall, *smalls)


def per_device(
    stream,
    norm_gain,
    norm_offset,
    attend_weight,
    attend_bias,
    output_weight,
    up_weight,
    up_bias,
    down_weight,
    final_bias,
    cotangent,
):
    R, S, D = stream.shape
    local = attend_weight.shape[2]
    hidden = up_weight.shape[1]
    TP, Z = lax.axis_size("tp"), lax.axis_size("seq")
    tokens = R * S * TP * Z
    inside = attention_inside(R * TP * Z)
    weights = jnp.swapaxes(attend_weight, 0, 1)
    (
        normed, grads, hid, pre, wide, tall, *smalls
    ) = block_call(
        stream, cotangent, norm_gain.reshape(1, D), norm_offset.reshape(1, D),
        final_bias.reshape(1, D), attend_bias, up_bias.reshape(1, hidden),
        weights, output_weight, up_weight, down_weight, Z, TP,
    )
    (
        up_grad, attend_grad, down_grad, output_grad,
        result, stream_grad, gain_grad, offset_grad, fbias_grad, abias_grad, ubias_grad,
    ) = weight_call(
        normed.reshape(tokens, D), grads.reshape(tokens, D), pre.reshape(tokens, hidden),
        wide if inside else wide.reshape(3, tokens, local), hid.reshape(tokens, hidden),
        tall if inside else tall.reshape(tokens, local), smalls, local, inside,
    )
    return (
        result,
        stream_grad,
        gain_grad.reshape(D),
        offset_grad.reshape(D),
        jnp.swapaxes(attend_grad, 0, 1),
        abias_grad,
        output_grad,
        up_grad,
        ubias_grad.reshape(hidden),
        down_grad,
        fbias_grad.reshape(D),
    )


def solution(mesh):
    in_specs = (
        P(("seq", "tp"), None, None),
        P(),
        P(),
        P(None, None, "tp"),
        P(None, "tp"),
        P("tp", None),
        P(None, "tp"),
        P("tp"),
        P("tp", None),
        P(),
        P(("seq", "tp"), None, None),
    )
    out_specs = (
        P(("seq", "tp"), None, None),
        P(("seq", "tp"), None, None),
        P(),
        P(),
        P(None, None, "tp"),
        P(None, "tp"),
        P("tp", None),
        P(None, "tp"),
        P("tp"),
        P("tp", None),
        P(),
    )
    return jax.shard_map(
        per_device, mesh=mesh, in_specs=in_specs, out_specs=out_specs, check_vma=False
    )
```
